8 devices in a mesh: gz: 2 (over z, y), gy: 2 (over x), gx: 2 (over core).
Axes of the slice: x: 2, y: 2, z: 1, core: 2. Of those that a mesh axis runs over, the one named last changes fastest.
Arguments:
- k_cell: float32 [144, 144, 144], P('gx', 'gy', 'gz')
- k_ghost: float32 [6, 144, 144], replicated
- f_rhs: float32 [144, 144, 144], P('gx', 'gy', 'gz')
- u_init: float32 [144, 144, 144], P('gx', 'gy', 'gz')
Outputs:
- output 1: float32 [144, 144, 144], P('gx', 'gy', 'gz')
- output 2: float32 [144, 144, 144], P('gx', 'gy', 'gz')
- output 3: float32 [8], replicated
All inputs are finite; a program needn't handle non-finite values.
Results may differ from the reference program's by a relative error of at most 0.001.
Values sent between devices are 32-bit elements.
A program may use at most 1 GiB of HBM per device.

```python
import jax
import jax.numpy as jnp
from jax import lax

GRID_SIDE = 144
CG_ITERS = 8


def setup_inputs(seed: int = 0) -> dict:
    grid_side = GRID_SIDE
    key_list = jax.random.split(jax.random.key(seed), 9)
    block_len = grid_side // 8
    cube_shape = (grid_side, grid_side, grid_side)
    cell_part = jax.random.uniform(key_list[0], cube_shape, jnp.float32, -1.0, 1.0)
    block_part = jax.random.uniform(key_list[1], (8, 8, 8), jnp.float32, -1.0, 1.0)
    block_part = jnp.repeat(jnp.repeat(jnp.repeat(block_part, block_len, axis=0), block_len, axis=1), block_len, axis=2)
    k_cell = jnp.exp(2.302585 * (0.5 * cell_part + 0.5 * block_part))
    k_ghost = jnp.exp(2.302585 * jax.random.uniform(key_list[2], (6, grid_side, grid_side), jnp.float32, -1.0, 1.0))
    coord_1d = jnp.arange(grid_side, dtype=jnp.float32) + 1.0
    wave_num = jax.random.randint(key_list[3], (3, 3), 1, 5).astype(jnp.float32)
    mode_amp = 2.0 * jax.random.normal(key_list[4], (3,), jnp.float32)
    profile = jnp.sin(jnp.pi * wave_num[:, :, None] * coord_1d[None, None, :] / (grid_side + 1.0))
    smooth = jnp.einsum('m,mi,mj,mk->ijk', mode_amp, profile[:, 0], profile[:, 1], profile[:, 2])
    src_pos = jax.random.randint(key_list[5], (64, 3), 1, 8) * block_len + jax.random.randint(key_list[6], (64, 3), -1, 1)
    src_amp = 10.0 * jax.random.normal(key_list[7], (64,), jnp.float32)
    f_rhs = smooth.at[src_pos[:, 0], src_pos[:, 1], src_pos[:, 2]].add(src_amp)
    u_init = 0.3 * jax.random.normal(key_list[8], cube_shape, jnp.float32)
    return {'k_cell': k_cell, 'k_ghost': k_ghost, 'f_rhs': f_rhs, 'u_init': u_init}


def reference(k_cell, k_ghost, f_rhs, u_init):
    k_x = jnp.concatenate([k_ghost[0][None], k_cell, k_ghost[1][None]], axis=0)
    k_y = jnp.concatenate([k_ghost[2][:, None], k_cell, k_ghost[3][:, None]], axis=1)
    k_z = jnp.concatenate([k_ghost[4][:, :, None], k_cell, k_ghost[5][:, :, None]], axis=2)
    coef_x = 2.0 * k_x[:-1] * k_x[1:] / (k_x[:-1] + k_x[1:])
    coef_y = 2.0 * k_y[:, :-1] * k_y[:, 1:] / (k_y[:, :-1] + k_y[:, 1:])
    coef_z = 2.0 * k_z[:, :, :-1] * k_z[:, :, 1:] / (k_z[:, :, :-1] + k_z[:, :, 1:])
    diag_sum = coef_x[:-1] + coef_x[1:] + coef_y[:, :-1] + coef_y[:, 1:] + coef_z[:, :, :-1] + coef_z[:, :, 1:]
    inv_diag = 1.0 / diag_sum

    def apply_op(grid_field):
        pad_x = jnp.pad(grid_field, ((1, 1), (0, 0), (0, 0)))
        pad_y = jnp.pad(grid_field, ((0, 0), (1, 1), (0, 0)))
        pad_z = jnp.pad(grid_field, ((0, 0), (0, 0), (1, 1)))
        flux_x = coef_x * (pad_x[1:] - pad_x[:-1])
        flux_y = coef_y * (pad_y[:, 1:] - pad_y[:, :-1])
        flux_z = coef_z * (pad_z[:, :, 1:] - pad_z[:, :, :-1])
        return (flux_x[:-1] - flux_x[1:]) + (flux_y[:, :-1] - flux_y[:, 1:]) + (flux_z[:, :, :-1] - flux_z[:, :, 1:])

    residual = f_rhs - apply_op(u_init)
    precond = residual * inv_diag
    rz_start = jnp.sum(residual * precond)

    def cg_step(cg_state, unused):
        approx, residual, direction, rz_old = cg_state
        q_vec = apply_op(direction)
        step_alpha = rz_old / jnp.sum(direction * q_vec)
        approx = approx + step_alpha * direction
        residual = residual - step_alpha * q_vec
        precond = residual * inv_diag
        rz_new = jnp.sum(residual * precond)
        direction = precond + (rz_new / rz_old) * direction
        return (approx, residual, direction, rz_new), jnp.sum(residual * residual)

    final_state, history = lax.scan(cg_step, (u_init, residual, precond, rz_start), None, length=CG_ITERS)
    return final_state[0], final_state[1], history
```

```python
import functools

import jax
import jax.numpy as jnp
from jax import lax
from jax.experimental import pallas as pl
from jax.experimental.pallas import tpu as pltpu
from jax.sharding import PartitionSpec as P


N = 72
H = 8
E = N + H
NB = 10
STEPS = 8
MESH = pl.DeviceIdType.MESH
F32 = jnp.float32
OTHERS = [(fx, fy, fz) for fx in (0, 1) for fy in (0, 1) for fz in (0, 1) if fx or fy or fz]
NDOT = 24
SUB = 8
LANES = 128
TILES = 9
PART = 24


def iota(axis):
    return lax.broadcasted_iota(jnp.int32, (SUB, LANES), axis)


def two_sum(a, b):
    s = a + b
    t = s - a
    return s, (a - (s - t)) + (b - t)


def quick(a, b):
    s = a + b
    return s, b - (s - a)


def two_prod(a, b):
    def split(x):
        t = x * 4097.0
        hi = t - (t - x)
        return hi, x - hi
    p = a * b
    ah, al = split(a)
    bh, bl = split(b)
    return p, ((ah * bh - p) + ah * bl + al * bh) + al * bl


def dadd(x, y):
    (xh, xl), (yh, yl) = x, y
    s, e = two_sum(xh, yh)
    return quick(s, e + (xl + yl))


def dsub(x, y):
    yh, yl = y
    return dadd(x, (-yh, -yl))


def dscale(x, c):
    hi, lo = x
    return hi * c, lo * c


def dmul(x, y):
    (xh, xl), (yh, yl) = x, y
    p, e = two_prod(xh, yh)
    return quick(p, e + (xh * yl + xl * yh))


def ddiv(x, y):
    (xh, xl), (yh, yl) = x, y
    q = xh / yh
    p, e = two_prod(q, yh)
    rest = ((xh - p) - e) + (xl - q * yl)
    return quick(q, rest / yh)


def step_lengths(m):
    alphas, betas = [], []
    y = dict(enumerate(m))
    p = {0: dsub(y[0], y[1])}
    for l in range(1, 15):
        p[l] = dsub(y[l], dscale(dadd(y[l + 1], y[l - 1]), 0.5))
    for t in range(STEPS):
        alpha = ddiv(y[t], p[t])
        alphas.append(alpha[0])
        if t == STEPS - 1:
            break
        y_next = {l: dsub(y[l], dmul(alpha, p[l])) for l in range(t + 1, 15 - t)}
        beta = ddiv(y_next[t + 1], p[t])
        if t:
            beta = dscale(beta, 0.5)
        betas.append(beta[0])
        p_next = {}
        for l in range(t + 1, 14 - t):
            side = y_next[l + 1] if l == t + 1 else dadd(y_next[l + 1], y_next[l - 1])
            p_next[l] = dadd(dsub(y_next[l], dscale(side, 0.5)), dmul(beta, p[l]))
        y, p = y_next, p_next
    return alphas, betas


def basis_coefs(alphas, betas):
    def add(a, b):
        return b if a is None else (a if b is None else a + b)

    def axpy(x, c, y):
        return [xi if yi is None else (c * yi if xi is None else xi + c * yi) for xi, yi in zip(x, y)]

    def apply_op(v):
        out = [None] * 11
        out[1] = v[0]
        for j in range(SUB):
            if v[1 + j] is None:
                continue
            c = v[1 + j]
            out[1 + j] = add(out[1 + j], c)
            if j == 0:
                out[2] = add(out[2], -c)
            else:
                half = -0.5 * c
                out[2 + j] = add(out[2 + j], half)
                out[j] = add(out[j], half)
        return out[:TILES]

    one = jnp.ones_like(alphas[0])
    y = [one] + [None] * SUB
    p = list(y)
    x = [None] * TILES
    ys = []
    for t in range(STEPS):
        q = apply_op(p)
        x = axpy(x, alphas[t], p)
        y = axpy(y, -alphas[t], q)
        ys.append(y)
        if t < STEPS - 1:
            p = axpy(y, betas[t], p)
    return ys, x


def row_down(v):
    return jnp.concatenate([pltpu.roll(v[NB - 1], 1, 0)[None], v[:NB - 1]], axis=0)


def row_up(v):
    return jnp.concatenate([v[1:], pltpu.roll(v[0], 7, 0)[None]], axis=0)


def lane_down(v):
    return pltpu.roll(v, 1, 2)


def lane_up(v):
    return pltpu.roll(v, 127, 2)


def load_chunk(ref, plane):
    return jnp.stack([ref[plane, pl.ds(b, SUB, stride=NB), :] for b in range(NB)], axis=0)


def replace(v, b, mask, value):
    return jnp.concatenate(([v[:b]] if b else []) + [jnp.where(mask, value, v[b])[None], v[b + 1:]], axis=0)


def harmonic(a, b):
    return 2.0 * a * b / (a + b)


def dot_pair(a, b):
    prod = a * b
    return jnp.sum(prod[:2], axis=0), jnp.sum(prod[2:], axis=0)


def own_cells(low, high):
    sub, lane = iota(0), iota(1)
    return jnp.where(lane < N, low + jnp.where(sub < 7, high, 0.0), 0.0)


def kernel(k_hbm, f_hbm, u_hbm, kg_hbm, kgt_hbm, uo_hbm, ro_hbm, rr_ref,
           k_in, u_in, f_in, k_nat, u_nat, z_nat, cx_a, cy_a, cz_a, isd_a, sd_a, v0_a, b_a,
           walls, wz_t, wy, ky, ux, zs, zr, ds_, dr, us, ur, uzs, uzr, acc, gath, rsend, rgath, coef,
           load_sem, out_sem, send_sem, recv_sem, all_send, all_recv):
    cx, cy, cz = lax.axis_index('gx'), lax.axis_index('gy'), lax.axis_index('gz')
    me = cx + 2 * cy + 4 * cz
    lane, sub = iota(1), iota(0)

    def peer(fx, fy, fz):
        out = {}
        if fx:
            out['gx'] = 1 - cx
        if fy:
            out['gy'] = 1 - cy
        if fz:
            out['gz'] = 1 - cz
        return out

    loads = []
    for n, (src, dst) in enumerate([(k_hbm, k_in), (u_hbm, u_in), (f_hbm, f_in)]):
        loads.append(pltpu.make_async_copy(src, dst, load_sem.at[n]))
    loads.append(pltpu.make_async_copy(kg_hbm.at[cx], walls.at[0], load_sem.at[3]))
    loads.append(pltpu.make_async_copy(kg_hbm.at[2 + cy], walls.at[1], load_sem.at[4]))
    loads.append(pltpu.make_async_copy(kgt_hbm.at[cz], walls.at[2], load_sem.at[5]))
    for n in (0, 1, 3, 4, 5, 2):
        loads[n].start()

    barrier = pltpu.get_barrier_semaphore()
    for flips in OTHERS:
        pl.semaphore_signal(barrier, inc=1, device_id=peer(*flips), device_id_type=MESH)
    pl.semaphore_wait(barrier, len(OTHERS))

    def send(n, src, dst, flips):
        copy = pltpu.make_async_remote_copy(src_ref=src, dst_ref=dst, send_sem=send_sem.at[n], recv_sem=recv_sem.at[n],
                                            device_id=peer(*flips), device_id_type=MESH)
        copy.start()
        return copy

    near_y = pl.multiple_of((N - H) * (1 - cy), SUB)
    near_x = (N - H) * (1 - cx)
    group8 = lane // SUB
    src8 = (N - H) * (1 - cz)
    dst8 = N + 48 * cz
    ghost8 = jnp.logical_and(lane >= dst8, lane < dst8 + SUB)
    wall_lane = 127 - 55 * cz
    own_lane = lane < N

    def widen(x):
        return x if x.shape[1] == LANES else jnp.concatenate([x, jnp.zeros((x.shape[0], LANES - x.shape[1]), F32)], axis=1)

    def pack(nat, packed, corner):
        def body(o, carry):
            for q in range(5):
                out = None
                for g in range(min(16, N - 16 * q)):
                    t = 16 * q + g
                    x = widen(nat[o * SUB + t // TILES, pl.ds(SUB * (t % TILES), SUB), :])
                    x = pltpu.roll(x, (SUB * g - src8 + LANES) % LANES, 1)
                    out = x if g == 0 else jnp.where(group8 == g, x, out)
                packed[o * 5 + q] = out
            out = None
            for g in range(SUB):
                x = widen(nat[o * SUB + g, pl.ds(near_y, SUB), :])
                x = pltpu.roll(x, (SUB * g - src8 + LANES) % LANES, 1)
                out = x if g == 0 else jnp.where(group8 == g, x, out)
            corner[o] = out
            return carry
        lax.fori_loop(0, TILES, body, 0)

    def unpack(own, side, nat, packed, corner, fill, wall):
        def body(o, carry):
            for pi in range(SUB):
                i = o * SUB + pi
                for jt in range(10):
                    if jt < TILES:
                        t = pi * TILES + jt
                        got, g = packed[o * 5 + t // 16], t % 16
                    else:
                        got, g = corner[o], pi
                    got = pltpu.roll(got, (dst8 - SUB * g + LANES) % LANES, 1)
                    x = widen(own[i, pl.ds(SUB * jt, SUB), :] if jt < TILES else side[i])
                    x = jnp.where(own_lane, x, jnp.where(ghost8, got, fill))
                    if wall is not None:
                        w = pltpu.roll(wall[pl.ds(SUB * jt, SUB), :], (wall_lane - i + LANES) % LANES, 1)
                        x = jnp.where(lane == wall_lane, w, x)
                    nat[i, pl.ds(SUB * jt, SUB), :] = x
            return carry
        lax.fori_loop(0, TILES, body, 0)

    loads[0].wait()
    k_y = send(0, k_in.at[:, pl.ds(near_y, SUB), :], ky, (0, 1, 0))
    pack(k_in, zs.at[0], ds_.at[0])
    loads[1].wait()
    u_row = (N - 1) * (1 - cy)
    u_lane = (N - 1) * (1 - cz)
    u_x = send(5, u_in.at[pl.ds((N - 1) * (1 - cx), 1)], ux, (1, 0, 0))

    def pack_u(o, carry):
        us[pl.ds(pl.multiple_of(o * SUB, SUB), SUB), :] = jnp.concatenate(
            [u_in[o * SUB + r, pl.ds(u_row, 1), :] for r in range(SUB)], axis=0)
        out = None
        for t in range(N):
            x = widen(u_in[o * SUB + t // TILES, pl.ds(SUB * (t % TILES), SUB), :])
            x = pltpu.roll(x, (t - u_lane + LANES) % LANES, 1)
            out = x if t == 0 else jnp.where(lane == t, x, out)
        uzs[o] = out
        return carry
    lax.fori_loop(0, TILES, pack_u, 0)

    k_z = send(1, zs.at[0], zr.at[0], (0, 0, 1))
    k_d = send(2, ds_.at[0], dr.at[0], (0, 1, 1))
    u_y = send(3, us, ur, (0, 1, 0))
    u_z = send(4, uzs, uzr, (0, 0, 1))

    for n in (3, 4, 5):
        loads[n].wait()

    def lane_ring(w, at, c):
        left, right = walls[w, pl.ds(at, SUB), 0:LANES], walls[w, pl.ds(at, SUB), LANES:144]
        right = jnp.concatenate([jnp.zeros((SUB, 56), F32), right, jnp.zeros((SUB, 56), F32)], axis=1)
        turned = jnp.where(jnp.logical_and(lane >= 56, lane < N), right, pltpu.roll(left, 56, 1))
        return jnp.where(c == 0, left, turned)

    for jt in range(10):
        at_j = pl.multiple_of(N * cy + SUB * jt if jt < TILES else N - H * cy, SUB)
        at_i = pl.multiple_of(N * cx + SUB * jt if jt < TILES else N - H * cx, SUB)
        k_nat[E, pl.ds(SUB * jt, SUB), :] = lane_ring(0, at_j, cz)
        wy[pl.ds(SUB * jt, SUB), :] = lane_ring(1, at_i, cz)
        wz_t[pl.ds(SUB * jt, SUB), :] = lane_ring(2, at_j, cx)

    loads[2].wait()

    def take_f(p, carry):
        for b in range(NB):
            rows = SUB if b < 2 else 7
            v0_a[p, b, 0:rows, 0:N] = f_in[p, pl.ds(b, rows, stride=NB), :]
        return carry
    lax.fori_loop(0, N, take_f, 0)

    k_y.wait()
    k_z.wait()
    k_d.wait()
    unpack(k_in, ky, k_nat, zr.at[0], dr.at[0], 1.0, wz_t)
    k_x = send(6, k_nat.at[pl.ds(near_x, SUB)], k_nat.at[pl.ds(N, SUB)], (1, 0, 0))

    u_z.wait()
    u_dst = N + 55 * cz

    def unpack_u(o, carry):
        for t in range(N):
            i, j = o * SUB + t // TILES, SUB * (t % TILES)
            got = pltpu.roll(uzr[o], (u_dst - t + LANES) % LANES, 1)
            x = widen(u_in[i, pl.ds(j, SUB), :])
            u_nat[i, pl.ds(j, SUB), :] = jnp.where(own_lane, x, jnp.where(lane == u_dst, got, 0.0))
        return carry
    u_x.wait()
    lax.fori_loop(0, TILES, unpack_u, 0)
    u_nat[E - 1 - 7 * cx] = jnp.zeros((E, LANES), F32)
    u_nat[N + 7 * cx, 0:N, 0:N] = ux[0]
    u_y.wait()
    k_x.wait()

    row0 = sub == 0
    row72 = sub == 7

    def faces(p, carry):
        kc = load_chunk(k_nat, p)
        before = jnp.where(jnp.logical_and(p == 0, cx == 0), E, jnp.where(p == 0, E - 1, p - 1))
        here = jnp.where(jnp.logical_and(p == N, cx == 1), E, p)
        cx_a[p] = harmonic(load_chunk(k_nat, here), load_chunk(k_nat, before))
        wall = jnp.broadcast_to(wy[pl.ds(p, 1), :], (SUB, LANES))
        low = replace(row_down(kc), 0, jnp.logical_and(row0, cy == 0), wall)
        high = replace(kc, 2, jnp.logical_and(row72, cy == 1), wall)
        cy_a[p] = harmonic(high, low)
        cz_a[p] = harmonic(kc, lane_down(kc))
        return carry
    lax.fori_loop(0, E, faces, 0)
    cx_a[E] = cx_a[0]

    def divergence(h_x, h_xn, h_y, h_z, v, v_prev, v_next, low_row, high_row):
        low = row_down(v)
        high = v
        if low_row is not None:
            low = replace(low, 0, row0, low_row)
            high = replace(v, 2, row72, high_row)
        else:
            low = replace(low, 0, jnp.logical_and(row0, cy == 0), 0.0)
            high = replace(v, 2, jnp.logical_and(row72, cy == 1), 0.0)
        f_y = h_y * (high - low)
        f_z = h_z * (v - lane_down(v))
        return ((h_x * (v - v_prev) - h_xn * (v_next - v)) + (f_y - row_up(f_y))) + (f_z - lane_up(f_z))

    def diag_of(p):
        h_x, h_xn, h_y, h_z = cx_a[p], cx_a[p + 1], cy_a[p], cz_a[p]
        d = ((h_x + h_xn) + (h_y + row_up(h_y))) + (h_z + lane_up(h_z))
        inv = lax.rsqrt(d)
        isd_a[p] = inv
        return h_x, h_xn, h_y, h_z, inv, d

    def start_own(p, carry):
        h_x, h_xn, h_y, h_z, inv, d = diag_of(p)
        sd_a[p] = d * inv
        before = jnp.where(p == 0, E - 1, p - 1)
        got = jnp.broadcast_to(widen(ur[pl.ds(p, 1), :]), (SUB, LANES))
        low_row = jnp.where(cy == 0, 0.0, got)
        high_row = jnp.where(cy == 0, got, 0.0)
        a_u = divergence(h_x, h_xn, h_y, h_z, load_chunk(u_nat, p), load_chunk(u_nat, before), load_chunk(u_nat, p + 1),
                         low_row, high_row)
        y0 = (v0_a[p] - a_u) * inv
        v0_a[p] = y0
        z0 = y0 * inv
        for b in range(NB):
            if b < 2:
                z_nat[p, pl.ds(b, SUB, stride=NB), :] = z0[b]
            else:
                z_nat[p, pl.ds(b, 7, stride=NB), :] = z0[b, :7]
        return carry
    lax.fori_loop(0, N, start_own, 0)

    def start_ghost(p, carry):
        diag_of(p)
        return carry

    z_y = send(7, z_nat.at[pl.ds(0, N), pl.ds(near_y, SUB), :], z_nat.at[pl.ds(0, N), pl.ds(N, SUB), :], (0, 1, 0))
    pack(z_nat, zs.at[1], ds_.at[1])
    lax.fori_loop(N, E, start_ghost, 0)
    z_z = send(SUB, zs.at[1], zr.at[1], (0, 0, 1))
    z_d = send(TILES, ds_.at[1], dr.at[1], (0, 1, 1))
    z_y.wait()
    z_z.wait()
    z_d.wait()
    unpack(z_nat, z_nat.at[:, pl.ds(N, SUB), :], z_nat, zr.at[1], dr.at[1], 0.0, None)
    z_x = send(10, z_nat.at[pl.ds(near_x, SUB)], z_nat.at[pl.ds(N, SUB)], (1, 0, 0))
    z_x.wait()

    def first(own, p, carry):
        before = jnp.where(p == 0, E - 1, p - 1)
        after = jnp.where(p == E - 1, 0, p + 1)
        h_x, h_xn, h_y, h_z, inv = cx_a[p], cx_a[p + 1], cy_a[p], cz_a[p], isd_a[p]
        z_p = jnp.where(jnp.logical_and(p == 0, cx == 0), 0.0, load_chunk(z_nat, before))
        z_n = jnp.where(jnp.logical_and(p == N - 1, cx == 1), 0.0, load_chunk(z_nat, after))
        b0 = inv * divergence(h_x, h_xn, h_y, h_z, load_chunk(z_nat, p), z_p, z_n, None, None)
        b_a[0, p] = b0
        cut = jnp.logical_or(jnp.logical_and(p == 0, cx == 0), jnp.logical_and(p == N, cx == 1))
        twice = 2.0 * inv
        cx_a[p] = jnp.where(cut, 0.0, h_x * (twice * isd_a[before]))
        c_y = h_y * (twice * row_down(inv))
        c_y = replace(c_y, 0, jnp.logical_and(row0, cy == 0), 0.0)
        cy_a[p] = replace(c_y, 2, jnp.logical_and(row72, cy == 1), 0.0)
        c_z = h_z * (twice * lane_down(inv))
        edge = N * cz
        cz_a[p] = jnp.where(lax.broadcasted_iota(jnp.int32, (NB, SUB, LANES), 2) == edge, 0.0, c_z)
        if not own:
            return carry
        v0 = v0_a[p]
        new = dot_pair(v0, v0) + dot_pair(v0, b0) + dot_pair(b0, b0)
        return tuple(c + n for c, n in zip(carry, new))

    zero = jnp.zeros((SUB, LANES), F32)
    sums = lax.fori_loop(0, N, functools.partial(first, True), (zero,) * 6)
    lax.fori_loop(N, E, functools.partial(first, False), 0)
    cx_a[E] = cx_a[0]
    acc[0] = own_cells(sums[0], sums[1])
    acc[1] = own_cells(sums[2], sums[3])
    acc[TILES] = own_cells(sums[4], sums[5])
    acc[23] = zero

    def advance(k, own, p, carry):
        before = jnp.where(p == 0, E - 1, p - 1)
        after = jnp.where(p == E - 1, 0, p + 1)
        v = b_a[k - 1, p]
        c_y, c_z = cy_a[p], cz_a[p]
        new = cx_a[p] * b_a[k - 1, before] + cx_a[p + 1] * b_a[k - 1, after]
        new = new + (c_y * row_down(v) + row_up(c_y * v))
        new = new + (c_z * lane_down(v) + lane_up(c_z * v))
        new = 0.5 * new if k == 1 else new - b_a[k - 2, p]
        b_a[k, p] = new
        if not own:
            return carry
        dots = dot_pair(v0_a[p], new) + dot_pair(v, new) + dot_pair(new, new)
        return tuple(c + n for c, n in zip(carry, dots))

    for k in range(1, STEPS):
        sums = lax.fori_loop(0, N, functools.partial(advance, k, True), (zero,) * 6)
        if k < STEPS - 1:
            lax.fori_loop(N, E, functools.partial(advance, k, False), 0)
        acc[1 + k] = own_cells(sums[0], sums[1])
        acc[16 + k - 1] = own_cells(sums[2], sums[3])
        if k < STEPS - 1:
            acc[TILES + k] = own_cells(sums[4], sums[5])

    def gather(buf, n_sem):
        copies = []
        for n, flips in enumerate(OTHERS):
            copies.append(pltpu.make_async_remote_copy(
                src_ref=buf.at[me], dst_ref=buf.at[me], send_sem=all_send.at[n_sem, n], recv_sem=all_recv.at[n_sem, n],
                device_id=peer(*flips), device_id_type=MESH))
        for copy in copies:
            copy.start()
        return copies

    hi = acc[:, 0, :]
    lo = jnp.zeros((NDOT, LANES), F32)
    for s in range(1, SUB):
        hi, err = two_sum(hi, acc[:, s, :])
        lo = lo + err
    gath[me, 0:NDOT] = hi
    gath[me, NDOT:2 * NDOT] = lo
    for copy in gather(gath, 0):
        copy.wait()
    hi, lo = gath[0, 0:NDOT], gath[0, NDOT:2 * NDOT]
    for dev in range(1, SUB):
        hi, err = two_sum(hi, gath[dev, 0:NDOT])
        lo = lo + (gath[dev, NDOT:2 * NDOT] + err)
    for shift in (64, 32, 16, SUB, 4, 2, 1):
        hi, err = two_sum(hi, pltpu.roll(hi, shift, 1))
        lo = (lo + pltpu.roll(lo, shift, 1)) + err
    hi, lo = quick(hi, lo)
    size = hi[0:1]
    factor = jnp.where(size > 1e30, 2.0 ** -110, jnp.where(size > 1e12, 2.0 ** -60, jnp.where(
        size < 1e-30, 2.0 ** 110, jnp.where(size < 1e-12, 2.0 ** 60, 1.0)))).astype(F32)
    hi, lo = hi * factor, lo * factor

    def total(row):
        return jnp.broadcast_to(hi[row:row + 1], (SUB, LANES)), jnp.broadcast_to(lo[row:row + 1], (SUB, LANES))

    n_mom = [total(TILES), total(16)]
    for j in range(1, 7):
        n_mom.append(dsub(dscale(total(TILES + j), 2.0), n_mom[0]))
        n_mom.append(dsub(dscale(total(16 + j), 2.0), n_mom[1]))
    l_mom = [total(1 + j) for j in range(SUB)]
    for j in range(7, 14):
        l_mom.append(dsub(dscale(dsub(l_mom[j], n_mom[j]), 2.0), l_mom[j - 1]))
    m_mom = [total(0)]
    m_mom.append(dsub(m_mom[0], l_mom[0]))
    for j in range(1, 15):
        m_mom.append(dsub(dscale(dsub(m_mom[j], l_mom[j]), 2.0), m_mom[j - 1]))
    ys, xs = basis_coefs(*step_lengths(m_mom))
    slot = {}
    for t in range(STEPS):
        for j in range(t + 1):
            slot[t, j] = len(slot)
            coef[slot[t, j]] = ys[t][1 + j]
    for j in range(SUB):
        slot['x', j] = len(slot)
        coef[slot['x', j]] = xs[j]

    def put(ref, p, b0, val):
        for b in range(val.shape[0]):
            if b0 + b < 2:
                ref[p, pl.ds(b0 + b, SUB, stride=NB), :] = val[b, :, :N]
            else:
                ref[p, pl.ds(b0 + b, 7, stride=NB), :] = val[b, :7, :N]

    def residuals(p, carry):
        carry = list(carry)
        for b0 in range(0, NB, 2):
            cut = pl.ds(b0, 2)
            v0, sd = v0_a[p, cut], sd_a[p, cut]
            bs = [b_a[j, p, cut] for j in range(SUB)]
            for t in range(STEPS):
                y = v0
                for j in range(t + 1):
                    y = y + coef[slot[t, j]] * bs[j]
                r = sd * y
                which = 2 * t + (b0 > 0)
                carry[which] = carry[which] + jnp.sum(r * r, axis=0)
                if t == STEPS - 1:
                    put(f_in, p, b0, r)
        return tuple(carry)

    outs = []

    def flush(n, nat, hbm, o):
        outs.append(pltpu.make_async_copy(nat.at[pl.ds(PART * o, PART)], hbm.at[pl.ds(PART * o, PART)],
                                          out_sem.at[n, o]))
        outs[-1].start()

    sums = (zero,) * 16
    for o in range(3):
        sums = lax.fori_loop(PART * o, PART * o + PART, residuals, sums)
        flush(0, f_in, ro_hbm, o)
    for t in range(STEPS):
        rsend[t] = own_cells(sums[2 * t], sums[2 * t + 1])
    part = rsend[:, 0, :]
    for s in range(1, SUB):
        part = part + rsend[:, s, :]
    rgath[me] = part
    rr_copies = gather(rgath, 1)

    def update(p, carry):
        for b0 in range(0, NB, 2):
            cut = pl.ds(b0, 2)
            x = coef[slot['x', 0]] * v0_a[p, cut]
            for j in range(1, SUB):
                x = x + coef[slot['x', j]] * b_a[j - 1, p, cut]
            x = x * isd_a[p, cut]
            u = jnp.stack([u_nat[p, pl.ds(b0 + b, SUB, stride=NB), :] for b in range(2)], axis=0)
            put(k_in, p, b0, u + x)
        return carry

    for o in range(3):
        lax.fori_loop(PART * o, PART * o + PART, update, 0)
        flush(1, k_in, uo_hbm, o)
    for copy in rr_copies:
        copy.wait()
    part = rgath[0]
    for dev in range(1, SUB):
        part = part + rgath[dev]
    part = jnp.broadcast_to(jnp.sum(part, axis=1, keepdims=True), (SUB, LANES))
    rr_ref[...] = part
    for copy in outs:
        copy.wait()


def solution(mesh):
    spec = P('gx', 'gy', 'gz')

    def local(k_cell, k_ghost, f_rhs, u_init):
        kgt = jnp.swapaxes(k_ghost[4:6], 1, 2)
        big = (E, NB, SUB, LANES)
        ext = (E + 1, NB, SUB, LANES)
        vm = lambda *shape: pltpu.VMEM(shape, F32)
        any_spec = pl.BlockSpec(memory_space=pl.ANY)
        block = jax.ShapeDtypeStruct((N, N, N), F32)
        u, r, rr = pl.pallas_call(
            kernel,
            out_shape=(block, block, jax.ShapeDtypeStruct((SUB, LANES), F32)),
            in_specs=[any_spec] * 5,
            out_specs=(any_spec, any_spec, pl.BlockSpec(memory_space=pltpu.VMEM)),
            scratch_shapes=[
                vm(N, N, N), vm(N, N, N), vm(N, N, N), vm(E + 1, E, LANES), vm(E, E, LANES), vm(E, E, LANES),
                vm(*ext), vm(*big), vm(*big), vm(*big), vm(N, NB, SUB, LANES), vm(N, NB, SUB, LANES), vm(SUB, *big),
                vm(3, 144, 144), vm(E, LANES), vm(E, LANES), vm(N, SUB, N), vm(1, N, N),
                vm(2, 45, SUB, LANES), vm(2, 45, SUB, LANES), vm(2, TILES, SUB, LANES), vm(2, TILES, SUB, LANES),
                vm(N, N), vm(N, N), vm(TILES, SUB, LANES), vm(TILES, SUB, LANES),
                vm(NDOT, SUB, LANES), vm(SUB, 2 * NDOT, LANES), vm(SUB, SUB, LANES), vm(SUB, SUB, LANES), vm(44, SUB, LANES),
                pltpu.SemaphoreType.DMA((6,)), pltpu.SemaphoreType.DMA((2, 3)),
                pltpu.SemaphoreType.DMA((11,)), pltpu.SemaphoreType.DMA((11,)),
                pltpu.SemaphoreType.DMA((2, 7)), pltpu.SemaphoreType.DMA((2, 7)),
            ],
            compiler_params=pltpu.CompilerParams(collective_id=0, has_side_effects=True, vmem_limit_bytes=67043328),
        )(k_cell, f_rhs, u_init, k_ghost, kgt)
        return u, r, rr[:, 0]

    return jax.shard_map(local, mesh=mesh, in_specs=(spec, P(), spec, spec), out_specs=(spec, spec, P()), check_vma=False)
```

```python
import functools

import jax
import jax.numpy as jnp
from jax import lax
from jax.experimental import pallas as pl
from jax.experimental.pallas import tpu as pltpu
from jax.sharding import PartitionSpec as P


N = 72
H = 8
E = N + H
NB = 10
STEPS = 8
MESH = pl.DeviceIdType.MESH
F32 = jnp.float32
OTHERS = [(fx, fy, fz) for fx in (0, 1) for fy in (0, 1) for fz in (0, 1) if fx or fy or fz]
NDOT = 24
SUB = 8
LANES = 128
TILES = 9
PART = 24


def iota(axis):
    return lax.broadcasted_iota(jnp.int32, (SUB, LANES), axis)


def two_sum(a, b):
    s = a + b
    t = s - a
    return s, (a - (s - t)) + (b - t)


def quick(a, b):
    s = a + b
    return s, b - (s - a)


def two_prod(a, b):
    def split(x):
        t = x * 4097.0
        hi = t - (t - x)
        return hi, x - hi
    p = a * b
    ah, al = split(a)
    bh, bl = split(b)
    return p, ((ah * bh - p) + ah * bl + al * bh) + al * bl


def dadd(x, y):
    (xh, xl), (yh, yl) = x, y
    s, e = two_sum(xh, yh)
    return quick(s, e + (xl + yl))


def dsub(x, y):
    yh, yl = y
    return dadd(x, (-yh, -yl))


def dscale(x, c):
    hi, lo = x
    return hi * c, lo * c


def dmul(x, y):
    (xh, xl), (yh, yl) = x, y
    p, e = two_prod(xh, yh)
    return quick(p, e + (xh * yl + xl * yh))


def ddiv(x, y):
    (xh, xl), (yh, yl) = x, y
    q = xh / yh
    p, e = two_prod(q, yh)
    rest = ((xh - p) - e) + (xl - q * yl)
    return quick(q, rest / yh)


def step_lengths(m):
    alphas, betas = [], []
    y = dict(enumerate(m))
    p = {0: dsub(y[0], y[1])}
    for l in range(1, 15):
        p[l] = dsub(y[l], dscale(dadd(y[l + 1], y[l - 1]), 0.5))
    for t in range(STEPS):
        alpha = ddiv(y[t], p[t])
        alphas.append(alpha[0])
        if t == STEPS - 1:
            break
        y_next = {l: dsub(y[l], dmul(alpha, p[l])) for l in range(t + 1, 15 - t)}
        beta = ddiv(y_next[t + 1], p[t])
        if t:
            beta = dscale(beta, 0.5)
        betas.append(beta[0])
        p_next = {}
        for l in range(t + 1, 14 - t):
            side = y_next[l + 1] if l == t + 1 else dadd(y_next[l + 1], y_next[l - 1])
            p_next[l] = dadd(dsub(y_next[l], dscale(side, 0.5)), dmul(beta, p[l]))
        y, p = y_next, p_next
    return alphas, betas


def basis_coefs(alphas, betas):
    def add(a, b):
        return b if a is None else (a if b is None else a + b)

    def axpy(x, c, y):
        return [xi if yi is None else (c * yi if xi is None else xi + c * yi) for xi, yi in zip(x, y)]

    def apply_op(v):
        out = [None] * 11
        out[1] = v[0]
        for j in range(SUB):
            if v[1 + j] is None:
                continue
            c = v[1 + j]
            out[1 + j] = add(out[1 + j], c)
            if j == 0:
                out[2] = add(out[2], -c)
            else:
                half = -0.5 * c
                out[2 + j] = add(out[2 + j], half)
                out[j] = add(out[j], half)
        return out[:TILES]

    one = jnp.ones_like(alphas[0])
    y = [one] + [None] * SUB
    p = list(y)
    x = [None] * TILES
    ys = []
    for t in range(STEPS):
        q = apply_op(p)
        x = axpy(x, alphas[t], p)
        y = axpy(y, -alphas[t], q)
        ys.append(y)
        if t < STEPS - 1:
            p = axpy(y, betas[t], p)
    return ys, x


def row_down(v):
    return jnp.concatenate([pltpu.roll(v[NB - 1], 1, 0)[None], v[:NB - 1]], axis=0)


def row_up(v):
    return jnp.concatenate([v[1:], pltpu.roll(v[0], 7, 0)[None]], axis=0)


def lane_down(v):
    return pltpu.roll(v, 1, 2)


def lane_up(v):
    return pltpu.roll(v, 127, 2)


def load_chunk(ref, plane):
    return jnp.stack([ref[plane, pl.ds(b, SUB, stride=NB), :] for b in range(NB)], axis=0)


def replace(v, b, mask, value):
    return jnp.concatenate(([v[:b]] if b else []) + [jnp.where(mask, value, v[b])[None], v[b + 1:]], axis=0)


def harmonic(a, b):
    return 2.0 * a * b / (a + b)


def dot_pair(a, b):
    prod = a * b
    return jnp.sum(prod[:2], axis=0), jnp.sum(prod[2:], axis=0)


def planes(lo, hi, body, init, width=4):
    def some(n, carry):
        for w in range(width):
            carry = body(lo + n * width + w, carry)
        return carry
    return lax.fori_loop(0, (hi - lo) // width, some, init)


def own_cells(low, high):
    sub, lane = iota(0), iota(1)
    return jnp.where(lane < N, low + jnp.where(sub < 7, high, 0.0), 0.0)


def kernel(k_hbm, f_hbm, u_hbm, kg_hbm, uo_hbm, ro_hbm, rr_ref,
           k_in, u_in, f_in, k_nat, u_nat, z_nat, cx_a, cy_a, cz_a, isd_a, v0_a, b0_a, b1_a, b2_a, b3_a, b4_a, b5_a, b6_a, b7_a,
           walls, wz, wz_t, wy, ky, ux, zs, zr, ds_, dr, us, ur, uzs, uzr, acc, gath, rsend, rgath, coef,
           load_sem, out_sem, send_sem, recv_sem, all_send, all_recv):
    cx, cy, cz = lax.axis_index('gx'), lax.axis_index('gy'), lax.axis_index('gz')
    me = cx + 2 * cy + 4 * cz
    b_a = (b0_a, b1_a, b2_a, b3_a, b4_a, b5_a, b6_a, b7_a)
    lane, sub = iota(1), iota(0)

    def peer(fx, fy, fz):
        out = {}
        if fx:
            out['gx'] = 1 - cx
        if fy:
            out['gy'] = 1 - cy
        if fz:
            out['gz'] = 1 - cz
        return out

    loads = []
    for n, (src, dst) in enumerate([(k_hbm, k_in), (u_hbm, u_in), (f_hbm, f_in)]):
        loads.append(pltpu.make_async_copy(src, dst, load_sem.at[n]))
    loads.append(pltpu.make_async_copy(kg_hbm.at[cx], walls.at[0], load_sem.at[3]))
    loads.append(pltpu.make_async_copy(kg_hbm.at[2 + cy], walls.at[1], load_sem.at[4]))
    loads.append(pltpu.make_async_copy(kg_hbm.at[4 + cz], walls.at[2], load_sem.at[5]))
    for n in (0, 1, 3, 4, 5, 2):
        loads[n].start()

    barrier = pltpu.get_barrier_semaphore()
    for flips in OTHERS:
        pl.semaphore_signal(barrier, inc=1, device_id=peer(*flips), device_id_type=MESH)
    pl.semaphore_wait(barrier, len(OTHERS))

    def send(n, src, dst, flips):
        copy = pltpu.make_async_remote_copy(src_ref=src, dst_ref=dst, send_sem=send_sem.at[n], recv_sem=recv_sem.at[n],
                                            device_id=peer(*flips), device_id_type=MESH)
        copy.start()
        return copy

    near_y = pl.multiple_of((N - H) * (1 - cy), SUB)
    near_x = (N - H) * (1 - cx)
    group8 = lane // SUB
    src8 = (N - H) * (1 - cz)
    dst8 = N + 48 * cz
    ghost8 = jnp.logical_and(lane >= dst8, lane < dst8 + SUB)
    wall_lane = 127 - 55 * cz
    own_lane = lane < N

    def widen(x):
        return x if x.shape[1] == LANES else jnp.concatenate([x, jnp.zeros((x.shape[0], LANES - x.shape[1]), F32)], axis=1)

    def pack(nat, packed, corner):
        def body(o, carry):
            for q in range(5):
                out = None
                for g in range(min(16, N - 16 * q)):
                    t = 16 * q + g
                    x = widen(nat[o * SUB + t // TILES, pl.ds(SUB * (t % TILES), SUB), :])
                    x = pltpu.roll(x, (SUB * g - src8 + LANES) % LANES, 1)
                    out = x if g == 0 else jnp.where(group8 == g, x, out)
                packed[o * 5 + q] = out
            out = None
            for g in range(SUB):
                x = widen(nat[o * SUB + g, pl.ds(near_y, SUB), :])
                x = pltpu.roll(x, (SUB * g - src8 + LANES) % LANES, 1)
                out = x if g == 0 else jnp.where(group8 == g, x, out)
            corner[o] = out
            return carry
        lax.fori_loop(0, TILES, body, 0)

    def unpack(own, side, nat, packed, corner, fill, wall):
        def body(o, carry):
            for pi in range(SUB):
                i = o * SUB + pi
                for jt in range(10):
                    if jt < TILES:
                        t = pi * TILES + jt
                        got, g = packed[o * 5 + t // 16], t % 16
                    else:
                        got, g = corner[o], pi
                    got = pltpu.roll(got, (dst8 - SUB * g + LANES) % LANES, 1)
                    x = widen(own[i, pl.ds(SUB * jt, SUB), :] if jt < TILES else side[i])
                    x = jnp.where(own_lane, x, jnp.where(ghost8, got, fill))
                    if wall is not None:
                        at = SUB * jt if jt < TILES else pl.multiple_of(N + 48 * cy, SUB)
                        w = pltpu.roll(wall[pl.ds(at, SUB), :], (wall_lane - i + LANES) % LANES, 1)
                        x = jnp.where(lane == wall_lane, w, x)
                    nat[i, pl.ds(SUB * jt, SUB), :] = x
            return carry
        lax.fori_loop(0, TILES, body, 0)

    loads[0].wait()
    k_y = send(0, k_in.at[:, pl.ds(near_y, SUB), :], ky, (0, 1, 0))
    pack(k_in, zs.at[0], ds_.at[0])
    loads[1].wait()
    u_row = (N - 1) * (1 - cy)
    u_lane = (N - 1) * (1 - cz)
    u_x = send(5, u_in.at[pl.ds((N - 1) * (1 - cx), 1)], ux, (1, 0, 0))

    def pack_u(o, carry):
        us[pl.ds(pl.multiple_of(o * SUB, SUB), SUB), :] = jnp.concatenate(
            [u_in[o * SUB + r, pl.ds(u_row, 1), :] for r in range(SUB)], axis=0)
        out = None
        for t in range(N):
            x = widen(u_in[o * SUB + t // TILES, pl.ds(SUB * (t % TILES), SUB), :])
            x = pltpu.roll(x, (t - u_lane + LANES) % LANES, 1)
            out = x if t == 0 else jnp.where(lane == t, x, out)
        uzs[o] = out
        return carry
    lax.fori_loop(0, TILES, pack_u, 0)

    k_z = send(1, zs.at[0], zr.at[0], (0, 0, 1))
    k_d = send(2, ds_.at[0], dr.at[0], (0, 1, 1))
    u_y = send(3, us, ur, (0, 1, 0))
    u_z = send(4, uzs, uzr, (0, 0, 1))

    for n in (3, 4, 5):
        loads[n].wait()

    def lane_ring(w, at, c):
        left, right = walls[w, pl.ds(at, SUB), 0:LANES], walls[w, pl.ds(at, SUB), LANES:144]
        right = jnp.concatenate([jnp.zeros((SUB, 56), F32), right, jnp.zeros((SUB, 56), F32)], axis=1)
        turned = jnp.where(jnp.logical_and(lane >= 56, lane < N), right, pltpu.roll(left, 56, 1))
        return jnp.where(c == 0, left, turned)

    for jt in range(10):
        at_j = pl.multiple_of(N * cy + SUB * jt if jt < TILES else N - H * cy, SUB)
        at_i = pl.multiple_of(N * cx + SUB * jt if jt < TILES else N - H * cx, SUB)
        k_nat[E, pl.ds(SUB * jt, SUB), :] = lane_ring(0, at_j, cz)
        wy[pl.ds(SUB * jt, SUB), :] = lane_ring(1, at_i, cz)
        if jt < TILES:
            wz[pl.ds(SUB * jt, SUB), :] = lane_ring(2, at_i, cy)

    loads[2].wait()

    def take_f(p, carry):
        for b in range(NB):
            rows = SUB if b < 2 else 7
            v0_a[p, b, 0:rows, 0:N] = f_in[p, pl.ds(b, rows, stride=NB), :]
        return carry
    lax.fori_loop(0, N, take_f, 0)

    wz_t[...] = wz[...].T

    k_y.wait()
    k_z.wait()
    k_d.wait()
    unpack(k_in, ky, k_nat, zr.at[0], dr.at[0], 1.0, wz_t)
    k_x = send(6, k_nat.at[pl.ds(near_x, SUB)], k_nat.at[pl.ds(N, SUB)], (1, 0, 0))

    u_z.wait()
    u_dst = N + 55 * cz

    def unpack_u(o, carry):
        for t in range(N):
            i, j = o * SUB + t // TILES, SUB * (t % TILES)
            got = pltpu.roll(uzr[o], (u_dst - t + LANES) % LANES, 1)
            x = widen(u_in[i, pl.ds(j, SUB), :])
            u_nat[i, pl.ds(j, SUB), :] = jnp.where(own_lane, x, jnp.where(lane == u_dst, got, 0.0))
        return carry
    u_x.wait()
    lax.fori_loop(0, TILES, unpack_u, 0)
    u_nat[E - 1 - 7 * cx] = jnp.zeros((E, LANES), F32)
    u_nat[N + 7 * cx, 0:N, 0:N] = ux[0]
    u_y.wait()
    k_x.wait()

    row0 = sub == 0
    row72 = sub == 7

    def faces(p, carry):
        kc = load_chunk(k_nat, p)
        before = jnp.where(jnp.logical_and(p == 0, cx == 0), E, jnp.where(p == 0, E - 1, p - 1))
        here = jnp.where(jnp.logical_and(p == N, cx == 1), E, p)
        cx_a[p] = harmonic(load_chunk(k_nat, here), load_chunk(k_nat, before))
        wall = jnp.broadcast_to(wy[pl.ds(p, 1), :], (SUB, LANES))
        low = replace(row_down(kc), 0, jnp.logical_and(row0, cy == 0), wall)
        high = replace(kc, 2, jnp.logical_and(row72, cy == 1), wall)
        cy_a[p] = harmonic(high, low)
        cz_a[p] = harmonic(kc, lane_down(kc))
        return carry
    planes(0, E, faces, 0)
    cx_a[E] = cx_a[0]

    def divergence(h_x, h_xn, h_y, h_z, v, v_prev, v_next, low_row, high_row):
        low = row_down(v)
        high = v
        if low_row is not None:
            low = replace(low, 0, row0, low_row)
            high = replace(v, 2, row72, high_row)
        else:
            low = replace(low, 0, jnp.logical_and(row0, cy == 0), 0.0)
            high = replace(v, 2, jnp.logical_and(row72, cy == 1), 0.0)
        f_y = h_y * (high - low)
        f_z = h_z * (v - lane_down(v))
        return ((h_x * (v - v_prev) - h_xn * (v_next - v)) + (f_y - row_up(f_y))) + (f_z - lane_up(f_z))

    def diag_of(p):
        h_x, h_xn, h_y, h_z = cx_a[p], cx_a[p + 1], cy_a[p], cz_a[p]
        d = ((h_x + h_xn) + (h_y + row_up(h_y))) + (h_z + lane_up(h_z))
        inv = lax.rsqrt(d)
        isd_a[p] = inv
        return h_x, h_xn, h_y, h_z, inv, d

    def start_own(p, carry):
        h_x, h_xn, h_y, h_z, inv, d = diag_of(p)
        sd = d * inv
        for b in range(NB):
            k_nat[p, pl.ds(SUB * b, SUB), :] = sd[b]
        before = jnp.where(p == 0, E - 1, p - 1)
        got = jnp.broadcast_to(widen(ur[pl.ds(p, 1), :]), (SUB, LANES))
        low_row = jnp.where(cy == 0, 0.0, got)
        high_row = jnp.where(cy == 0, got, 0.0)
        a_u = divergence(h_x, h_xn, h_y, h_z, load_chunk(u_nat, p), load_chunk(u_nat, before), load_chunk(u_nat, p + 1),
                         low_row, high_row)
        y0 = (v0_a[p] - a_u) * inv
        v0_a[p] = y0
        z0 = y0 * inv
        for b in range(NB):
            if b < 2:
                z_nat[p, pl.ds(b, SUB, stride=NB), :] = z0[b]
            else:
                z_nat[p, pl.ds(b, 7, stride=NB), :] = z0[b, :7]
        return carry
    planes(0, N, start_own, 0)

    def start_ghost(p, carry):
        diag_of(p)
        return carry

    z_y = send(7, z_nat.at[pl.ds(0, N), pl.ds(near_y, SUB), :], z_nat.at[pl.ds(0, N), pl.ds(N, SUB), :], (0, 1, 0))
    pack(z_nat, zs.at[1], ds_.at[1])
    planes(N, E, start_ghost, 0)
    z_z = send(SUB, zs.at[1], zr.at[1], (0, 0, 1))
    z_d = send(TILES, ds_.at[1], dr.at[1], (0, 1, 1))
    z_y.wait()
    z_z.wait()
    z_d.wait()
    unpack(z_nat, z_nat.at[:, pl.ds(N, SUB), :], z_nat, zr.at[1], dr.at[1], 0.0, None)
    z_x = send(10, z_nat.at[pl.ds(near_x, SUB)], z_nat.at[pl.ds(N, SUB)], (1, 0, 0))
    z_x.wait()

    def first(own, p, carry):
        before = jnp.where(p == 0, E - 1, p - 1)
        after = jnp.where(p == E - 1, 0, p + 1)
        h_x, h_xn, h_y, h_z, inv = cx_a[p], cx_a[p + 1], cy_a[p], cz_a[p], isd_a[p]
        z_p = jnp.where(jnp.logical_and(p == 0, cx == 0), 0.0, load_chunk(z_nat, before))
        z_n = jnp.where(jnp.logical_and(p == N - 1, cx == 1), 0.0, load_chunk(z_nat, after))
        b0 = inv * divergence(h_x, h_xn, h_y, h_z, load_chunk(z_nat, p), z_p, z_n, None, None)
        b_a[0][p + 1] = b0
        cut = jnp.logical_or(jnp.logical_and(p == 0, cx == 0), jnp.logical_and(p == N, cx == 1))
        twice = 2.0 * inv
        cx_a[p] = jnp.where(cut, 0.0, h_x * (twice * isd_a[before]))
        c_y = h_y * (twice * row_down(inv))
        c_y = replace(c_y, 0, jnp.logical_and(row0, cy == 0), 0.0)
        cy_a[p] = replace(c_y, 2, jnp.logical_and(row72, cy == 1), 0.0)
        c_z = h_z * (twice * lane_down(inv))
        edge = N * cz
        cz_a[p] = jnp.where(lax.broadcasted_iota(jnp.int32, (NB, SUB, LANES), 2) == edge, 0.0, c_z)
        if not own:
            return carry
        v0 = v0_a[p]
        new = dot_pair(v0, v0) + dot_pair(v0, b0) + dot_pair(b0, b0)
        return tuple(c + n for c, n in zip(carry, new))

    zero = jnp.zeros((SUB, LANES), F32)

    def wrap(ref):
        ref[0] = ref[E]
        ref[E + 1] = ref[1]
    sums = planes(0, N, functools.partial(first, True), (zero,) * 6)
    planes(N, E, functools.partial(first, False), 0)
    cx_a[E] = cx_a[0]
    wrap(b_a[0])
    acc[0] = own_cells(sums[0], sums[1])
    acc[1] = own_cells(sums[2], sums[3])
    acc[TILES] = own_cells(sums[4], sums[5])
    acc[23] = zero

    def advance(k, own, p, carry):
        old, here = b_a[k - 1], p + 1
        v = old[here]
        c_y, c_z = cy_a[p], cz_a[p]
        new = cx_a[p] * old[here - 1] + cx_a[p + 1] * old[here + 1]
        new = new + (c_y * row_down(v) + row_up(c_y * v))
        new = new + (c_z * lane_down(v) + lane_up(c_z * v))
        new = 0.5 * new if k == 1 else new - b_a[k - 2][here]
        b_a[k][here] = new
        if not own:
            return carry
        dots = dot_pair(v0_a[p], new) + dot_pair(v, new) + dot_pair(new, new)
        return tuple(c + n for c, n in zip(carry, dots))

    for k in range(1, STEPS):
        sums = planes(0, N, functools.partial(advance, k, True), (zero,) * 6)
        if k < STEPS - 1:
            planes(N, E, functools.partial(advance, k, False), 0)
            wrap(b_a[k])
        acc[1 + k] = own_cells(sums[0], sums[1])
        acc[16 + k - 1] = own_cells(sums[2], sums[3])
        if k < STEPS - 1:
            acc[TILES + k] = own_cells(sums[4], sums[5])

    def gather(buf, n_sem):
        copies = []
        for n, flips in enumerate(OTHERS):
            copies.append(pltpu.make_async_remote_copy(
                src_ref=buf.at[me], dst_ref=buf.at[me], send_sem=all_send.at[n_sem, n], recv_sem=all_recv.at[n_sem, n],
                device_id=peer(*flips), device_id_type=MESH))
        for copy in copies:
            copy.start()
        return copies

    hi = acc[:, 0, :]
    lo = jnp.zeros((NDOT, LANES), F32)
    for s in range(1, SUB):
        hi, err = two_sum(hi, acc[:, s, :])
        lo = lo + err
    gath[me, 0:NDOT] = hi
    gath[me, NDOT:2 * NDOT] = lo
    for copy in gather(gath, 0):
        copy.wait()
    hi, lo = gath[0, 0:NDOT], gath[0, NDOT:2 * NDOT]
    for dev in range(1, SUB):
        hi, err = two_sum(hi, gath[dev, 0:NDOT])
        lo = lo + (gath[dev, NDOT:2 * NDOT] + err)
    for shift in (64, 32, 16, SUB, 4, 2, 1):
        hi, err = two_sum(hi, pltpu.roll(hi, shift, 1))
        lo = (lo + pltpu.roll(lo, shift, 1)) + err
    hi, lo = quick(hi, lo)
    size = hi[0:1]
    factor = jnp.where(size > 1e30, 2.0 ** -110, jnp.where(size > 1e12, 2.0 ** -60, jnp.where(
        size < 1e-30, 2.0 ** 110, jnp.where(size < 1e-12, 2.0 ** 60, 1.0)))).astype(F32)
    hi, lo = hi * factor, lo * factor

    def total(row):
        return jnp.broadcast_to(hi[row:row + 1], (SUB, LANES)), jnp.broadcast_to(lo[row:row + 1], (SUB, LANES))

    n_mom = [total(TILES), total(16)]
    for j in range(1, 7):
        n_mom.append(dsub(dscale(total(TILES + j), 2.0), n_mom[0]))
        n_mom.append(dsub(dscale(total(16 + j), 2.0), n_mom[1]))
    l_mom = [total(1 + j) for j in range(SUB)]
    for j in range(7, 14):
        l_mom.append(dsub(dscale(dsub(l_mom[j], n_mom[j]), 2.0), l_mom[j - 1]))
    m_mom = [total(0)]
    m_mom.append(dsub(m_mom[0], l_mom[0]))
    for j in range(1, 15):
        m_mom.append(dsub(dscale(dsub(m_mom[j], l_mom[j]), 2.0), m_mom[j - 1]))
    ys, xs = basis_coefs(*step_lengths(m_mom))
    slot = {}
    for t in range(STEPS):
        for j in range(t + 1):
            slot[t, j] = len(slot)
            coef[slot[t, j]] = ys[t][1 + j]
    for j in range(SUB):
        slot['x', j] = len(slot)
        coef[slot['x', j]] = xs[j]

    def put(ref, p, b0, val):
        for b in range(val.shape[0]):
            if b0 + b < 2:
                ref[p, pl.ds(b0 + b, SUB, stride=NB), :] = val[b, :, :N]
            else:
                ref[p, pl.ds(b0 + b, 7, stride=NB), :] = val[b, :7, :N]

    def residuals(p, carry):
        carry = list(carry)
        for b0 in range(0, NB, 2):
            cut = pl.ds(b0, 2)
            v0 = v0_a[p, cut]
            sd = jnp.stack([k_nat[p, pl.ds(SUB * (b0 + b), SUB), :] for b in range(2)], axis=0)
            bs = [ref[p + 1, cut] for ref in b_a]
            for t in range(STEPS):
                y = v0
                for j in range(t + 1):
                    y = y + coef[slot[t, j]] * bs[j]
                r = sd * y
                which = 2 * t + (b0 > 0)
                carry[which] = carry[which] + jnp.sum(r * r, axis=0)
                if t == STEPS - 1:
                    put(f_in, p, b0, r)
        return tuple(carry)

    outs = []

    def flush(n, nat, hbm, o):
        outs.append(pltpu.make_async_copy(nat.at[pl.ds(PART * o, PART)], hbm.at[pl.ds(PART * o, PART)],
                                          out_sem.at[n, o]))
        outs[-1].start()

    sums = (zero,) * 16
    for o in range(3):
        sums = lax.fori_loop(PART * o, PART * o + PART, residuals, sums)
        flush(0, f_in, ro_hbm, o)
    for t in range(STEPS):
        rsend[t] = own_cells(sums[2 * t], sums[2 * t + 1])
    part = rsend[:, 0, :]
    for s in range(1, SUB):
        part = part + rsend[:, s, :]
    rgath[me] = part
    rr_copies = gather(rgath, 1)

    def update(p, carry):
        for b0 in range(0, NB, 2):
            cut = pl.ds(b0, 2)
            x = coef[slot['x', 0]] * v0_a[p, cut]
            for j in range(1, SUB):
                x = x + coef[slot['x', j]] * b_a[j - 1][p + 1, cut]
            x = x * isd_a[p, cut]
            u = jnp.stack([u_nat[p, pl.ds(b0 + b, SUB, stride=NB), :] for b in range(2)], axis=0)
            put(k_in, p, b0, u + x)
        return carry

    for o in range(3):
        lax.fori_loop(PART * o, PART * o + PART, update, 0)
        flush(1, k_in, uo_hbm, o)
    for copy in rr_copies:
        copy.wait()
    part = rgath[0]
    for dev in range(1, SUB):
        part = part + rgath[dev]
    part = jnp.broadcast_to(jnp.sum(part, axis=1, keepdims=True), (SUB, LANES))
    rr_ref[...] = jnp.sum(jnp.where(lane == sub, part, 0.0), axis=0, keepdims=True)[:, :STEPS]
    for copy in outs:
        copy.wait()


def solution(mesh):
    spec = P('gx', 'gy', 'gz')

    def local(k_cell, k_ghost, f_rhs, u_init):
        big = (E, NB, SUB, LANES)
        ext = (E + 1, NB, SUB, LANES)
        vm = lambda *shape: pltpu.VMEM(shape, F32)
        any_spec = pl.BlockSpec(memory_space=pl.ANY)
        block = jax.ShapeDtypeStruct((N, N, N), F32)
        u, r, rr = pl.pallas_call(
            kernel,
            out_shape=(block, block, jax.ShapeDtypeStruct((1, STEPS), F32)),
            in_specs=[any_spec] * 4,
            out_specs=(any_spec, any_spec, pl.BlockSpec(memory_space=pltpu.VMEM)),
            scratch_shapes=[
                vm(N, N, N), vm(N, N, N), vm(N, N, N), vm(E + 1, E, LANES), vm(E, E, LANES), vm(E, E, LANES),
                vm(*ext), vm(*big), vm(*big), vm(*big), vm(N, NB, SUB, LANES),
                *[vm(E + 2, NB, SUB, LANES)] * STEPS,
                vm(3, 144, 144), vm(LANES, LANES), vm(LANES, LANES), vm(E, LANES), vm(N, SUB, N), vm(1, N, N),
                vm(2, 45, SUB, LANES), vm(2, 45, SUB, LANES), vm(2, TILES, SUB, LANES), vm(2, TILES, SUB, LANES),
                vm(N, N), vm(N, N), vm(TILES, SUB, LANES), vm(TILES, SUB, LANES),
                vm(NDOT, SUB, LANES), vm(SUB, 2 * NDOT, LANES), vm(SUB, SUB, LANES), vm(SUB, SUB, LANES), vm(44, SUB, LANES),
                pltpu.SemaphoreType.DMA((6,)), pltpu.SemaphoreType.DMA((2, 3)),
                pltpu.SemaphoreType.DMA((11,)), pltpu.SemaphoreType.DMA((11,)),
                pltpu.SemaphoreType.DMA((2, 7)), pltpu.SemaphoreType.DMA((2, 7)),
            ],
            compiler_params=pltpu.CompilerParams(collective_id=0, has_side_effects=True, vmem_limit_bytes=67043328),
        )(k_cell, f_rhs, u_init, k_ghost)
        return u, r, rr.reshape(STEPS)

    return jax.shard_map(local, mesh=mesh, in_specs=(spec, P(), spec, spec), out_specs=(spec, spec, P()), check_vma=False)
```

```python
import functools

import jax
import jax.numpy as jnp
from jax import lax
from jax.experimental import pallas as pl
from jax.experimental.pallas import tpu as pltpu
from jax.sharding import PartitionSpec as P


N = 72
H = 8
E = N + H
NB = 10
STEPS = 8
MESH = pl.DeviceIdType.MESH
F32 = jnp.float32
OTHERS = [(fx, fy, fz) for fx in (0, 1) for fy in (0, 1) for fz in (0, 1) if fx or fy or fz]
NDOT = 24
SUB = 8
LANES = 128
TILES = 9
PART = 24
WIDTH = 4
LAST = 7
GROUPS = 16
PIECES = 5
ZERO, ONE, HALF, TWO = 0.0, 1.0, 0.5, 2.0


def iota(axis):
    return lax.broadcasted_iota(jnp.int32, (SUB, LANES), axis)


def two_sum(a, b):
    s = a + b
    t = s - a
    return s, (a - (s - t)) + (b - t)


def quick(a, b):
    s = a + b
    return s, b - (s - a)


def two_prod(a, b):
    def split(x):
        t = x * 4097.0
        hi = t - (t - x)
        return hi, x - hi
    p = a * b
    ah, al = split(a)
    bh, bl = split(b)
    return p, ((ah * bh - p) + ah * bl + al * bh) + al * bl


def dadd(x, y):
    (xh, xl), (yh, yl) = x, y
    s, e = two_sum(xh, yh)
    return quick(s, e + (xl + yl))


def dsub(x, y):
    yh, yl = y
    return dadd(x, (-yh, -yl))


def dscale(x, c):
    hi, lo = x
    return hi * c, lo * c


def dmul(x, y):
    (xh, xl), (yh, yl) = x, y
    p, e = two_prod(xh, yh)
    return quick(p, e + (xh * yl + xl * yh))


def ddiv(x, y):
    (xh, xl), (yh, yl) = x, y
    q = xh / yh
    p, e = two_prod(q, yh)
    rest = ((xh - p) - e) + (xl - q * yl)
    return quick(q, rest / yh)


def step_lengths(m):
    alphas, betas = [], []
    y = dict(enumerate(m))
    p = {0: dsub(y[0], y[1])}
    for l in range(1, 15):
        p[l] = dsub(y[l], dscale(dadd(y[l + 1], y[l - 1]), HALF))
    for t in range(STEPS):
        alpha = ddiv(y[t], p[t])
        alphas.append(alpha[0])
        if t == STEPS - 1:
            break
        y_next = {l: dsub(y[l], dmul(alpha, p[l])) for l in range(t + 1, 15 - t)}
        beta = ddiv(y_next[t + 1], p[t])
        if t:
            beta = dscale(beta, HALF)
        betas.append(beta[0])
        p_next = {}
        for l in range(t + 1, 14 - t):
            side = y_next[l + 1] if l == t + 1 else dadd(y_next[l + 1], y_next[l - 1])
            p_next[l] = dadd(dsub(y_next[l], dscale(side, HALF)), dmul(beta, p[l]))
        y, p = y_next, p_next
    return alphas, betas


def basis_coefs(alphas, betas):
    def add(a, b):
        return b if a is None else (a if b is None else a + b)

    def axpy(x, c, y):
        return [xi if yi is None else (c * yi if xi is None else xi + c * yi) for xi, yi in zip(x, y)]

    def apply_op(v):
        out = [None] * 11
        out[1] = v[0]
        for j in range(SUB):
            if v[1 + j] is None:
                continue
            c = v[1 + j]
            out[1 + j] = add(out[1 + j], c)
            if j == 0:
                out[2] = add(out[2], -c)
            else:
                half = -HALF * c
                out[2 + j] = add(out[2 + j], half)
                out[j] = add(out[j], half)
        return out[:TILES]

    one = jnp.ones_like(alphas[0])
    y = [one] + [None] * SUB
    p = list(y)
    x = [None] * TILES
    ys = []
    for t in range(STEPS):
        q = apply_op(p)
        x = axpy(x, alphas[t], p)
        y = axpy(y, -alphas[t], q)
        ys.append(y)
        if t < STEPS - 1:
            p = axpy(y, betas[t], p)
    return ys, x


def row_down(v):
    return jnp.concatenate([pltpu.roll(v[NB - 1], 1, 0)[None], v[:NB - 1]], axis=0)


def row_up(v):
    return jnp.concatenate([v[1:], pltpu.roll(v[0], LAST, 0)[None]], axis=0)


def lane_down(v):
    return pltpu.roll(v, 1, 2)


def lane_up(v):
    return pltpu.roll(v, 127, 2)


def load_chunk(ref, plane):
    return jnp.stack([ref[plane, pl.ds(b, SUB, stride=NB), :] for b in range(NB)], axis=0)


def replace(v, b, mask, value):
    return jnp.concatenate(([v[:b]] if b else []) + [jnp.where(mask, value, v[b])[None], v[b + 1:]], axis=0)


def harmonic(a, b):
    return TWO * a * b / (a + b)


def dot_pair(a, b):
    prod = a * b
    return jnp.sum(prod[:2], axis=0), jnp.sum(prod[2:], axis=0)


def pick(mask, a, b):
    return lax.select_n(mask, b, a)


def planes(lo, hi, body, init, width=WIDTH):
    def some(n, carry):
        for w in range(width):
            carry = body(lo + n * width + w, carry)
        return carry
    return lax.fori_loop(0, (hi - lo) // width, some, init)


def own_cells(low, high):
    sub, lane = iota(0), iota(1)
    return jnp.where(lane < N, low + jnp.where(sub < LAST, high, ZERO), ZERO)


def kernel(k_hbm, f_hbm, u_hbm, kg_hbm, uo_hbm, ro_hbm, rr_ref,
           k_in, u_in, f_in, k_nat, u_nat, z_nat, cx_a, cy_a, cz_a, isd_a, v0_a, b0_a, b1_a, b2_a, b3_a, b4_a, b5_a, b6_a, b7_a,
           walls, wz, wz_t, wy, ky, kx, ux, zs, zr, ds_, dr, row_s, row_r, lane_s, lane_r, acc, gath, rsend, rgath, coef,
           load_sem, out_sem, send_sem, recv_sem, all_send, all_recv):
    cx, cy, cz = lax.axis_index('gx'), lax.axis_index('gy'), lax.axis_index('gz')
    me = cx + 2 * cy + 4 * cz
    b_a = (b0_a, b1_a, b2_a, b3_a, b4_a, b5_a, b6_a, b7_a)
    lane, sub = iota(1), iota(0)

    def peer(fx, fy, fz):
        out = {}
        if fx:
            out['gx'] = 1 - cx
        if fy:
            out['gy'] = 1 - cy
        if fz:
            out['gz'] = 1 - cz
        return out

    loads = []
    for n, (src, dst) in enumerate([(k_hbm, k_in), (u_hbm, u_in), (f_hbm, f_in)]):
        loads.append(pltpu.make_async_copy(src, dst, load_sem.at[n]))
    loads.append(pltpu.make_async_copy(kg_hbm.at[cx], walls.at[0], load_sem.at[3]))
    loads.append(pltpu.make_async_copy(kg_hbm.at[2 + cy], walls.at[1], load_sem.at[4]))
    loads.append(pltpu.make_async_copy(kg_hbm.at[4 + cz], walls.at[2], load_sem.at[PIECES]))
    for n in (0, 1, 3, 4, PIECES, 2):
        loads[n].start()

    barrier = pltpu.get_barrier_semaphore()
    for flips in OTHERS:
        pl.semaphore_signal(barrier, inc=1, device_id=peer(*flips), device_id_type=MESH)
    pl.semaphore_wait(barrier, len(OTHERS))

    def send(n, src, dst, flips):
        copy = pltpu.make_async_remote_copy(src_ref=src, dst_ref=dst, send_sem=send_sem.at[n], recv_sem=recv_sem.at[n],
                                            device_id=peer(*flips), device_id_type=MESH)
        copy.start()
        return copy

    near_y = pl.multiple_of((N - H) * (1 - cy), SUB)
    near_x = (N - H) * (1 - cx)
    group8 = lane // SUB
    src8 = (N - H) * (1 - cz)
    dst8 = N + 48 * cz
    ghost8 = jnp.logical_and(lane >= dst8, lane < dst8 + SUB)
    wall_lane = 127 - 55 * cz
    own_lane = lane < N
    at_wall = lane == wall_lane
    zero = jnp.zeros((SUB, LANES), F32)
    ones = jnp.ones((SUB, LANES), F32)

    def turn(x, by):
        return pltpu.roll(x, lax.rem(by + LANES, LANES), 1)

    def widen(x):
        return x if x.shape[1] == LANES else jnp.concatenate([x, jnp.zeros((x.shape[0], LANES - x.shape[1]), F32)], axis=1)

    def pack(nat, packed, corner):
        groups = [group8 == g for g in range(GROUPS)]

        def body(o, carry):
            for q in range(PIECES):
                out = None
                for g in range(min(GROUPS, N - GROUPS * q)):
                    t = GROUPS * q + g
                    if t % TILES == 0:
                        plane = widen(nat[o * SUB + t // TILES, 0:N, :])
                    x = turn(plane[SUB * (t % TILES):SUB * (t % TILES) + SUB], SUB * g - src8)
                    out = x if g == 0 else pick(groups[g], x, out)
                packed[o * PIECES + q] = out
            out = None
            for g in range(SUB):
                x = widen(nat[o * SUB + g, pl.ds(near_y, SUB), :])
                x = turn(x, SUB * g - src8)
                out = x if g == 0 else pick(groups[g], x, out)
            corner[o] = out
            return carry
        lax.fori_loop(0, TILES, body, 0)

    def unpack(own, side, nat, packed, corner, fill, wall, o, carry):
        packs, corner_in = [packed[o * PIECES + q] for q in range(PIECES)], corner[o]
        for pi in range(SUB):
            i, out = o * SUB + pi, []
            plane = widen(own[i, 0:N, :])
            for jt in range(NB):
                if jt < TILES:
                    t = pi * TILES + jt
                    got, g = packs[t // GROUPS], t % GROUPS
                else:
                    got, g = corner_in, pi
                x = plane[SUB * jt:SUB * jt + SUB] if jt < TILES else widen(side[i])
                other = fill if wall is None else pick(at_wall, wall_column(i, jt), fill)
                out.append(pick(own_lane, x, pick(ghost8, turn(got, dst8 - SUB * g), other)))
            nat[i, 0:E, :] = jnp.concatenate(out, axis=0)
        return carry

    def wall_column(i, jt):
        at = SUB * jt if jt < TILES else pl.multiple_of(N + 48 * cy, SUB)
        return turn(wz_t[pl.ds(at, SUB), :], wall_lane - i)

    loads[0].wait()
    loads[1].wait()
    last_x, last_y, last_z = (N - 1) * (1 - cx), (N - 1) * (1 - cy), (N - 1) * (1 - cz)
    one_x = [send(0, k_in.at[pl.ds(last_x, 1)], kx, (1, 0, 0)), send(1, u_in.at[pl.ds(last_x, 1)], ux, (1, 0, 0))]

    def pack_one(o, carry):
        for n, src in enumerate((k_in, u_in)):
            row_s[n, pl.ds(pl.multiple_of(o * SUB, SUB), SUB), :] = jnp.concatenate(
                [src[o * SUB + r, pl.ds(last_y, 1), :] for r in range(SUB)], axis=0)
            out = None
            for t in range(N):
                if t % TILES == 0:
                    plane = widen(src[o * SUB + t // TILES])
                x = turn(plane[SUB * (t % TILES):SUB * (t % TILES) + SUB], t - last_z)
                out = x if t == 0 else pick(lane == t, x, out)
            lane_s[n, o] = out
        return carry
    lax.fori_loop(0, TILES, pack_one, 0)
    one_y = send(2, row_s, row_r, (0, 1, 0))
    one_z = send(3, lane_s, lane_r, (0, 0, 1))
    k_y = send(4, k_in.at[:, pl.ds(near_y, SUB), :], ky, (0, 1, 0))
    pack(k_in, zs.at[0], ds_.at[0])
    k_z = send(PIECES, zs.at[0], zr.at[0], (0, 0, 1))
    k_d = send(6, ds_.at[0], dr.at[0], (0, 1, 1))

    for n in (3, 4, PIECES):
        loads[n].wait()

    def lane_ring(w, at, c):
        left, right = walls[w, pl.ds(at, SUB), 0:LANES], walls[w, pl.ds(at, SUB), LANES:144]
        gap = jnp.zeros((SUB, 56), F32)
        right = jnp.concatenate([gap, right, gap], axis=1)
        turned = jnp.where(jnp.logical_and(lane >= 56, lane < N), right, pltpu.roll(left, 56, 1))
        return jnp.where(c == 0, left, turned)

    for jt in range(NB):
        at_j = pl.multiple_of(N * cy + SUB * jt if jt < TILES else N - H * cy, SUB)
        at_i = pl.multiple_of(N * cx + SUB * jt if jt < TILES else N - H * cx, SUB)
        k_nat[E, pl.ds(SUB * jt, SUB), :] = lane_ring(0, at_j, cz)
        wy[pl.ds(SUB * jt, SUB), :] = lane_ring(1, at_i, cz)
        if jt < TILES:
            wz[pl.ds(SUB * jt, SUB), :] = lane_ring(2, at_i, cy)
    wz_t[...] = wz[...].T

    loads[2].wait()

    def take_f(p, carry):
        for b in range(NB):
            rows = SUB if b < 2 else LAST
            v0_a[p, b, 0:rows, 0:N] = f_in[p, pl.ds(b, rows, stride=NB), :]
        return carry
    planes(0, N, take_f, 0)

    u_nat[E - 1 - LAST * cx] = jnp.zeros((E, LANES), F32)
    one_lane = N + 55 * cz
    at_one = lane == one_lane
    for copy in one_x + [one_y, one_z]:
        copy.wait()
    u_nat[N + LAST * cx, 0:N, 0:N] = ux[0]
    k_nat[E + 1, 0:N, 0:N] = kx[0]

    def unpack_one(o, carry):
        lanes_in = [lane_r[n, o] for n in range(2)]
        for pi in range(SUB):
            i = o * SUB + pi
            planes_in = [widen(k_in[i]), widen(u_in[i])]
            for n, nat in enumerate((k_nat, u_nat)):
                out = []
                for jt in range(TILES):
                    other = zero if n else pick(at_wall, wall_column(i, jt), ones)
                    other = pick(at_one, turn(lanes_in[n], one_lane - (pi * TILES + jt)), other)
                    out.append(pick(own_lane, planes_in[n][SUB * jt:SUB * jt + SUB], other))
                nat[i, 0:N, :] = jnp.concatenate(out, axis=0)
        return carry
    lax.fori_loop(0, TILES, unpack_one, 0)

    row0 = sub == 0
    row72 = sub == LAST

    def divergence(h_x, h_xn, h_y, h_z, v, v_prev, v_next, low_row, high_row):
        low = row_down(v)
        high = v
        if low_row is not None:
            low = replace(low, 0, row0, low_row)
            high = replace(v, 2, row72, high_row)
        else:
            low = replace(low, 0, jnp.logical_and(row0, cy == 0), ZERO)
            high = replace(v, 2, jnp.logical_and(row72, cy == 1), ZERO)
        f_y = h_y * (high - low)
        f_z = h_z * (v - lane_down(v))
        return ((h_x * (v - v_prev) - h_xn * (v_next - v)) + (f_y - row_up(f_y))) + (f_z - lane_up(f_z))

    def full(row):
        return jnp.broadcast_to(widen(row), (SUB, LANES))

    def add_up(h_x, h_xn, h_y, h_z):
        return ((h_x + h_xn) + (h_y + row_up(h_y))) + (h_z + lane_up(h_z))

    def start_own(n, carry):
        p0 = WIDTH * n
        first_trip, last_trip = n == 0, n == N // WIDTH - 1
        k_p = [load_chunk(k_nat, jnp.where(first_trip, E + cx, p0 - 1))]
        u_p = [load_chunk(u_nat, jnp.where(first_trip, E - 1, p0 - 1))]
        for w in range(WIDTH):
            k_p.append(load_chunk(k_nat, p0 + w))
            u_p.append(load_chunk(u_nat, p0 + w))
        k_p.append(load_chunk(k_nat, jnp.where(last_trip, E + 1 - cx, p0 + WIDTH)))
        u_p.append(load_chunk(u_nat, p0 + WIDTH))
        h_x = [harmonic(k_p[w + 1], k_p[w]) for w in range(WIDTH + 1)]
        for w in range(WIDTH):
            p, kc = p0 + w, k_p[w + 1]
            wall, got = full(wy[pl.ds(p, 1), :]), full(row_r[0, pl.ds(p, 1), :])
            low = replace(row_down(kc), 0, row0, jnp.where(cy == 0, wall, got))
            high = replace(kc, 2, row72, jnp.where(cy == 0, got, wall))
            h_y = harmonic(high, low)
            h_z = harmonic(kc, lane_down(kc))
            inv = lax.rsqrt(add_up(h_x[w], h_x[w + 1], h_y, h_z))
            got = full(row_r[1, pl.ds(p, 1), :])
            a_u = divergence(h_x[w], h_x[w + 1], h_y, h_z, u_p[w + 1], u_p[w], u_p[w + 2],
                             jnp.where(cy == 0, ZERO, got), jnp.where(cy == 0, got, ZERO))
            y0 = (v0_a[p] - a_u) * inv
            v0_a[p] = y0
            z0 = y0 * inv
            for b in range(NB):
                if b < 2:
                    z_nat[p, pl.ds(b, SUB, stride=NB), :] = z0[b]
                else:
                    z_nat[p, pl.ds(b, LAST, stride=NB), :] = z0[b, :LAST]
        return carry
    lax.fori_loop(0, N // WIDTH, start_own, 0)

    z_y = send(LAST, z_nat.at[pl.ds(0, N), pl.ds(near_y, SUB), :], z_nat.at[pl.ds(0, N), pl.ds(N, SUB), :], (0, 1, 0))
    pack(z_nat, zs.at[1], ds_.at[1])
    z_z = send(8, zs.at[1], zr.at[1], (0, 0, 1))
    z_d = send(9, ds_.at[1], dr.at[1], (0, 1, 1))

    def spread(n, nat, take):
        take(SUB * (1 - cx), 0)
        copy = send(n, nat.at[pl.ds(near_x, SUB)], nat.at[pl.ds(N, SUB)], (1, 0, 0))
        lax.fori_loop(0, SUB, lambda o, carry: take(o + cx, carry), 0)
        return copy

    for copy in (k_y, k_z, k_d):
        copy.wait()
    spread(NB, k_nat, functools.partial(unpack, k_in, ky, k_nat, zr.at[0], dr.at[0], ones, wz_t)).wait()

    def faces(p, carry):
        kc = load_chunk(k_nat, p)
        before = jnp.where(jnp.logical_and(p == 0, cx == 0), E, jnp.where(p == 0, E - 1, p - 1))
        here = jnp.where(jnp.logical_and(p == N, cx == 1), E, p)
        cx_a[p] = harmonic(load_chunk(k_nat, here), load_chunk(k_nat, before))
        wall = full(wy[pl.ds(p, 1), :])
        low = replace(row_down(kc), 0, jnp.logical_and(row0, cy == 0), wall)
        high = replace(kc, 2, jnp.logical_and(row72, cy == 1), wall)
        cy_a[p] = harmonic(high, low)
        cz_a[p] = harmonic(kc, lane_down(kc))
        return carry
    planes(0, E, faces, 0)
    cx_a[E] = cx_a[0]
    cx_a[E + 1] = cx_a[1]

    def scales(own, p, carry):
        d = add_up(cx_a[p], cx_a[p + 1], cy_a[p], cz_a[p])
        inv = lax.rsqrt(d)
        isd_a[p] = inv
        if own:
            sd = d * inv
            for b in range(NB):
                k_nat[p, pl.ds(SUB * b, SUB), :] = sd[b]
        return carry
    planes(0, N, functools.partial(scales, True), 0)
    planes(N, E, functools.partial(scales, False), 0)

    for copy in (z_y, z_z, z_d):
        copy.wait()
    z_x = spread(11, z_nat, functools.partial(unpack, z_nat, z_nat.at[:, pl.ds(N, SUB), :], z_nat, zr.at[1], dr.at[1],
                                              zero, None))

    def first(own, p, carry):
        static = isinstance(p, int)
        before = (p - 1) % E if static else p - 1
        after = p + 1 if static else lax.rem(p + 1, E)
        h_x, h_xn, h_y, h_z, inv = cx_a[p], cx_a[E + 1 if static and p == 0 else p + 1], cy_a[p], cz_a[p], isd_a[p]
        z_p = jnp.where(jnp.logical_and(p == 0, cx == 0), ZERO, load_chunk(z_nat, before))
        z_n = jnp.where(jnp.logical_and(p == N - 1, cx == 1), ZERO, load_chunk(z_nat, after))
        b0 = inv * divergence(h_x, h_xn, h_y, h_z, load_chunk(z_nat, p), z_p, z_n, None, None)
        b_a[0][p + 1] = b0
        cut = jnp.logical_or(jnp.logical_and(p == 0, cx == 0), jnp.logical_and(p == N, cx == 1))
        twice = TWO * inv
        cx_a[p] = jnp.where(cut, ZERO, h_x * (twice * isd_a[before]))
        c_y = h_y * (twice * row_down(inv))
        c_y = replace(c_y, 0, jnp.logical_and(row0, cy == 0), ZERO)
        cy_a[p] = replace(c_y, 2, jnp.logical_and(row72, cy == 1), ZERO)
        c_z = h_z * (twice * lane_down(inv))
        edge = N * cz
        cz_a[p] = jnp.where(lax.broadcasted_iota(jnp.int32, (NB, SUB, LANES), 2) == edge, ZERO, c_z)
        if not own:
            return carry
        v0 = v0_a[p]
        new = dot_pair(v0, v0) + dot_pair(v0, b0) + dot_pair(b0, b0)
        return tuple(c + n for c, n in zip(carry, new))


    def wrap(ref):
        ref[0] = ref[E]
        ref[E + 1] = ref[1]
    sums = planes(1, N - 1, functools.partial(first, True), (zero,) * 6, PIECES)
    z_x.wait()
    for p in (0, N - 1):
        sums = first(True, p, sums)
    planes(N, E, functools.partial(first, False), 0)
    cx_a[E] = cx_a[0]
    wrap(b_a[0])
    acc[0] = own_cells(sums[0], sums[1])
    acc[1] = own_cells(sums[2], sums[3])
    acc[TILES] = own_cells(sums[4], sums[PIECES])
    acc[23] = zero

    def advance(k, own, p, carry):
        old, here = b_a[k - 1], p + 1
        v = old[here]
        c_y, c_z = cy_a[p], cz_a[p]
        new = cx_a[p] * old[here - 1] + cx_a[p + 1] * old[here + 1]
        new = new + (c_y * row_down(v) + row_up(c_y * v))
        new = new + (c_z * lane_down(v) + lane_up(c_z * v))
        new = HALF * new if k == 1 else new - b_a[k - 2][here]
        b_a[k][here] = new
        if not own:
            return carry
        dots = dot_pair(v0_a[p], new) + dot_pair(v, new) + dot_pair(new, new)
        return tuple(c + n for c, n in zip(carry, dots))

    for k in range(1, STEPS):
        sums = planes(0, N, functools.partial(advance, k, True), (zero,) * 6)
        if k < STEPS - 1:
            planes(N, E, functools.partial(advance, k, False), 0)
            wrap(b_a[k])
        acc[1 + k] = own_cells(sums[0], sums[1])
        acc[GROUPS + k - 1] = own_cells(sums[2], sums[3])
        if k < STEPS - 1:
            acc[TILES + k] = own_cells(sums[4], sums[PIECES])

    def gather(buf, n_sem):
        copies = []
        for n, flips in enumerate(OTHERS):
            copies.append(pltpu.make_async_remote_copy(
                src_ref=buf.at[me], dst_ref=buf.at[me], send_sem=all_send.at[n_sem, n], recv_sem=all_recv.at[n_sem, n],
                device_id=peer(*flips), device_id_type=MESH))
        for copy in copies:
            copy.start()
        return copies

    hi = acc[:, 0, :]
    lo = jnp.zeros((NDOT, LANES), F32)
    for s in range(1, SUB):
        hi, err = two_sum(hi, acc[:, s, :])
        lo = lo + err
    gath[me, 0:NDOT] = hi
    gath[me, NDOT:2 * NDOT] = lo
    for copy in gather(gath, 0):
        copy.wait()
    hi, lo = gath[0, 0:NDOT], gath[0, NDOT:2 * NDOT]
    for dev in range(1, SUB):
        hi, err = two_sum(hi, gath[dev, 0:NDOT])
        lo = lo + (gath[dev, NDOT:2 * NDOT] + err)
    for shift in (64, 32, GROUPS, SUB, 4, 2, 1):
        hi, err = two_sum(hi, pltpu.roll(hi, shift, 1))
        lo = (lo + pltpu.roll(lo, shift, 1)) + err
    hi, lo = quick(hi, lo)
    size = hi[0:1]
    factor = jnp.where(size > 1e30, TWO ** -110, jnp.where(size > 1e12, TWO ** -60, jnp.where(
        size < 1e-30, TWO ** 110, jnp.where(size < 1e-12, TWO ** 60, ONE)))).astype(F32)
    hi, lo = hi * factor, lo * factor

    def total(row):
        return jnp.broadcast_to(hi[row:row + 1], (SUB, LANES)), jnp.broadcast_to(lo[row:row + 1], (SUB, LANES))

    n_mom = [total(TILES), total(GROUPS)]
    for j in range(1, LAST):
        n_mom.append(dsub(dscale(total(TILES + j), TWO), n_mom[0]))
        n_mom.append(dsub(dscale(total(GROUPS + j), TWO), n_mom[1]))
    l_mom = [total(1 + j) for j in range(SUB)]
    for j in range(LAST, 14):
        l_mom.append(dsub(dscale(dsub(l_mom[j], n_mom[j]), TWO), l_mom[j - 1]))
    m_mom = [total(0)]
    m_mom.append(dsub(m_mom[0], l_mom[0]))
    for j in range(1, 15):
        m_mom.append(dsub(dscale(dsub(m_mom[j], l_mom[j]), TWO), m_mom[j - 1]))
    ys, xs = basis_coefs(*step_lengths(m_mom))
    slot = {}
    for t in range(STEPS):
        for j in range(t + 1):
            slot[t, j] = len(slot)
            coef[slot[t, j]] = ys[t][1 + j]
    for j in range(SUB):
        slot['x', j] = len(slot)
        coef[slot['x', j]] = xs[j]

    def put(ref, p, b0, val):
        for b in range(val.shape[0]):
            if b0 + b < 2:
                ref[p, pl.ds(b0 + b, SUB, stride=NB), :] = val[b, :, :N]
            else:
                ref[p, pl.ds(b0 + b, LAST, stride=NB), :] = val[b, :LAST, :N]

    def residuals(p, carry):
        carry = list(carry)
        for b0 in range(0, NB, 2):
            cut = pl.ds(b0, 2)
            v0 = v0_a[p, cut]
            sd = jnp.stack([k_nat[p, pl.ds(SUB * (b0 + b), SUB), :] for b in range(2)], axis=0)
            bs = [ref[p + 1, cut] for ref in b_a]
            for t in range(STEPS):
                y = v0
                for j in range(t + 1):
                    y = y + coef[slot[t, j]] * bs[j]
                r = sd * y
                which = 2 * t + (b0 > 0)
                carry[which] = carry[which] + jnp.sum(r * r, axis=0)
                if t == STEPS - 1:
                    put(f_in, p, b0, r)
        return tuple(carry)

    outs = []

    def flush(n, nat, hbm, o):
        outs.append(pltpu.make_async_copy(nat.at[pl.ds(PART * o, PART)], hbm.at[pl.ds(PART * o, PART)],
                                          out_sem.at[n, o]))
        outs[-1].start()

    sums = (zero,) * GROUPS
    for o in range(3):
        sums = lax.fori_loop(PART * o, PART * o + PART, residuals, sums)
        flush(0, f_in, ro_hbm, o)
    for t in range(STEPS):
        rsend[t] = own_cells(sums[2 * t], sums[2 * t + 1])
    part = rsend[:, 0, :]
    for s in range(1, SUB):
        part = part + rsend[:, s, :]
    rgath[me] = part
    rr_copies = gather(rgath, 1)

    def update(p, carry):
        for b0 in range(0, NB, 2):
            cut = pl.ds(b0, 2)
            x = coef[slot['x', 0]] * v0_a[p, cut]
            for j in range(1, SUB):
                x = x + coef[slot['x', j]] * b_a[j - 1][p + 1, cut]
            x = x * isd_a[p, cut]
            u = jnp.stack([u_nat[p, pl.ds(b0 + b, SUB, stride=NB), :] for b in range(2)], axis=0)
            put(k_in, p, b0, u + x)
        return carry

    for o in range(3):
        lax.fori_loop(PART * o, PART * o + PART, update, 0)
        flush(1, k_in, uo_hbm, o)
    for copy in rr_copies:
        copy.wait()
    part = rgath[0]
    for dev in range(1, SUB):
        part = part + rgath[dev]
    part = jnp.broadcast_to(jnp.sum(part, axis=1, keepdims=True), (SUB, LANES))
    rr_ref[...] = jnp.sum(jnp.where(lane == sub, part, ZERO), axis=0, keepdims=True)[:, :STEPS]
    for copy in outs:
        copy.wait()


def solution(mesh):
    spec = P('gx', 'gy', 'gz')

    def local(k_cell, k_ghost, f_rhs, u_init):
        big = (E, NB, SUB, LANES)
        ext = (E + 2, NB, SUB, LANES)
        vm = lambda *shape: pltpu.VMEM(shape, F32)
        any_spec = pl.BlockSpec(memory_space=pl.ANY)
        block = jax.ShapeDtypeStruct((N, N, N), F32)
        u, r, rr = pl.pallas_call(
            kernel,
            out_shape=(block, block, jax.ShapeDtypeStruct((1, STEPS), F32)),
            in_specs=[any_spec] * 4,
            out_specs=(any_spec, any_spec, pl.BlockSpec(memory_space=pltpu.VMEM)),
            scratch_shapes=[
                vm(N, N, N), vm(N, N, N), vm(N, N, N), vm(E + 2, E, LANES), vm(E, E, LANES), vm(E, E, LANES),
                vm(*ext), vm(*big), vm(*big), vm(*big), vm(N, NB, SUB, LANES),
                *[vm(E + 2, NB, SUB, LANES)] * STEPS,
                vm(3, 144, 144), vm(LANES, LANES), vm(LANES, LANES), vm(E, LANES), vm(N, SUB, N), vm(1, N, N), vm(1, N, N),
                vm(2, 45, SUB, LANES), vm(2, 45, SUB, LANES), vm(2, TILES, SUB, LANES), vm(2, TILES, SUB, LANES),
                vm(2, N, N), vm(2, N, N), vm(2, TILES, SUB, LANES), vm(2, TILES, SUB, LANES),
                vm(NDOT, SUB, LANES), vm(SUB, 2 * NDOT, LANES), vm(SUB, SUB, LANES), vm(SUB, SUB, LANES), vm(44, SUB, LANES),
                pltpu.SemaphoreType.DMA((6,)), pltpu.SemaphoreType.DMA((2, 3)),
                pltpu.SemaphoreType.DMA((12,)), pltpu.SemaphoreType.DMA((12,)),
                pltpu.SemaphoreType.DMA((2, LAST)), pltpu.SemaphoreType.DMA((2, LAST)),
            ],
            compiler_params=pltpu.CompilerParams(collective_id=0, has_side_effects=True, vmem_limit_bytes=67043328),
        )(k_cell, f_rhs, u_init, k_ghost)
        return u, r, rr.reshape(STEPS)

    return jax.shard_map(local, mesh=mesh, in_specs=(spec, P(), spec, spec), out_specs=(spec, spec, P()), check_vma=False)
```

```python
import functools

import jax
import jax.numpy as jnp
from jax import lax
from jax.experimental import pallas as pl
from jax.experimental.pallas import tpu as pltpu
from jax.sharding import PartitionSpec as P


N = 72
H = 8
E = N + H
NB = 10
STEPS = 8
MESH = pl.DeviceIdType.MESH
F32 = jnp.float32
OTHERS = [(fx, fy, fz) for fx in (0, 1) for fy in (0, 1) for fz in (0, 1) if fx or fy or fz]
NDOT = 24
SUB = 8
LANES = 128
TILES = 9
PART = 24
WIDTH = 4
LAST = 7
GROUPS = 16
PIECES = 5
ZERO, ONE, HALF, TWO = 0.0, 1.0, 0.5, 2.0
UNIT = 1


def iota(axis):
    return lax.broadcasted_iota(jnp.int32, (SUB, LANES), axis)


def two_sum(a, b):
    s = a + b
    t = s - a
    return s, (a - (s - t)) + (b - t)


def quick(a, b):
    s = a + b
    return s, b - (s - a)


def two_prod(a, b):
    def split(x):
        t = x * 4097.0
        hi = t - (t - x)
        return hi, x - hi
    p = a * b
    ah, al = split(a)
    bh, bl = split(b)
    return p, ((ah * bh - p) + ah * bl + al * bh) + al * bl


def dadd(x, y):
    (xh, xl), (yh, yl) = x, y
    s, e = two_sum(xh, yh)
    return quick(s, e + (xl + yl))


def dsub(x, y):
    yh, yl = y
    return dadd(x, (-yh, -yl))


def dscale(x, c):
    hi, lo = x
    return hi * c, lo * c


def dmul(x, y):
    (xh, xl), (yh, yl) = x, y
    p, e = two_prod(xh, yh)
    return quick(p, e + (xh * yl + xl * yh))


def ddiv(x, y):
    (xh, xl), (yh, yl) = x, y
    q = xh / yh
    p, e = two_prod(q, yh)
    rest = ((xh - p) - e) + (xl - q * yl)
    return quick(q, rest / yh)


def step_lengths(m):
    alphas, betas = [], []
    y = dict(enumerate(m))
    p = {0: dsub(y[0], y[1])}
    for l in range(1, 15):
        p[l] = dsub(y[l], dscale(dadd(y[l + UNIT], y[l - UNIT]), HALF))
    for t in range(STEPS):
        alpha = ddiv(y[t], p[t])
        alphas.append(alpha[0])
        if t == STEPS - UNIT:
            break
        y_next = {l: dsub(y[l], dmul(alpha, p[l])) for l in range(t + UNIT, 15 - t)}
        beta = ddiv(y_next[t + UNIT], p[t])
        if t:
            beta = dscale(beta, HALF)
        betas.append(beta[0])
        p_next = {}
        for l in range(t + UNIT, 14 - t):
            side = y_next[l + UNIT] if l == t + UNIT else dadd(y_next[l + UNIT], y_next[l - UNIT])
            p_next[l] = dadd(dsub(y_next[l], dscale(side, HALF)), dmul(beta, p[l]))
        y, p = y_next, p_next
    return alphas, betas


def basis_coefs(alphas, betas):
    def add(a, b):
        return b if a is None else (a if b is None else a + b)

    def axpy(x, c, y):
        return [xi if yi is None else (c * yi if xi is None else xi + c * yi) for xi, yi in zip(x, y)]

    def apply_op(v):
        out = [None] * 11
        out[1] = v[0]
        for j in range(SUB):
            if v[1 + j] is None:
                continue
            c = v[1 + j]
            out[1 + j] = add(out[1 + j], c)
            if j == 0:
                out[2] = add(out[2], -c)
            else:
                half = -HALF * c
                out[2 + j] = add(out[2 + j], half)
                out[j] = add(out[j], half)
        return out[:TILES]

    one = jnp.ones_like(alphas[0])
    y = [one] + [None] * SUB
    p = list(y)
    x = [None] * TILES
    ys = []
    for t in range(STEPS):
        q = apply_op(p)
        x = axpy(x, alphas[t], p)
        y = axpy(y, -alphas[t], q)
        ys.append(y)
        if t < STEPS - UNIT:
            p = axpy(y, betas[t], p)
    return ys, x


def row_down(v):
    return jnp.concatenate([pltpu.roll(v[NB - UNIT], 1, 0)[None], v[:NB - UNIT]], axis=0)


def row_up(v):
    return jnp.concatenate([v[1:], pltpu.roll(v[0], LAST, 0)[None]], axis=0)


def lane_down(v):
    return pltpu.roll(v, 1, 2)


def lane_up(v):
    return pltpu.roll(v, 127, 2)


def load_chunk(ref, plane):
    return jnp.stack([ref[plane, pl.ds(b, SUB, stride=NB), :] for b in range(NB)], axis=0)


def replace(v, b, mask, value):
    return jnp.concatenate(([v[:b]] if b else []) + [jnp.where(mask, value, v[b])[None], v[b + UNIT:]], axis=0)


def harmonic(a, b):
    return TWO * a * b / (a + b)


def pick(mask, a, b):
    return lax.select_n(mask, b, a)


def planes(lo, hi, body, init, width=WIDTH):
    def some(n, carry):
        for w in range(width):
            carry = body(lo + n * width + w, carry)
        return carry
    return lax.fori_loop(0, (hi - lo) // width, some, init)


def own_cells(low, high):
    sub, lane = iota(0), iota(1)
    return jnp.where(lane < N, low + jnp.where(sub < LAST, high, ZERO), ZERO)


def kernel(k_hbm, f_hbm, u_hbm, kg_hbm, uo_hbm, ro_hbm, rr_ref,
           k_in, u_in, f_in, k_nat, u_nat, z_nat, cx_a, cy_a, cz_a, isd_a, v0_a, b0_a, b1_a, b2_a, b3_a, b4_a, b5_a, b6_a, b7_a,
           walls, wz, wz_t, wy, ky, kx, ux, zs, zr, ds_, dr, row_s, row_r, lane_s, lane_r, acc, gath, rsend, rgath, coef,
           load_sem, out_sem, send_sem, recv_sem, all_send, all_recv):
    cx, cy, cz = lax.axis_index('gx'), lax.axis_index('gy'), lax.axis_index('gz')
    me = cx + 2 * cy + 4 * cz
    b_a = (b0_a, b1_a, b2_a, b3_a, b4_a, b5_a, b6_a, b7_a)
    lane, sub = iota(1), iota(0)

    def peer(fx, fy, fz):
        out = {}
        if fx:
            out['gx'] = 1 - cx
        if fy:
            out['gy'] = 1 - cy
        if fz:
            out['gz'] = 1 - cz
        return out

    loads = []
    for n, (src, dst) in enumerate([(k_hbm, k_in), (u_hbm, u_in), (f_hbm, f_in)]):
        loads.append([pltpu.make_async_copy(src.at[pl.ds(PART * q, PART)], dst.at[pl.ds(PART * q, PART)], load_sem.at[n, q])
                      for q in range(N // PART)])
    loads.append([pltpu.make_async_copy(kg_hbm.at[cx], walls.at[0], load_sem.at[3, 0])])
    loads.append([pltpu.make_async_copy(kg_hbm.at[2 + cy], walls.at[1], load_sem.at[4, 0])])
    loads.append([pltpu.make_async_copy(kg_hbm.at[4 + cz], walls.at[2], load_sem.at[PIECES, 0])])
    for n in (0, 1, 3, 4, PIECES, 2):
        for copy in loads[n]:
            copy.start()

    barrier = pltpu.get_barrier_semaphore()
    for flips in OTHERS:
        pl.semaphore_signal(barrier, inc=1, device_id=peer(*flips), device_id_type=MESH)
    pl.semaphore_wait(barrier, len(OTHERS))

    def send(n, src, dst, flips):
        copy = pltpu.make_async_remote_copy(src_ref=src, dst_ref=dst, send_sem=send_sem.at[n], recv_sem=recv_sem.at[n],
                                            device_id=peer(*flips), device_id_type=MESH)
        copy.start()
        return copy

    near_y = pl.multiple_of((N - H) * (1 - cy), SUB)
    near_x = (N - H) * (1 - cx)
    src8 = (N - H) * (1 - cz)
    dst8 = N + 48 * cz
    ghost8 = jnp.logical_and(lane >= dst8, lane < dst8 + SUB)
    wall_lane = 127 - 55 * cz
    own_lane = lane < N
    at_wall = lane == wall_lane
    zero = jnp.zeros((SUB, LANES), F32)
    ones = jnp.ones((SUB, LANES), F32)

    def turn(x, by):
        return pltpu.roll(x, lax.rem(by + LANES, LANES), 1)

    def shift(x, by):
        return pltpu.roll(x, by % LANES, 1) if by % LANES else x

    def widen(x):
        return x if x.shape[1] == LANES else jnp.concatenate([x, jnp.zeros((x.shape[0], LANES - x.shape[1]), F32)], axis=1)

    def pack(nat, packed, corner):
        group8 = lax.rem(lane + (LANES - src8), LANES) // SUB
        groups = [group8 == g for g in range(GROUPS)]

        def body(o, carry):
            for q in range(PIECES):
                out = None
                for g in range(min(GROUPS, N - GROUPS * q)):
                    t = GROUPS * q + g
                    if t % TILES == 0:
                        plane = widen(nat[o * SUB + t // TILES, 0:N, :])
                    x = shift(plane[SUB * (t % TILES):SUB * (t % TILES) + SUB], SUB * g)
                    out = x if g == 0 else pick(groups[g], x, out)
                packed[o * PIECES + q] = out
            out = None
            for g in range(SUB):
                x = widen(nat[o * SUB + g, pl.ds(near_y, SUB), :])
                x = shift(x, SUB * g)
                out = x if g == 0 else pick(groups[g], x, out)
            corner[o] = out
            return carry
        lax.fori_loop(0, TILES, body, 0)

    def unpack(own, side, nat, packed, corner, fill, wall, o, carry):
        by = dst8 - (N - H - src8)
        packs, corner_in = [turn(packed[o * PIECES + q], by) for q in range(PIECES)], turn(corner[o], by)
        for pi in range(SUB):
            i, out = o * SUB + pi, []
            plane = widen(own[i, 0:N, :])
            for jt in range(NB):
                if jt < TILES:
                    t = pi * TILES + jt
                    got, g = packs[t // GROUPS], t % GROUPS
                else:
                    got, g = corner_in, pi
                x = plane[SUB * jt:SUB * jt + SUB] if jt < TILES else widen(side[i])
                other = fill if wall is None else pick(at_wall, wall_column(i, jt), fill)
                out.append(pick(own_lane, x, pick(ghost8, shift(got, -SUB * g), other)))
            nat[i, 0:E, :] = jnp.concatenate(out, axis=0)
        return carry

    def wall_column(i, jt):
        at = SUB * jt if jt < TILES else pl.multiple_of(N + 48 * cy, SUB)
        return pltpu.roll(wz_t[pl.ds(at, SUB), :], LANES - UNIT - i, 1)

    for copy in loads[0] + loads[1]:
        copy.wait()
    last_x, last_y, last_z = (N - UNIT) * (1 - cx), (N - UNIT) * (1 - cy), (N - UNIT) * (1 - cz)
    one_x = [send(0, k_in.at[pl.ds(last_x, 1)], kx, (1, 0, 0)), send(1, u_in.at[pl.ds(last_x, 1)], ux, (1, 0, 0))]

    slots = lax.rem(lane + (LANES - last_z), LANES)

    def pack_one(o, carry):
        for n, src in enumerate((k_in, u_in)):
            row_s[n, pl.ds(pl.multiple_of(o * SUB, SUB), SUB), :] = jnp.concatenate(
                [src[o * SUB + r, pl.ds(last_y, 1), :] for r in range(SUB)], axis=0)
            out = None
            for t in range(N):
                if t % TILES == 0:
                    plane = widen(src[o * SUB + t // TILES])
                x = shift(plane[SUB * (t % TILES):SUB * (t % TILES) + SUB], t)
                out = x if t == 0 else pick(slots == t, x, out)
            lane_s[n, o] = out
        return carry
    lax.fori_loop(0, TILES, pack_one, 0)
    one_y = send(2, row_s, row_r, (0, 1, 0))
    one_z = send(3, lane_s, lane_r, (0, 0, 1))
    k_y = send(4, k_in.at[:, pl.ds(near_y, SUB), :], ky, (0, 1, 0))
    pack(k_in, zs.at[0], ds_.at[0])
    k_z = send(PIECES, zs.at[0], zr.at[0], (0, 0, 1))
    k_d = send(6, ds_.at[0], dr.at[0], (0, 1, 1))

    for n in (3, 4, PIECES):
        loads[n][0].wait()

    def lane_ring(w, at, c):
        left, right = walls[w, pl.ds(at, SUB), 0:LANES], walls[w, pl.ds(at, SUB), LANES:144]
        gap = jnp.zeros((SUB, 56), F32)
        right = jnp.concatenate([gap, right, gap], axis=1)
        turned = jnp.where(jnp.logical_and(lane >= 56, lane < N), right, pltpu.roll(left, 56, 1))
        return jnp.where(c == 0, left, turned)

    for jt in range(NB):
        at_j = pl.multiple_of(N * cy + SUB * jt if jt < TILES else N - H * cy, SUB)
        at_i = pl.multiple_of(N * cx + SUB * jt if jt < TILES else N - H * cx, SUB)
        k_nat[E, pl.ds(SUB * jt, SUB), :] = lane_ring(0, at_j, cz)
        wy[pl.ds(SUB * jt, SUB), :] = lane_ring(1, at_i, cz)
        if jt < TILES:
            wz[pl.ds(SUB * jt, SUB), :] = lane_ring(2, at_i, cy)
    wz_t[...] = turn(wz[...].T, wall_lane + UNIT)

    for copy in loads[2]:
        copy.wait()

    def take_f(p, carry):
        for b in range(NB):
            rows = SUB if b < 2 else LAST
            v0_a[p, b, 0:rows, 0:N] = f_in[p, pl.ds(b, rows, stride=NB), :]
        return carry
    planes(0, N, take_f, 0)

    u_nat[E - UNIT - LAST * cx] = jnp.zeros((E, LANES), F32)
    one_lane = N + 55 * cz
    at_one = lane == one_lane
    for copy in one_x + [one_y, one_z]:
        copy.wait()
    u_nat[N + LAST * cx, 0:N, 0:N] = ux[0]
    k_nat[E + UNIT, 0:N, 0:N] = kx[0]

    def unpack_one(o, carry):
        lanes_in = [turn(lane_r[n, o], one_lane - (N - UNIT - last_z)) for n in range(2)]
        for pi in range(SUB):
            i = o * SUB + pi
            planes_in = [widen(k_in[i]), widen(u_in[i])]
            for n, nat in enumerate((k_nat, u_nat)):
                out = []
                for jt in range(TILES):
                    other = zero if n else pick(at_wall, wall_column(i, jt), ones)
                    other = pick(at_one, shift(lanes_in[n], -(pi * TILES + jt)), other)
                    out.append(pick(own_lane, planes_in[n][SUB * jt:SUB * jt + SUB], other))
                nat[i, 0:N, :] = jnp.concatenate(out, axis=0)
        return carry
    lax.fori_loop(0, TILES, unpack_one, 0)

    row0 = sub == 0
    row72 = sub == LAST

    def divergence(h_x, h_xn, h_y, h_z, v, v_prev, v_next, low_row, high_row):
        low = row_down(v)
        high = v
        if low_row is not None:
            low = replace(low, 0, row0, low_row)
            high = replace(v, 2, row72, high_row)
        else:
            low = replace(low, 0, jnp.logical_and(row0, cy == 0), ZERO)
            high = replace(v, 2, jnp.logical_and(row72, cy == 1), ZERO)
        f_y = h_y * (high - low)
        f_z = h_z * (v - lane_down(v))
        return ((h_x * (v - v_prev) - h_xn * (v_next - v)) + (f_y - row_up(f_y))) + (f_z - lane_up(f_z))

    def full(row):
        return jnp.broadcast_to(widen(row), (SUB, LANES))

    def add_up(h_x, h_xn, h_y, h_z):
        return ((h_x + h_xn) + (h_y + row_up(h_y))) + (h_z + lane_up(h_z))

    def start_own(n, carry):
        p0 = WIDTH * n
        first_trip, last_trip = n == 0, n == N // WIDTH - UNIT
        k_p = [load_chunk(k_nat, jnp.where(first_trip, E + cx, p0 - UNIT))]
        u_p = [load_chunk(u_nat, jnp.where(first_trip, E - UNIT, p0 - UNIT))]
        for w in range(WIDTH):
            k_p.append(load_chunk(k_nat, p0 + w))
            u_p.append(load_chunk(u_nat, p0 + w))
        k_p.append(load_chunk(k_nat, jnp.where(last_trip, E + UNIT - cx, p0 + WIDTH)))
        u_p.append(load_chunk(u_nat, p0 + WIDTH))
        h_x = [harmonic(k_p[w + UNIT], k_p[w]) for w in range(WIDTH + UNIT)]
        for w in range(WIDTH):
            p, kc = p0 + w, k_p[w + UNIT]
            wall, got = full(wy[pl.ds(p, 1), :]), full(row_r[0, pl.ds(p, 1), :])
            low = replace(row_down(kc), 0, row0, jnp.where(cy == 0, wall, got))
            high = replace(kc, 2, row72, jnp.where(cy == 0, got, wall))
            h_y = harmonic(high, low)
            h_z = harmonic(kc, lane_down(kc))
            inv = lax.rsqrt(add_up(h_x[w], h_x[w + UNIT], h_y, h_z))
            got = full(row_r[1, pl.ds(p, 1), :])
            a_u = divergence(h_x[w], h_x[w + UNIT], h_y, h_z, u_p[w + UNIT], u_p[w], u_p[w + 2],
                             jnp.where(cy == 0, ZERO, got), jnp.where(cy == 0, got, ZERO))
            y0 = (v0_a[p] - a_u) * inv
            v0_a[p] = y0
            z0 = y0 * inv
            for b in range(NB):
                if b < 2:
                    z_nat[p, pl.ds(b, SUB, stride=NB), :] = z0[b]
                else:
                    z_nat[p, pl.ds(b, LAST, stride=NB), :] = z0[b, :LAST]
        return carry
    lax.fori_loop(0, N // WIDTH, start_own, 0)

    z_y = send(LAST, z_nat.at[pl.ds(0, N), pl.ds(near_y, SUB), :], z_nat.at[pl.ds(0, N), pl.ds(N, SUB), :], (0, 1, 0))
    pack(z_nat, zs.at[1], ds_.at[1])
    z_z = send(8, zs.at[1], zr.at[1], (0, 0, 1))
    z_d = send(9, ds_.at[1], dr.at[1], (0, 1, 1))

    def spread(n, nat, take):
        take(SUB * (1 - cx), 0)
        copy = send(n, nat.at[pl.ds(near_x, SUB)], nat.at[pl.ds(N, SUB)], (1, 0, 0))
        lax.fori_loop(0, SUB, lambda o, carry: take(o + cx, carry), 0)
        return copy

    for copy in (k_y, k_z, k_d):
        copy.wait()
    spread(NB, k_nat, functools.partial(unpack, k_in, ky, k_nat, zr.at[0], dr.at[0], ones, wz_t)).wait()

    def faces(p, carry):
        kc = load_chunk(k_nat, p)
        before = jnp.where(jnp.logical_and(p == 0, cx == 0), E, jnp.where(p == 0, E - UNIT, p - UNIT))
        here = jnp.where(jnp.logical_and(p == N, cx == 1), E, p)
        cx_a[p] = harmonic(load_chunk(k_nat, here), load_chunk(k_nat, before))
        wall = full(wy[pl.ds(p, 1), :])
        low = replace(row_down(kc), 0, jnp.logical_and(row0, cy == 0), wall)
        high = replace(kc, 2, jnp.logical_and(row72, cy == 1), wall)
        cy_a[p] = harmonic(high, low)
        cz_a[p] = harmonic(kc, lane_down(kc))
        return carry
    planes(0, E, faces, 0)
    cx_a[E] = cx_a[0]
    cx_a[E + UNIT] = cx_a[1]

    def scales(own, p, carry):
        d = add_up(cx_a[p], cx_a[p + UNIT], cy_a[p], cz_a[p])
        inv = lax.rsqrt(d)
        isd_a[p] = inv
        if own:
            sd = d * inv
            for b in range(NB):
                k_nat[p, pl.ds(SUB * b, SUB), :] = sd[b]
        return carry
    planes(0, N, functools.partial(scales, True), 0)
    planes(N, E, functools.partial(scales, False), 0)

    for copy in (z_y, z_z, z_d):
        copy.wait()
    z_x = spread(11, z_nat, functools.partial(unpack, z_nat, z_nat.at[:, pl.ds(N, SUB), :], z_nat, zr.at[1], dr.at[1],
                                              zero, None))

    def column(ref, p, b, width):
        return ref[pl.ds(p, width), b]

    def z_column(p, b, width=1):
        return z_nat[pl.ds(p, width), pl.ds(b, SUB, stride=NB), :]

    def tally(carry, b, products):
        return [c + jnp.sum(products[n // 2], axis=0) if n % 2 == (b > 1) else c for n, c in enumerate(carry)]

    def first(own, width, p, carry, before=None, after=None, x_after=None):
        before = p - UNIT if before is None else before
        z, inv, low, f_y, h_y = {}, {}, {}, {}, {}

        def load(b):
            z[b], inv[b], h_y[b] = z_column(p, b, width), column(isd_a, p, b, width), column(cy_a, p, b, width)
            under = z[b - UNIT] if b else pltpu.roll(z_column(p, NB - UNIT, width), 1, 1)
            over = z[b]
            if b == 0:
                under = jnp.where(jnp.logical_and(row0, cy == 0), ZERO, under)
            if b == 2:
                over = jnp.where(jnp.logical_and(row72, cy == 1), ZERO, over)
            f_y[b] = h_y[b] * (over - under)
        carry = list(carry)
        load(0)
        for b in range(NB):
            if b < NB - UNIT:
                load(b + UNIT)
            up = f_y[b + UNIT] if b < NB - UNIT else pltpu.roll(f_y[0], LAST, 1)
            z_p = z_column(before, b)
            z_n = z_column(p + width if after is None else after, b)
            if isinstance(p, int) and p == 0:
                z_p = jnp.where(cx == 0, ZERO, z_p)
            if isinstance(p, int) and p == N - UNIT:
                z_n = jnp.where(cx == 1, ZERO, z_n)
            if x_after is None:
                h_x = column(cx_a, p, b, width + UNIT)
            else:
                h_x = jnp.concatenate([column(cx_a, p, b, 1), column(cx_a, x_after, b, 1)], axis=0)
            f_x = h_x * (jnp.concatenate([z[b], z_n], axis=0) - jnp.concatenate([z_p, z[b]], axis=0))
            h_z = column(cz_a, p, b, width)
            f_z = h_z * (z[b] - lane_down(z[b]))
            b0 = inv[b] * (((f_x[:width] - f_x[1:]) + (f_y[b] - up)) + (f_z - lane_up(f_z)))
            b_a[0][pl.ds(p + UNIT, width), b] = b0
            twice = TWO * inv[b]
            side = column(isd_a, before, b, 1)
            if width > 1:
                side = jnp.concatenate([side, inv[b][:width - UNIT]], axis=0)
            cx_a[pl.ds(p, width), b] = h_x[:width] * (twice * side)
            side = inv[b - UNIT] if b else pltpu.roll(column(isd_a, p, NB - UNIT, width), 1, 1)
            c_y = h_y[b] * (twice * side)
            if b == 0:
                c_y = jnp.where(jnp.logical_and(row0, cy == 0), ZERO, c_y)
            if b == 2:
                c_y = jnp.where(jnp.logical_and(row72, cy == 1), ZERO, c_y)
            cy_a[pl.ds(p, width), b] = c_y
            cz_a[pl.ds(p, width), b] = jnp.where(at_edge, ZERO, h_z * (twice * lane_down(inv[b])))
            if own:
                v0 = column(v0_a, p, b, width)
                carry = tally(carry, b, (v0 * v0, v0 * b0, b0 * b0))
        return tuple(carry)

    at_edge = lane == N * cz

    def wrap(ref):
        ref[0] = ref[E]
        ref[E + UNIT] = ref[1]

    sums = lax.fori_loop(0, 14, lambda n, carry: first(True, PIECES, 1 + PIECES * n, carry), (zero,) * 6)
    z_x.wait()
    sums = first(True, 1, 0, sums, E - UNIT, None, E + UNIT)
    sums = first(True, 1, N - UNIT, sums)
    first(False, WIDTH, N, ())
    first(False, WIDTH, N + WIDTH, (), None, 0)
    cx_a[0] = jnp.where(cx == 0, ZERO, cx_a[0])
    cx_a[N] = jnp.where(cx == 1, ZERO, cx_a[N])
    cx_a[E] = cx_a[0]
    wrap(b_a[0])
    acc[0] = own_cells(sums[0], sums[1])
    acc[1] = own_cells(sums[2], sums[3])
    acc[TILES] = own_cells(sums[4], sums[PIECES])
    acc[23] = zero

    def advance(k, own, width, p, carry):
        old, carry = b_a[k - UNIT], list(carry)
        v_low = pltpu.roll(column(old, p + UNIT, NB - UNIT, width), 1, 1)
        v, c_y = column(old, p + UNIT, 0, width), column(cy_a, p, 0, width)
        t_first = c_y * v
        for b in range(NB):
            if b < NB - UNIT:
                v_high, c_high = column(old, p + UNIT, b + UNIT, width), column(cy_a, p, b + UNIT, width)
                t_high = c_high * v_high
            else:
                t_high = pltpu.roll(t_first, LAST, 1)
            c_x, c_z = column(cx_a, p, b, width + UNIT), column(cz_a, p, b, width)
            below, above = column(old, p, b, 1), column(old, p + width + UNIT, b, 1)
            if width > 1:
                below = jnp.concatenate([below, v[:width - UNIT]], axis=0)
                above = jnp.concatenate([v[1:], above], axis=0)
            new = c_x[:width] * below + c_x[1:] * above
            new = new + (c_y * v_low + t_high)
            new = new + (c_z * lane_down(v) + lane_up(c_z * v))
            new = HALF * new if k == 1 else new - column(b_a[k - 2], p + UNIT, b, width)
            b_a[k][pl.ds(p + UNIT, width), b] = new
            if own:
                carry = tally(carry, b, (column(v0_a, p, b, width) * new, v * new, new * new))
            v_low, v, c_y = v, v_high, c_high
        return tuple(carry)

    for k in range(1, STEPS):
        sums = lax.fori_loop(0, N // WIDTH, lambda n, carry: advance(k, True, WIDTH, WIDTH * n, carry), (zero,) * 6)
        if k < STEPS - UNIT:
            lax.fori_loop(0, 2, lambda n, carry: advance(k, False, WIDTH, N + WIDTH * n, carry), ())
            wrap(b_a[k])
        acc[1 + k] = own_cells(sums[0], sums[1])
        acc[GROUPS + k - UNIT] = own_cells(sums[2], sums[3])
        if k < STEPS - UNIT:
            acc[TILES + k] = own_cells(sums[4], sums[PIECES])

    def gather(buf, n_sem):
        copies = []
        for n, flips in enumerate(OTHERS):
            copies.append(pltpu.make_async_remote_copy(
                src_ref=buf.at[me], dst_ref=buf.at[me], send_sem=all_send.at[n_sem, n], recv_sem=all_recv.at[n_sem, n],
                device_id=peer(*flips), device_id_type=MESH))
        for copy in copies:
            copy.start()
        return copies

    hi = acc[:, 0, :]
    lo = jnp.zeros((NDOT, LANES), F32)
    for s in range(1, SUB):
        hi, err = two_sum(hi, acc[:, s, :])
        lo = lo + err
    gath[me, 0:NDOT] = hi
    gath[me, NDOT:2 * NDOT] = lo
    for copy in gather(gath, 0):
        copy.wait()
    hi, lo = gath[0, 0:NDOT], gath[0, NDOT:2 * NDOT]
    for dev in range(1, SUB):
        hi, err = two_sum(hi, gath[dev, 0:NDOT])
        lo = lo + (gath[dev, NDOT:2 * NDOT] + err)
    for shift in (64, 32, GROUPS, SUB, 4, 2, 1):
        hi, err = two_sum(hi, pltpu.roll(hi, shift, 1))
        lo = (lo + pltpu.roll(lo, shift, 1)) + err
    hi, lo = quick(hi, lo)
    size = hi[0:1]
    factor = jnp.where(size > 1e30, TWO ** -110, jnp.where(size > 1e12, TWO ** -60, jnp.where(
        size < 1e-30, TWO ** 110, jnp.where(size < 1e-12, TWO ** 60, ONE)))).astype(F32)
    hi, lo = hi * factor, lo * factor

    def total(row):
        return jnp.broadcast_to(hi[row:row + UNIT], (SUB, LANES)), jnp.broadcast_to(lo[row:row + UNIT], (SUB, LANES))

    n_mom = [total(TILES), total(GROUPS)]
    for j in range(1, LAST):
        n_mom.append(dsub(dscale(total(TILES + j), TWO), n_mom[0]))
        n_mom.append(dsub(dscale(total(GROUPS + j), TWO), n_mom[1]))
    l_mom = [total(1 + j) for j in range(SUB)]
    for j in range(LAST, 14):
        l_mom.append(dsub(dscale(dsub(l_mom[j], n_mom[j]), TWO), l_mom[j - UNIT]))
    m_mom = [total(0)]
    m_mom.append(dsub(m_mom[0], l_mom[0]))
    for j in range(1, 15):
        m_mom.append(dsub(dscale(dsub(m_mom[j], l_mom[j]), TWO), m_mom[j - UNIT]))
    ys, xs = basis_coefs(*step_lengths(m_mom))
    slot = {}
    for t in range(STEPS):
        for j in range(t + UNIT):
            slot[t, j] = len(slot)
            coef[slot[t, j]] = ys[t][1 + j]
    for j in range(SUB):
        slot['x', j] = len(slot)
        coef[slot['x', j]] = xs[j]

    def put(ref, p, b0, val):
        for b in range(val.shape[0]):
            if b0 + b < 2:
                ref[p, pl.ds(b0 + b, SUB, stride=NB), :] = val[b, :, :N]
            else:
                ref[p, pl.ds(b0 + b, LAST, stride=NB), :] = val[b, :LAST, :N]

    def residuals(p, carry):
        carry = list(carry)
        for b0 in range(0, NB, 2):
            cut = pl.ds(b0, 2)
            v0 = v0_a[p, cut]
            sd = jnp.stack([k_nat[p, pl.ds(SUB * (b0 + b), SUB), :] for b in range(2)], axis=0)
            bs = [ref[p + UNIT, cut] for ref in b_a]
            for t in range(STEPS):
                y = v0
                for j in range(t + UNIT):
                    y = y + coef[slot[t, j]] * bs[j]
                r = sd * y
                which = 2 * t + (b0 > 0)
                carry[which] = carry[which] + jnp.sum(r * r, axis=0)
                if t == STEPS - UNIT:
                    put(f_in, p, b0, r)
        return tuple(carry)

    outs = []

    def flush(n, nat, hbm, o):
        outs.append(pltpu.make_async_copy(nat.at[pl.ds(PART * o, PART)], hbm.at[pl.ds(PART * o, PART)],
                                          out_sem.at[n, o]))
        outs[-1].start()

    sums = (zero,) * GROUPS
    for o in range(3):
        sums = lax.fori_loop(PART * o, PART * o + PART, residuals, sums)
        flush(0, f_in, ro_hbm, o)
    for t in range(STEPS):
        rsend[t] = own_cells(sums[2 * t], sums[2 * t + UNIT])
    part = rsend[:, 0, :]
    for s in range(1, SUB):
        part = part + rsend[:, s, :]
    rgath[me] = part
    rr_copies = gather(rgath, 1)

    def update(p, carry):
        for b0 in range(0, NB, 2):
            cut = pl.ds(b0, 2)
            x = coef[slot['x', 0]] * v0_a[p, cut]
            for j in range(1, SUB):
                x = x + coef[slot['x', j]] * b_a[j - UNIT][p + UNIT, cut]
            x = x * isd_a[p, cut]
            u = jnp.stack([u_nat[p, pl.ds(b0 + b, SUB, stride=NB), :] for b in range(2)], axis=0)
            put(k_in, p, b0, u + x)
        return carry

    for o in range(3):
        lax.fori_loop(PART * o, PART * o + PART, update, 0)
        flush(1, k_in, uo_hbm, o)
    for copy in rr_copies:
        copy.wait()
    part = rgath[0]
    for dev in range(1, SUB):
        part = part + rgath[dev]
    part = jnp.broadcast_to(jnp.sum(part, axis=1, keepdims=True), (SUB, LANES))
    rr_ref[...] = jnp.sum(jnp.where(lane == sub, part, ZERO), axis=0, keepdims=True)[:, :STEPS]
    for copy in outs:
        copy.wait()


def solution(mesh):
    spec = P('gx', 'gy', 'gz')

    def local(k_cell, k_ghost, f_rhs, u_init):
        big = (E, NB, SUB, LANES)
        ext = (E + 2, NB, SUB, LANES)
        vm = lambda *shape: pltpu.VMEM(shape, F32)
        any_spec = pl.BlockSpec(memory_space=pl.ANY)
        block = jax.ShapeDtypeStruct((N, N, N), F32)
        u, r, rr = pl.pallas_call(
            kernel,
            out_shape=(block, block, jax.ShapeDtypeStruct((1, STEPS), F32)),
            in_specs=[any_spec] * 4,
            out_specs=(any_spec, any_spec, pl.BlockSpec(memory_space=pltpu.VMEM)),
            scratch_shapes=[
                vm(N, N, N), vm(N, N, N), vm(N, N, N), vm(E + 2, E, LANES), vm(E, E, LANES), vm(E, E, LANES),
                vm(*ext), vm(*big), vm(*big), vm(*big), vm(N, NB, SUB, LANES),
                *[vm(E + 2, NB, SUB, LANES)] * STEPS,
                vm(3, 144, 144), vm(LANES, LANES), vm(LANES, LANES), vm(E, LANES), vm(N, SUB, N), vm(1, N, N), vm(1, N, N),
                vm(2, 45, SUB, LANES), vm(2, 45, SUB, LANES), vm(2, TILES, SUB, LANES), vm(2, TILES, SUB, LANES),
                vm(2, N, N), vm(2, N, N), vm(2, TILES, SUB, LANES), vm(2, TILES, SUB, LANES),
                vm(NDOT, SUB, LANES), vm(SUB, 2 * NDOT, LANES), vm(SUB, SUB, LANES), vm(SUB, SUB, LANES), vm(44, SUB, LANES),
                pltpu.SemaphoreType.DMA((6, 3)), pltpu.SemaphoreType.DMA((2, 3)),
                pltpu.SemaphoreType.DMA((12,)), pltpu.SemaphoreType.DMA((12,)),
                pltpu.SemaphoreType.DMA((2, LAST)), pltpu.SemaphoreType.DMA((2, LAST)),
            ],
            compiler_params=pltpu.CompilerParams(collective_id=0, has_side_effects=True, vmem_limit_bytes=67043328),
        )(k_cell, f_rhs, u_init, k_ghost)
        return u, r, rr.reshape(STEPS)

    return jax.shard_map(local, mesh=mesh, in_specs=(spec, P(), spec, spec), out_specs=(spec, spec, P()), check_vma=False)
```

```python
import functools

import jax
import jax.numpy as jnp
from jax import lax
from jax.experimental import pallas as pl
from jax.experimental.pallas import tpu as pltpu
from jax.sharding import PartitionSpec as P


N = 72
H = 8
E = N + H
NB = 10
STEPS = 8
MESH = pl.DeviceIdType.MESH
F32 = jnp.float32
OTHERS = [(fx, fy, fz) for fx in (0, 1) for fy in (0, 1) for fz in (0, 1) if fx or fy or fz]
NDOT = 24
SUB = 8
LANES = 128
TILES = 9
PART = 24
WIDTH = 4
LAST = 7
GROUPS = 16
PIECES = 5
ZERO, ONE, HALF, TWO = 0.0, 1.0, 0.5, 2.0
UNIT = 1
HEAD = 4


def iota(axis):
    return lax.broadcasted_iota(jnp.int32, (SUB, LANES), axis)


def two_sum(a, b):
    s = a + b
    t = s - a
    return s, (a - (s - t)) + (b - t)


def quick(a, b):
    s = a + b
    return s, b - (s - a)


def two_prod(a, b):
    def split(x):
        t = x * 4097.0
        hi = t - (t - x)
        return hi, x - hi
    p = a * b
    ah, al = split(a)
    bh, bl = split(b)
    return p, ((ah * bh - p) + ah * bl + al * bh) + al * bl


def dadd(x, y):
    (xh, xl), (yh, yl) = x, y
    s, e = two_sum(xh, yh)
    return quick(s, e + (xl + yl))


def dsub(x, y):
    yh, yl = y
    return dadd(x, (-yh, -yl))


def dscale(x, c):
    hi, lo = x
    return hi * c, lo * c


def dmul(x, y):
    (xh, xl), (yh, yl) = x, y
    p, e = two_prod(xh, yh)
    return quick(p, e + (xh * yl + xl * yh))


def ddiv(x, y):
    (xh, xl), (yh, yl) = x, y
    q = xh / yh
    p, e = two_prod(q, yh)
    rest = ((xh - p) - e) + (xl - q * yl)
    return quick(q, rest / yh)


def step_lengths(m):
    alphas, betas = [], []
    y = dict(enumerate(m))
    p = {0: dsub(y[0], y[1])}
    for l in range(1, 15):
        p[l] = dsub(y[l], dscale(dadd(y[l + UNIT], y[l - UNIT]), HALF))
    for t in range(STEPS):
        alpha = ddiv(y[t], p[t])
        alphas.append(alpha[0])
        if t == STEPS - UNIT:
            break
        y_next = {l: dsub(y[l], dmul(alpha, p[l])) for l in range(t + UNIT, 15 - t)}
        beta = ddiv(y_next[t + UNIT], p[t])
        if t:
            beta = dscale(beta, HALF)
        betas.append(beta[0])
        p_next = {}
        for l in range(t + UNIT, 14 - t):
            side = y_next[l + UNIT] if l == t + UNIT else dadd(y_next[l + UNIT], y_next[l - UNIT])
            p_next[l] = dadd(dsub(y_next[l], dscale(side, HALF)), dmul(beta, p[l]))
        y, p = y_next, p_next
    return alphas, betas


def basis_coefs(alphas, betas):
    def add(a, b):
        return b if a is None else (a if b is None else a + b)

    def axpy(x, c, y):
        return [xi if yi is None else (c * yi if xi is None else xi + c * yi) for xi, yi in zip(x, y)]

    def apply_op(v):
        out = [None] * 11
        out[1] = v[0]
        for j in range(SUB):
            if v[1 + j] is None:
                continue
            c = v[1 + j]
            out[1 + j] = add(out[1 + j], c)
            if j == 0:
                out[2] = add(out[2], -c)
            else:
                half = -HALF * c
                out[2 + j] = add(out[2 + j], half)
                out[j] = add(out[j], half)
        return out[:TILES]

    one = jnp.ones_like(alphas[0])
    y = [one] + [None] * SUB
    p = list(y)
    x = [None] * TILES
    ys = []
    for t in range(STEPS):
        q = apply_op(p)
        x = axpy(x, alphas[t], p)
        y = axpy(y, -alphas[t], q)
        ys.append(y)
        if t < STEPS - UNIT:
            p = axpy(y, betas[t], p)
    return ys, x


def row_down(v):
    return jnp.concatenate([pltpu.roll(v[NB - UNIT], 1, 0)[None], v[:NB - UNIT]], axis=0)


def row_up(v):
    return jnp.concatenate([v[1:], pltpu.roll(v[0], LAST, 0)[None]], axis=0)


def lane_down(v):
    return pltpu.roll(v, 1, 2)


def lane_up(v):
    return pltpu.roll(v, 127, 2)


def load_chunk(ref, plane):
    return jnp.stack([ref[plane, pl.ds(b, SUB, stride=NB), :] for b in range(NB)], axis=0)


def replace(v, b, mask, value):
    return jnp.concatenate(([v[:b]] if b else []) + [jnp.where(mask, value, v[b])[None], v[b + UNIT:]], axis=0)


def harmonic(a, b):
    return TWO * a * b / (a + b)


def pick(mask, a, b):
    return lax.select_n(mask, b, a)


def planes(lo, hi, body, init, width=WIDTH):
    def some(n, carry):
        for w in range(width):
            carry = body(lo + n * width + w, carry)
        return carry
    return lax.fori_loop(0, (hi - lo) // width, some, init)


def own_cells(low, high):
    sub, lane = iota(0), iota(1)
    return jnp.where(lane < N, low + jnp.where(sub < LAST, high, ZERO), ZERO)


def kernel(k_hbm, f_hbm, u_hbm, kg_hbm, k_in, f_in, rr_ref,
           u_in, k_nat, u_nat, z_nat, cx_a, cy_a, cz_a, isd_a, v0_a, b0_a, b1_a, b2_a, b3_a, b4_a, b5_a, b6_a, b7_a,
           walls, wz, wz_t, wy, ky, kx, ux, zs, zr, ds_, dr, row_s, row_r, lane_s, lane_r, acc, gath, rsend, rgath, coef,
           load_sem, send_sem, recv_sem, all_send, all_recv):
    cx, cy, cz = lax.axis_index('gx'), lax.axis_index('gy'), lax.axis_index('gz')
    me = cx + 2 * cy + 4 * cz
    b_a = (b0_a, b1_a, b2_a, b3_a, b4_a, b5_a, b6_a, b7_a)
    lane, sub = iota(1), iota(0)

    def peer(fx, fy, fz):
        out = {}
        if fx:
            out['gx'] = 1 - cx
        if fy:
            out['gy'] = 1 - cy
        if fz:
            out['gz'] = 1 - cz
        return out

    loads = []
    for n, (src, dst) in enumerate([(k_hbm, k_in), (u_hbm, u_in), (f_hbm, f_in)]):
        loads.append([pltpu.make_async_copy(src.at[pl.ds(PART * q, PART)], dst.at[pl.ds(PART * q, PART)], load_sem.at[n, q])
                      for q in range(N // PART)])
    loads.append([pltpu.make_async_copy(kg_hbm.at[cx], walls.at[0], load_sem.at[3, 0])])
    loads.append([pltpu.make_async_copy(kg_hbm.at[2 + cy], walls.at[1], load_sem.at[4, 0])])
    loads.append([pltpu.make_async_copy(kg_hbm.at[4 + cz], walls.at[2], load_sem.at[PIECES, 0])])
    for n in (0, 1, 3, 4, PIECES, 2):
        for copy in loads[n]:
            copy.start()

    barrier = pltpu.get_barrier_semaphore()
    for flips in OTHERS:
        pl.semaphore_signal(barrier, inc=1, device_id=peer(*flips), device_id_type=MESH)

    def send(n, src, dst, flips):
        copy = pltpu.make_async_remote_copy(src_ref=src, dst_ref=dst, send_sem=send_sem.at[n], recv_sem=recv_sem.at[n],
                                            device_id=peer(*flips), device_id_type=MESH)
        copy.start()
        return copy

    near_y = pl.multiple_of((N - H) * (1 - cy), SUB)
    near_x = (N - H) * (1 - cx)
    src8 = (N - H) * (1 - cz)
    dst8 = N + 48 * cz
    ghost8 = jnp.logical_and(lane >= dst8, lane < dst8 + SUB)
    wall_lane = 127 - 55 * cz
    own_lane = lane < N
    at_wall = lane == wall_lane
    zero = jnp.zeros((SUB, LANES), F32)
    ones = jnp.ones((SUB, LANES), F32)

    def turn(x, by):
        return pltpu.roll(x, lax.rem(by + LANES, LANES), 1)

    def shift(x, by):
        return pltpu.roll(x, by % LANES, 1) if by % LANES else x

    def widen(x):
        return x if x.shape[1] == LANES else jnp.concatenate([x, jnp.zeros((x.shape[0], LANES - x.shape[1]), F32)], axis=1)

    def pack(nat, packed, corner):
        group8 = lax.rem(lane + (LANES - src8), LANES) // SUB
        groups = [group8 == g for g in range(GROUPS)]

        def body(o, carry):
            for q in range(PIECES):
                out = None
                for g in range(min(GROUPS, N - GROUPS * q)):
                    t = GROUPS * q + g
                    if t % TILES == 0:
                        plane = widen(nat[o * SUB + t // TILES, 0:N, :])
                    x = shift(plane[SUB * (t % TILES):SUB * (t % TILES) + SUB], SUB * g)
                    out = x if g == 0 else pick(groups[g], x, out)
                packed[o * PIECES + q] = out
            out = None
            for g in range(SUB):
                x = widen(nat[o * SUB + g, pl.ds(near_y, SUB), :])
                x = shift(x, SUB * g)
                out = x if g == 0 else pick(groups[g], x, out)
            corner[o] = out
            return carry
        lax.fori_loop(0, TILES, body, 0)

    def unpack(own, side, nat, packed, corner, fill, wall, o, carry):
        by = dst8 - (N - H - src8)
        packs, corner_in = [turn(packed[o * PIECES + q], by) for q in range(PIECES)], turn(corner[o], by)
        for pi in range(SUB):
            i, out = o * SUB + pi, []
            plane = widen(own[i, 0:N, :])
            for jt in range(NB):
                if jt < TILES:
                    t = pi * TILES + jt
                    got, g = packs[t // GROUPS], t % GROUPS
                else:
                    got, g = corner_in, pi
                x = plane[SUB * jt:SUB * jt + SUB] if jt < TILES else widen(side[i])
                other = fill if wall is None else pick(at_wall, wall_column(i, jt), fill)
                out.append(pick(own_lane, x, pick(ghost8, shift(got, -SUB * g), other)))
            nat[i, 0:E, :] = jnp.concatenate(out, axis=0)
        return carry

    def wall_column(i, jt):
        at = SUB * jt if jt < TILES else pl.multiple_of(N + 48 * cy, SUB)
        return pltpu.roll(wz_t[pl.ds(at, SUB), :], LANES - UNIT - i, 1)

    for copy in loads[0] + loads[1]:
        copy.wait()
    last_x, last_y, last_z = (N - UNIT) * (1 - cx), (N - UNIT) * (1 - cy), (N - UNIT) * (1 - cz)

    slots = lax.rem(lane + (LANES - last_z), LANES)

    def pack_one(o, carry):
        for n, src in enumerate((k_in, u_in)):
            row_s[n, pl.ds(pl.multiple_of(o * SUB, SUB), SUB), :] = jnp.concatenate(
                [src[o * SUB + r, pl.ds(last_y, 1), :] for r in range(SUB)], axis=0)
            out = None
            for t in range(N):
                if t % TILES == 0:
                    plane = widen(src[o * SUB + t // TILES])
                x = shift(plane[SUB * (t % TILES):SUB * (t % TILES) + SUB], t)
                out = x if t == 0 else pick(slots == t, x, out)
            lane_s[n, o] = out
        return carry
    lax.fori_loop(0, TILES, pack_one, 0)
    pl.semaphore_wait(barrier, len(OTHERS))
    one_x = [send(0, k_in.at[pl.ds(last_x, 1)], kx, (1, 0, 0)), send(1, u_in.at[pl.ds(last_x, 1)], ux, (1, 0, 0))]
    one_y = send(2, row_s, row_r, (0, 1, 0))
    one_z = send(3, lane_s, lane_r, (0, 0, 1))
    k_y = send(4, k_in.at[:, pl.ds(near_y, SUB), :], ky, (0, 1, 0))
    pack(k_in, zs.at[0], ds_.at[0])
    k_z = send(PIECES, zs.at[0], zr.at[0], (0, 0, 1))
    k_d = send(6, ds_.at[0], dr.at[0], (0, 1, 1))

    for n in (3, 4, PIECES):
        loads[n][0].wait()

    def lane_ring(w, at, c):
        left, right = walls[w, pl.ds(at, SUB), 0:LANES], walls[w, pl.ds(at, SUB), LANES:144]
        gap = jnp.zeros((SUB, 56), F32)
        right = jnp.concatenate([gap, right, gap], axis=1)
        turned = jnp.where(jnp.logical_and(lane >= 56, lane < N), right, pltpu.roll(left, 56, 1))
        return jnp.where(c == 0, left, turned)

    for jt in range(NB):
        at_j = pl.multiple_of(N * cy + SUB * jt if jt < TILES else N - H * cy, SUB)
        at_i = pl.multiple_of(N * cx + SUB * jt if jt < TILES else N - H * cx, SUB)
        k_nat[E, pl.ds(SUB * jt, SUB), :] = lane_ring(0, at_j, cz)
        wy[pl.ds(SUB * jt, SUB), :] = lane_ring(1, at_i, cz)
        if jt < TILES:
            wz[pl.ds(SUB * jt, SUB), :] = lane_ring(2, at_i, cy)
    wz_t[...] = turn(wz[...].T, wall_lane + UNIT)

    for copy in loads[2]:
        copy.wait()

    def take_f(p, carry):
        for b in range(NB):
            rows = SUB if b < 2 else LAST
            v0_a[p, b, 0:rows, 0:N] = f_in[p, pl.ds(b, rows, stride=NB), :]
        return carry
    planes(0, N, take_f, 0)

    u_nat[E - UNIT - LAST * cx] = jnp.zeros((E, LANES), F32)
    one_lane = N + 55 * cz
    at_one = lane == one_lane
    for copy in one_x + [one_y, one_z]:
        copy.wait()
    u_nat[N + LAST * cx, 0:N, 0:N] = ux[0]
    k_nat[E + UNIT, 0:N, 0:N] = kx[0]

    def unpack_one(o, carry):
        lanes_in = [turn(lane_r[n, o], one_lane - (N - UNIT - last_z)) for n in range(2)]
        for pi in range(SUB):
            i = o * SUB + pi
            planes_in = [widen(k_in[i]), widen(u_in[i])]
            for n, nat in enumerate((k_nat, u_nat)):
                out = []
                for jt in range(TILES):
                    other = zero if n else pick(at_wall, wall_column(i, jt), ones)
                    other = pick(at_one, shift(lanes_in[n], -(pi * TILES + jt)), other)
                    out.append(pick(own_lane, planes_in[n][SUB * jt:SUB * jt + SUB], other))
                nat[i, 0:N, :] = jnp.concatenate(out, axis=0)
        return carry
    lax.fori_loop(0, TILES, unpack_one, 0)

    row0 = sub == 0
    row72 = sub == LAST

    def divergence(h_x, h_xn, h_y, h_z, v, v_prev, v_next, low_row, high_row):
        low = row_down(v)
        high = v
        if low_row is not None:
            low = replace(low, 0, row0, low_row)
            high = replace(v, 2, row72, high_row)
        else:
            low = replace(low, 0, jnp.logical_and(row0, cy == 0), ZERO)
            high = replace(v, 2, jnp.logical_and(row72, cy == 1), ZERO)
        f_y = h_y * (high - low)
        f_z = h_z * (v - lane_down(v))
        return ((h_x * (v - v_prev) - h_xn * (v_next - v)) + (f_y - row_up(f_y))) + (f_z - lane_up(f_z))

    def full(row):
        return jnp.broadcast_to(widen(row), (SUB, LANES))

    def add_up(h_x, h_xn, h_y, h_z):
        return ((h_x + h_xn) + (h_y + row_up(h_y))) + (h_z + lane_up(h_z))

    def start_own(n, carry):
        p0 = WIDTH * n
        first_trip, last_trip = n == 0, n == N // WIDTH - UNIT
        k_p = [load_chunk(k_nat, jnp.where(first_trip, E + cx, p0 - UNIT))]
        u_p = [load_chunk(u_nat, jnp.where(first_trip, E - UNIT, p0 - UNIT))]
        for w in range(WIDTH):
            k_p.append(load_chunk(k_nat, p0 + w))
            u_p.append(load_chunk(u_nat, p0 + w))
        k_p.append(load_chunk(k_nat, jnp.where(last_trip, E + UNIT - cx, p0 + WIDTH)))
        u_p.append(load_chunk(u_nat, p0 + WIDTH))
        h_x = [harmonic(k_p[w + UNIT], k_p[w]) for w in range(WIDTH + UNIT)]
        for w in range(WIDTH):
            p, kc = p0 + w, k_p[w + UNIT]
            wall, got = full(wy[pl.ds(p, 1), :]), full(row_r[0, pl.ds(p, 1), :])
            low = replace(row_down(kc), 0, row0, jnp.where(cy == 0, wall, got))
            high = replace(kc, 2, row72, jnp.where(cy == 0, got, wall))
            h_y = harmonic(high, low)
            h_z = harmonic(kc, lane_down(kc))
            inv = lax.rsqrt(add_up(h_x[w], h_x[w + UNIT], h_y, h_z))
            got = full(row_r[1, pl.ds(p, 1), :])
            a_u = divergence(h_x[w], h_x[w + UNIT], h_y, h_z, u_p[w + UNIT], u_p[w], u_p[w + 2],
                             jnp.where(cy == 0, ZERO, got), jnp.where(cy == 0, got, ZERO))
            y0 = (v0_a[p] - a_u) * inv
            for b in range(NB):
                v0_a[p, b] = y0[b] if b < 2 else pick(row72, zero, y0[b])
            z0 = y0 * inv
            for b in range(NB):
                if b < 2:
                    z_nat[p, pl.ds(b, SUB, stride=NB), :] = z0[b]
                else:
                    z_nat[p, pl.ds(b, LAST, stride=NB), :] = z0[b, :LAST]
        return carry
    lax.fori_loop(0, N // WIDTH, start_own, 0)

    z_y = send(LAST, z_nat.at[pl.ds(0, N), pl.ds(near_y, SUB), :], z_nat.at[pl.ds(0, N), pl.ds(N, SUB), :], (0, 1, 0))
    pack(z_nat, zs.at[1], ds_.at[1])
    z_z = send(8, zs.at[1], zr.at[1], (0, 0, 1))
    z_d = send(9, ds_.at[1], dr.at[1], (0, 1, 1))

    def spread(n, nat, take):
        take(SUB * (1 - cx), 0)
        copy = send(n, nat.at[pl.ds(near_x, SUB)], nat.at[pl.ds(N, SUB)], (1, 0, 0))
        lax.fori_loop(0, SUB, lambda o, carry: take(o + cx, carry), 0)
        return copy

    for copy in (k_y, k_z, k_d):
        copy.wait()
    spread(NB, k_nat, functools.partial(unpack, k_in, ky, k_nat, zr.at[0], dr.at[0], ones, wz_t)).wait()

    def faces(p, carry):
        kc = load_chunk(k_nat, p)
        before = jnp.where(jnp.logical_and(p == 0, cx == 0), E, jnp.where(p == 0, E - UNIT, p - UNIT))
        here = jnp.where(jnp.logical_and(p == N, cx == 1), E, p)
        cx_a[p] = harmonic(load_chunk(k_nat, here), load_chunk(k_nat, before))
        wall = full(wy[pl.ds(p, 1), :])
        low = replace(row_down(kc), 0, jnp.logical_and(row0, cy == 0), wall)
        high = replace(kc, 2, jnp.logical_and(row72, cy == 1), wall)
        cy_a[p] = harmonic(high, low)
        cz_a[p] = harmonic(kc, lane_down(kc))
        return carry
    planes(0, E, faces, 0)
    cx_a[E] = cx_a[0]
    cx_a[E + UNIT] = cx_a[1]

    def scales(own, p, carry):
        d = add_up(cx_a[p], cx_a[p + UNIT], cy_a[p], cz_a[p])
        inv = lax.rsqrt(d)
        isd_a[p] = inv
        if own:
            sd = d * inv
            for b in range(NB):
                k_nat[p, pl.ds(SUB * b, SUB), :] = sd[b] if b < 2 else pick(row72, zero, sd[b])
        return carry
    planes(0, N, functools.partial(scales, True), 0)
    planes(N, E, functools.partial(scales, False), 0)

    for copy in (z_y, z_z, z_d):
        copy.wait()
    z_x = spread(11, z_nat, functools.partial(unpack, z_nat, z_nat.at[:, pl.ds(N, SUB), :], z_nat, zr.at[1], dr.at[1],
                                              zero, None))

    def column(ref, p, b, width):
        return ref[pl.ds(p, width), b]

    def z_column(p, b, width=1):
        return z_nat[pl.ds(p, width), pl.ds(b, SUB, stride=NB), :]

    def tally(carry, b, products):
        return [c + jnp.sum(products[n // 2], axis=0) if n % 2 == (b > 1) else c for n, c in enumerate(carry)]

    def first(own, width, p, carry, before=None, after=None, x_after=None):
        before = p - UNIT if before is None else before
        z, inv, low, f_y, h_y = {}, {}, {}, {}, {}

        def load(b):
            z[b], inv[b], h_y[b] = z_column(p, b, width), column(isd_a, p, b, width), column(cy_a, p, b, width)
            under = z[b - UNIT] if b else pltpu.roll(z_column(p, NB - UNIT, width), 1, 1)
            over = z[b]
            if b == 0:
                under = jnp.where(jnp.logical_and(row0, cy == 0), ZERO, under)
            if b == 2:
                over = jnp.where(jnp.logical_and(row72, cy == 1), ZERO, over)
            f_y[b] = h_y[b] * (over - under)
        carry = list(carry)
        load(0)
        for b in range(NB):
            if b < NB - UNIT:
                load(b + UNIT)
            up = f_y[b + UNIT] if b < NB - UNIT else pltpu.roll(f_y[0], LAST, 1)
            z_p = z_column(before, b)
            z_n = z_column(p + width if after is None else after, b)
            if isinstance(p, int) and p == 0:
                z_p = jnp.where(cx == 0, ZERO, z_p)
            if isinstance(p, int) and p == N - UNIT:
                z_n = jnp.where(cx == 1, ZERO, z_n)
            if x_after is None:
                h_x = column(cx_a, p, b, width + UNIT)
            else:
                h_x = jnp.concatenate([column(cx_a, p, b, 1), column(cx_a, x_after, b, 1)], axis=0)
            f_x = h_x * (jnp.concatenate([z[b], z_n], axis=0) - jnp.concatenate([z_p, z[b]], axis=0))
            h_z = column(cz_a, p, b, width)
            f_z = h_z * (z[b] - lane_down(z[b]))
            b0 = inv[b] * (((f_x[:width] - f_x[1:]) + (f_y[b] - up)) + (f_z - lane_up(f_z)))
            b_a[0][pl.ds(p + UNIT, width), b] = b0
            twice = TWO * inv[b]
            side = column(isd_a, before, b, 1)
            if width > 1:
                side = jnp.concatenate([side, inv[b][:width - UNIT]], axis=0)
            cx_a[pl.ds(p, width), b] = h_x[:width] * (twice * side)
            side = inv[b - UNIT] if b else pltpu.roll(column(isd_a, p, NB - UNIT, width), 1, 1)
            c_y = h_y[b] * (twice * side)
            if b == 0:
                c_y = jnp.where(jnp.logical_and(row0, cy == 0), ZERO, c_y)
            if b == 2:
                c_y = jnp.where(jnp.logical_and(row72, cy == 1), ZERO, c_y)
            cy_a[pl.ds(p, width), b] = c_y
            cz_a[pl.ds(p, width), b] = jnp.where(at_edge, ZERO, h_z * (twice * lane_down(inv[b])))
            if own:
                v0 = column(v0_a, p, b, width)
                carry = tally(carry, b, (v0 * v0, v0 * b0, b0 * b0))
        return tuple(carry)

    at_edge = lane == N * cz

    def wrap(ref):
        ref[0] = ref[E]
        ref[E + UNIT] = ref[1]

    sums = lax.fori_loop(0, 14, lambda n, carry: first(True, PIECES, 1 + PIECES * n, carry), (zero,) * 6)
    z_x.wait()
    sums = first(True, 1, 0, sums, E - UNIT, None, E + UNIT)
    sums = first(True, 1, N - UNIT, sums)
    first(False, WIDTH, N, ())
    first(False, WIDTH, N + WIDTH, (), None, 0)
    cx_a[0] = jnp.where(cx == 0, ZERO, cx_a[0])
    cx_a[N] = jnp.where(cx == 1, ZERO, cx_a[N])
    cx_a[E] = cx_a[0]
    wrap(b_a[0])
    acc[0] = own_cells(sums[0], sums[1])
    acc[1] = own_cells(sums[2], sums[3])
    acc[TILES] = own_cells(sums[4], sums[PIECES])
    acc[23] = zero

    def advance(k, own, width, p, carry):
        old, carry = b_a[k - UNIT], list(carry)
        v_low = pltpu.roll(column(old, p + UNIT, NB - UNIT, width), 1, 1)
        v, c_y = column(old, p + UNIT, 0, width), column(cy_a, p, 0, width)
        t_first = c_y * v
        for b in range(NB):
            if b < NB - UNIT:
                v_high, c_high = column(old, p + UNIT, b + UNIT, width), column(cy_a, p, b + UNIT, width)
                t_high = c_high * v_high
            else:
                t_high = pltpu.roll(t_first, LAST, 1)
            c_x, c_z = column(cx_a, p, b, width + UNIT), column(cz_a, p, b, width)
            below, above = column(old, p, b, 1), column(old, p + width + UNIT, b, 1)
            if width > 1:
                below = jnp.concatenate([below, v[:width - UNIT]], axis=0)
                above = jnp.concatenate([v[1:], above], axis=0)
            new = c_x[:width] * below + c_x[1:] * above
            new = new + (c_y * v_low + t_high)
            new = new + (c_z * lane_down(v) + lane_up(c_z * v))
            new = HALF * new if k == 1 else new - column(b_a[k - 2], p + UNIT, b, width)
            b_a[k][pl.ds(p + UNIT, width), b] = new
            if own:
                carry = tally(carry, b, (column(v0_a, p, b, width) * new, v * new, new * new))
            v_low, v, c_y = v, v_high, c_high
        return tuple(carry)

    for k in range(1, STEPS):
        sums = lax.fori_loop(0, N // SUB, lambda n, carry: advance(k, True, SUB, SUB * n, carry), (zero,) * 6)
        if k < STEPS - UNIT:
            advance(k, False, SUB, N, ())
            wrap(b_a[k])
        acc[1 + k] = own_cells(sums[0], sums[1])
        acc[GROUPS + k - UNIT] = own_cells(sums[2], sums[3])
        if k < STEPS - UNIT:
            acc[TILES + k] = own_cells(sums[4], sums[PIECES])

    def gather(buf, n_sem):
        copies = []
        for n, flips in enumerate(OTHERS):
            copies.append(pltpu.make_async_remote_copy(
                src_ref=buf.at[me], dst_ref=buf.at[me], send_sem=all_send.at[n_sem, n], recv_sem=all_recv.at[n_sem, n],
                device_id=peer(*flips), device_id_type=MESH))
        for copy in copies:
            copy.start()
        return copies

    hi = acc[:, 0, :]
    lo = jnp.zeros((NDOT, LANES), F32)
    for s in range(1, SUB):
        hi, err = two_sum(hi, acc[:, s, :])
        lo = lo + err
    gath[me, 0:NDOT] = hi
    gath[me, NDOT:2 * NDOT] = lo
    gath_copies = gather(gath, 0)
    pair = {}
    for i in range(HEAD + UNIT):
        for j in range(i, HEAD + UNIT):
            pair[i, j] = len(pair)

    def products(n, carry):
        p, carry = WIDTH * n, list(carry)
        for b in range(NB):
            sd = k_nat[pl.ds(p, WIDTH), pl.ds(SUB * b, SUB), :]
            w = [sd * column(v0_a, p, b, WIDTH)] + [sd * column(b_a[j], p + UNIT, b, WIDTH) for j in range(HEAD)]
            for (i, j), at in pair.items():
                carry[at] = carry[at] + jnp.sum(w[i] * w[j], axis=0)
        return tuple(carry)
    gram = lax.fori_loop(0, N // WIDTH, products, (zero,) * len(pair))
    for copy in gath_copies:
        copy.wait()
    hi, lo = gath[0, 0:NDOT], gath[0, NDOT:2 * NDOT]
    for dev in range(1, SUB):
        hi, err = two_sum(hi, gath[dev, 0:NDOT])
        lo = lo + (gath[dev, NDOT:2 * NDOT] + err)
    for shift in (64, 32, GROUPS, SUB, 4, 2, 1):
        hi, err = two_sum(hi, pltpu.roll(hi, shift, 1))
        lo = (lo + pltpu.roll(lo, shift, 1)) + err
    hi, lo = quick(hi, lo)
    size = hi[0:1]
    factor = jnp.where(size > 1e30, TWO ** -110, jnp.where(size > 1e12, TWO ** -60, jnp.where(
        size < 1e-30, TWO ** 110, jnp.where(size < 1e-12, TWO ** 60, ONE)))).astype(F32)
    hi, lo = hi * factor, lo * factor

    def total(row):
        return jnp.broadcast_to(hi[row:row + UNIT], (SUB, LANES)), jnp.broadcast_to(lo[row:row + UNIT], (SUB, LANES))

    n_mom = [total(TILES), total(GROUPS)]
    for j in range(1, LAST):
        n_mom.append(dsub(dscale(total(TILES + j), TWO), n_mom[0]))
        n_mom.append(dsub(dscale(total(GROUPS + j), TWO), n_mom[1]))
    l_mom = [total(1 + j) for j in range(SUB)]
    for j in range(LAST, 14):
        l_mom.append(dsub(dscale(dsub(l_mom[j], n_mom[j]), TWO), l_mom[j - UNIT]))
    m_mom = [total(0)]
    m_mom.append(dsub(m_mom[0], l_mom[0]))
    for j in range(1, 15):
        m_mom.append(dsub(dscale(dsub(m_mom[j], l_mom[j]), TWO), m_mom[j - UNIT]))
    ys, xs = basis_coefs(*step_lengths(m_mom))
    slot = {}
    for t in range(STEPS):
        for j in range(t + UNIT):
            slot[t, j] = len(slot)
            coef[slot[t, j]] = ys[t][1 + j]
    for j in range(SUB):
        slot['x', j] = len(slot)
        coef[slot['x', j]] = xs[j]

    def put(ref, p, b0, val):
        for b in range(val.shape[0]):
            if b0 + b < 2:
                ref[p, pl.ds(b0 + b, SUB, stride=NB), :] = val[b, :, :N]
            else:
                ref[p, pl.ds(b0 + b, LAST, stride=NB), :] = val[b, :LAST, :N]

    def residuals(p, carry):
        carry = list(carry)
        for b0 in range(0, NB, 2):
            cut = pl.ds(b0, 2)
            v0 = v0_a[p, cut]
            sd = jnp.stack([k_nat[p, pl.ds(SUB * (b0 + b), SUB), :] for b in range(2)], axis=0)
            bs = [ref[p + UNIT, cut] for ref in b_a]
            for t in range(HEAD, STEPS):
                y = v0
                for j in range(t + UNIT):
                    y = y + coef[slot[t, j]] * bs[j]
                r = sd * y
                which = 2 * (t - HEAD) + (b0 > 0)
                carry[which] = carry[which] + jnp.sum(r * r, axis=0)
                if t == STEPS - UNIT:
                    put(f_in, p, b0, r)
        return tuple(carry)

    sums = lax.fori_loop(0, N, residuals, (zero,) * (2 * (STEPS - HEAD)))
    for t in range(STEPS):
        if t < HEAD:
            form = zero
            g = [None] + [coef[slot[t, j]] for j in range(t + 1)]
            for i in range(t + 2):
                part = gram[pair[0, i]] if not i else g[i] * gram[pair[0, i]]
                form = form + (part if not i else part + part)
            for i in range(UNIT, t + 2):
                part = zero
                for j in range(UNIT, t + 2):
                    part = part + g[j] * gram[pair[min(i, j), max(i, j)]]
                form = form + g[i] * part
            rsend[t] = pick(own_lane, form, zero)
        else:
            rsend[t] = own_cells(sums[2 * (t - HEAD)], sums[2 * (t - HEAD) + UNIT])
    part = rsend[:, 0, :]
    for s in range(1, SUB):
        part = part + rsend[:, s, :]
    rgath[me] = part
    rr_copies = gather(rgath, 1)

    def update(p, carry):
        for b0 in range(0, NB, 2):
            cut = pl.ds(b0, 2)
            x = coef[slot['x', 0]] * v0_a[p, cut]
            for j in range(1, SUB):
                x = x + coef[slot['x', j]] * b_a[j - UNIT][p + UNIT, cut]
            x = x * isd_a[p, cut]
            u = jnp.stack([u_nat[p, pl.ds(b0 + b, SUB, stride=NB), :] for b in range(2)], axis=0)
            put(k_in, p, b0, u + x)
        return carry

    lax.fori_loop(0, N, update, 0)
    for copy in rr_copies:
        copy.wait()
    part = rgath[0]
    for dev in range(1, SUB):
        part = part + rgath[dev]
    part = jnp.broadcast_to(jnp.sum(part, axis=1, keepdims=True), (SUB, LANES))
    rr_ref[...] = jnp.sum(jnp.where(lane == sub, part, ZERO), axis=0, keepdims=True)[:, :STEPS]


def solution(mesh):
    spec = P('gx', 'gy', 'gz')

    def local(k_cell, k_ghost, f_rhs, u_init):
        big = (E, NB, SUB, LANES)
        ext = (E + 2, NB, SUB, LANES)
        vm = lambda *shape: pltpu.VMEM(shape, F32)
        any_spec = pl.BlockSpec(memory_space=pl.ANY)
        u, r, rr = pl.pallas_call(
            kernel,
            out_shape=(vm(N, N, N), vm(N, N, N), vm(1, STEPS)),
            in_specs=[any_spec] * 4,
            out_specs=[pl.BlockSpec(memory_space=pltpu.VMEM)] * 3,
            scratch_shapes=[
                vm(N, N, N), vm(E + 2, E, LANES), vm(E, E, LANES), vm(E, E, LANES),
                vm(*ext), vm(*big), vm(*big), vm(*big), vm(N, NB, SUB, LANES),
                *[vm(E + 2, NB, SUB, LANES)] * STEPS,
                vm(3, 144, 144), vm(LANES, LANES), vm(LANES, LANES), vm(E, LANES), vm(N, SUB, N), vm(1, N, N), vm(1, N, N),
                vm(2, 45, SUB, LANES), vm(2, 45, SUB, LANES), vm(2, TILES, SUB, LANES), vm(2, TILES, SUB, LANES),
                vm(2, N, N), vm(2, N, N), vm(2, TILES, SUB, LANES), vm(2, TILES, SUB, LANES),
                vm(NDOT, SUB, LANES), vm(SUB, 2 * NDOT, LANES), vm(SUB, SUB, LANES), vm(SUB, SUB, LANES), vm(44, SUB, LANES),
                pltpu.SemaphoreType.DMA((6, 3)),
                pltpu.SemaphoreType.DMA((12,)), pltpu.SemaphoreType.DMA((12,)),
                pltpu.SemaphoreType.DMA((2, LAST)), pltpu.SemaphoreType.DMA((2, LAST)),
            ],
            compiler_params=pltpu.CompilerParams(collective_id=0, has_side_effects=True, vmem_limit_bytes=57 << 20),
        )(k_cell, f_rhs, u_init, k_ghost)
        return u, r, rr.reshape(STEPS)

    return jax.shard_map(local, mesh=mesh, in_specs=(spec, P(), spec, spec), out_specs=(spec, spec, P()), check_vma=False)
```

```python
import functools

import jax
import jax.numpy as jnp
from jax import lax
from jax.experimental import pallas as pl
from jax.experimental.pallas import tpu as pltpu
from jax.sharding import PartitionSpec as P


N = 72
H = 8
E = N + H
NB = 10
STEPS = 8
MESH = pl.DeviceIdType.MESH
F32 = jnp.float32
OTHERS = [(fx, fy, fz) for fx in (0, 1) for fy in (0, 1) for fz in (0, 1) if fx or fy or fz]
NDOT = 24
SUB = 8
LANES = 128
TILES = 9
PART = 24
WIDTH = 4
LAST = 7
GROUPS = 16
PIECES = 5
ZERO, ONE, HALF, TWO = 0.0, 1.0, 0.5, 2.0
UNIT = 1
HEAD = 4


def iota(axis):
    return lax.broadcasted_iota(jnp.int32, (SUB, LANES), axis)


def two_sum(a, b):
    s = a + b
    t = s - a
    return s, (a - (s - t)) + (b - t)


def quick(a, b):
    s = a + b
    return s, b - (s - a)


def two_prod(a, b):
    def split(x):
        t = x * 4097.0
        hi = t - (t - x)
        return hi, x - hi
    p = a * b
    ah, al = split(a)
    bh, bl = split(b)
    return p, ((ah * bh - p) + ah * bl + al * bh) + al * bl


def dadd(x, y):
    (xh, xl), (yh, yl) = x, y
    s, e = two_sum(xh, yh)
    return quick(s, e + (xl + yl))


def dsub(x, y):
    yh, yl = y
    return dadd(x, (-yh, -yl))


def dscale(x, c):
    hi, lo = x
    return hi * c, lo * c


def dmul(x, y):
    (xh, xl), (yh, yl) = x, y
    p, e = two_prod(xh, yh)
    return quick(p, e + (xh * yl + xl * yh))


def ddiv(x, y):
    (xh, xl), (yh, yl) = x, y
    q = xh / yh
    p, e = two_prod(q, yh)
    rest = ((xh - p) - e) + (xl - q * yl)
    return quick(q, rest / yh)


def step_lengths(m):
    alphas, betas = [], []
    y = dict(enumerate(m))
    p = {0: dsub(y[0], y[1])}
    for l in range(1, 15):
        p[l] = dsub(y[l], dscale(dadd(y[l + UNIT], y[l - UNIT]), HALF))
    for t in range(STEPS):
        alpha = ddiv(y[t], p[t])
        alphas.append(alpha[0])
        if t == STEPS - UNIT:
            break
        y_next = {l: dsub(y[l], dmul(alpha, p[l])) for l in range(t + UNIT, 15 - t)}
        beta = ddiv(y_next[t + UNIT], p[t])
        if t:
            beta = dscale(beta, HALF)
        betas.append(beta[0])
        p_next = {}
        for l in range(t + UNIT, 14 - t):
            side = y_next[l + UNIT] if l == t + UNIT else dadd(y_next[l + UNIT], y_next[l - UNIT])
            p_next[l] = dadd(dsub(y_next[l], dscale(side, HALF)), dmul(beta, p[l]))
        y, p = y_next, p_next
    return alphas, betas


def basis_coefs(alphas, betas):
    def add(a, b):
        return b if a is None else (a if b is None else a + b)

    def axpy(x, c, y):
        return [xi if yi is None else (c * yi if xi is None else xi + c * yi) for xi, yi in zip(x, y)]

    def apply_op(v):
        out = [None] * 11
        out[1] = v[0]
        for j in range(SUB):
            if v[1 + j] is None:
                continue
            c = v[1 + j]
            out[1 + j] = add(out[1 + j], c)
            if j == 0:
                out[2] = add(out[2], -c)
            else:
                half = -HALF * c
                out[2 + j] = add(out[2 + j], half)
                out[j] = add(out[j], half)
        return out[:TILES]

    one = jnp.ones_like(alphas[0])
    y = [one] + [None] * SUB
    p = list(y)
    x = [None] * TILES
    ys = []
    for t in range(STEPS):
        q = apply_op(p)
        x = axpy(x, alphas[t], p)
        y = axpy(y, -alphas[t], q)
        ys.append(y)
        if t < STEPS - UNIT:
            p = axpy(y, betas[t], p)
    return ys, x


def row_down(v):
    return jnp.concatenate([pltpu.roll(v[NB - UNIT], 1, 0)[None], v[:NB - UNIT]], axis=0)


def row_up(v):
    return jnp.concatenate([v[1:], pltpu.roll(v[0], LAST, 0)[None]], axis=0)


def lane_down(v):
    return pltpu.roll(v, 1, 2)


def lane_up(v):
    return pltpu.roll(v, 127, 2)


def load_chunk(ref, plane):
    return jnp.stack([ref[plane, pl.ds(b, SUB, stride=NB), :] for b in range(NB)], axis=0)


def replace(v, b, mask, value):
    return jnp.concatenate(([v[:b]] if b else []) + [jnp.where(mask, value, v[b])[None], v[b + UNIT:]], axis=0)


def harmonic(a, b):
    return TWO * a * b / (a + b)


def pick(mask, a, b):
    return lax.select_n(mask, b, a)


def planes(lo, hi, body, init, width=WIDTH):
    def some(n, carry):
        for w in range(width):
            carry = body(lo + n * width + w, carry)
        return carry
    return lax.fori_loop(0, (hi - lo) // width, some, init)


def own_cells(low, high):
    sub, lane = iota(0), iota(1)
    return jnp.where(lane < N, low + jnp.where(sub < LAST, high, ZERO), ZERO)


def kernel(k_hbm, f_hbm, u_hbm, kg_hbm, k_in, f_in, rr_ref,
           u_in, k_nat, u_nat, z_nat, cx_a, cy_a, cz_a, isd_a, v0_a, b0_a, b1_a, b2_a, b3_a, b4_a, b5_a, b6_a, b7_a,
           walls, wz, wz_t, wy, ky, kx, ux, zs, zr, ds_, dr, row_s, row_r, lane_s, lane_r, acc, gath, rsend, rgath, coef,
           load_sem, send_sem, recv_sem, all_send, all_recv):
    cx, cy, cz = lax.axis_index('gx'), lax.axis_index('gy'), lax.axis_index('gz')
    me = cx + 2 * cy + 4 * cz
    b_a = (b0_a, b1_a, b2_a, b3_a, b4_a, b5_a, b6_a, b7_a)
    lane, sub = iota(1), iota(0)

    def peer(fx, fy, fz):
        out = {}
        if fx:
            out['gx'] = 1 - cx
        if fy:
            out['gy'] = 1 - cy
        if fz:
            out['gz'] = 1 - cz
        return out

    loads = []
    for n, (src, dst) in enumerate([(k_hbm, k_in), (u_hbm, u_in), (f_hbm, f_in)]):
        loads.append([pltpu.make_async_copy(src.at[pl.ds(PART * q, PART)], dst.at[pl.ds(PART * q, PART)], load_sem.at[n, q])
                      for q in range(N // PART)])
    loads.append([pltpu.make_async_copy(kg_hbm.at[cx], walls.at[0], load_sem.at[3, 0])])
    loads.append([pltpu.make_async_copy(kg_hbm.at[2 + cy], walls.at[1], load_sem.at[4, 0])])
    loads.append([pltpu.make_async_copy(kg_hbm.at[4 + cz], walls.at[2], load_sem.at[PIECES, 0])])
    for n in (0, 1, 3, 4, PIECES, 2):
        for copy in loads[n]:
            copy.start()

    barrier = pltpu.get_barrier_semaphore()
    for flips in OTHERS:
        pl.semaphore_signal(barrier, inc=1, device_id=peer(*flips), device_id_type=MESH)

    def send(n, src, dst, flips):
        copy = pltpu.make_async_remote_copy(src_ref=src, dst_ref=dst, send_sem=send_sem.at[n], recv_sem=recv_sem.at[n],
                                            device_id=peer(*flips), device_id_type=MESH)
        copy.start()
        return copy

    near_y = pl.multiple_of((N - H) * (1 - cy), SUB)
    near_x = (N - H) * (1 - cx)
    src8 = (N - H) * (1 - cz)
    dst8 = N + 48 * cz
    ghost8 = jnp.logical_and(lane >= dst8, lane < dst8 + SUB)
    wall_lane = 127 - 55 * cz
    own_lane = lane < N
    at_wall = lane == wall_lane
    zero = jnp.zeros((SUB, LANES), F32)
    ones = jnp.ones((SUB, LANES), F32)

    def turn(x, by):
        return pltpu.roll(x, lax.rem(by + LANES, LANES), 1)

    def shift(x, by):
        return pltpu.roll(x, by % LANES, 1) if by % LANES else x

    def widen(x):
        return x if x.shape[1] == LANES else jnp.concatenate([x, jnp.zeros((x.shape[0], LANES - x.shape[1]), F32)], axis=1)

    def pack(nat, packed, corner):
        group8 = lax.rem(lane + (LANES - src8), LANES) // SUB
        groups = [group8 == g for g in range(GROUPS)]

        def body(o, carry):
            for q in range(PIECES):
                out = None
                for g in range(min(GROUPS, N - GROUPS * q)):
                    t = GROUPS * q + g
                    if t % TILES == 0:
                        plane = widen(nat[o * SUB + t // TILES, 0:N, :])
                    x = shift(plane[SUB * (t % TILES):SUB * (t % TILES) + SUB], SUB * g)
                    out = x if g == 0 else pick(groups[g], x, out)
                packed[o * PIECES + q] = out
            out = None
            for g in range(SUB):
                x = widen(nat[o * SUB + g, pl.ds(near_y, SUB), :])
                x = shift(x, SUB * g)
                out = x if g == 0 else pick(groups[g], x, out)
            corner[o] = out
            return carry
        lax.fori_loop(0, TILES, body, 0)

    def unpack(own, side, nat, packed, corner, fill, wall, o, carry):
        by = dst8 - (N - H - src8)
        packs, corner_in = [turn(packed[o * PIECES + q], by) for q in range(PIECES)], turn(corner[o], by)
        for pi in range(SUB):
            i, out = o * SUB + pi, []
            plane = widen(own[i, 0:N, :])
            for jt in range(NB):
                if jt < TILES:
                    t = pi * TILES + jt
                    got, g = packs[t // GROUPS], t % GROUPS
                else:
                    got, g = corner_in, pi
                x = plane[SUB * jt:SUB * jt + SUB] if jt < TILES else widen(side[i])
                other = fill if wall is None else pick(at_wall, wall_column(i, jt), fill)
                out.append(pick(own_lane, x, pick(ghost8, shift(got, -SUB * g), other)))
            nat[i, 0:E, :] = jnp.concatenate(out, axis=0)
        return carry

    def wall_column(i, jt):
        at = SUB * jt if jt < TILES else pl.multiple_of(N + 48 * cy, SUB)
        return pltpu.roll(wz_t[pl.ds(at, SUB), :], LANES - UNIT - i, 1)

    for copy in loads[0] + loads[1]:
        copy.wait()
    last_x, last_y, last_z = (N - UNIT) * (1 - cx), (N - UNIT) * (1 - cy), (N - UNIT) * (1 - cz)

    slots = lax.rem(lane + (LANES - last_z), LANES)

    def pack_one(o, carry):
        for n, src in enumerate((k_in, u_in)):
            row_s[n, pl.ds(pl.multiple_of(o * SUB, SUB), SUB), :] = jnp.concatenate(
                [src[o * SUB + r, pl.ds(last_y, 1), :] for r in range(SUB)], axis=0)
            out = None
            for t in range(N):
                if t % TILES == 0:
                    plane = widen(src[o * SUB + t // TILES])
                x = shift(plane[SUB * (t % TILES):SUB * (t % TILES) + SUB], t)
                out = x if t == 0 else pick(slots == t, x, out)
            lane_s[n, o] = out
        return carry
    planes(0, TILES, pack_one, 0, 3)
    pl.semaphore_wait(barrier, len(OTHERS))
    one_x = [send(0, k_in.at[pl.ds(last_x, 1)], kx, (1, 0, 0)), send(1, u_in.at[pl.ds(last_x, 1)], ux, (1, 0, 0))]
    one_y = send(2, row_s, row_r, (0, 1, 0))
    one_z = send(3, lane_s, lane_r, (0, 0, 1))
    k_y = send(4, k_in.at[:, pl.ds(near_y, SUB), :], ky, (0, 1, 0))
    pack(k_in, zs.at[0], ds_.at[0])
    k_z = send(PIECES, zs.at[0], zr.at[0], (0, 0, 1))
    k_d = send(6, ds_.at[0], dr.at[0], (0, 1, 1))

    for n in (3, 4, PIECES):
        loads[n][0].wait()

    def lane_ring(w, at, c):
        left, right = walls[w, pl.ds(at, SUB), 0:LANES], walls[w, pl.ds(at, SUB), LANES:144]
        gap = jnp.zeros((SUB, 56), F32)
        right = jnp.concatenate([gap, right, gap], axis=1)
        turned = jnp.where(jnp.logical_and(lane >= 56, lane < N), right, pltpu.roll(left, 56, 1))
        return jnp.where(c == 0, left, turned)

    for jt in range(NB):
        at_j = pl.multiple_of(N * cy + SUB * jt if jt < TILES else N - H * cy, SUB)
        at_i = pl.multiple_of(N * cx + SUB * jt if jt < TILES else N - H * cx, SUB)
        k_nat[E, pl.ds(SUB * jt, SUB), :] = lane_ring(0, at_j, cz)
        wy[pl.ds(SUB * jt, SUB), :] = lane_ring(1, at_i, cz)
        if jt < TILES:
            wz[pl.ds(SUB * jt, SUB), :] = lane_ring(2, at_i, cy)
    wz_t[...] = turn(wz[...].T, wall_lane + UNIT)

    for copy in loads[2]:
        copy.wait()

    def take_f(p, carry):
        for b in range(NB):
            rows = SUB if b < 2 else LAST
            v0_a[p, b, 0:rows, 0:N] = f_in[p, pl.ds(b, rows, stride=NB), :]
        return carry
    planes(0, N, take_f, 0)

    def lay_out(i, carry):
        side = jnp.concatenate([pick(at_wall, wall_column(i, jt), ones) for jt in range(TILES)], axis=0)
        for nat, src, rest in ((k_nat, k_in, side), (u_nat, u_in, jnp.zeros((N, LANES), F32))):
            nat[i, 0:N, N:] = rest[:, N:]
            nat[i, 0:N, 0:N] = src[i]
        return carry
    planes(0, N, lay_out, 0)

    u_nat[E - UNIT - LAST * cx] = jnp.zeros((E, LANES), F32)
    one_lane = N + 55 * cz
    at_one = lane == one_lane
    for copy in one_x + [one_y, one_z]:
        copy.wait()
    u_nat[N + LAST * cx, 0:N, 0:N] = ux[0]
    k_nat[E + UNIT, 0:N, 0:N] = kx[0]

    def unpack_one(o, carry):
        for n, nat in enumerate((k_nat, u_nat)):
            got = turn(lane_r[n, o], one_lane - (N - 1 - last_z))
            for t in range(N):
                here = nat.at[o * SUB + t // TILES, pl.ds(SUB * (t % TILES), SUB), :]
                pltpu.store(here, shift(got, -t), mask=at_one)
        return carry
    lax.fori_loop(0, TILES, unpack_one, 0)

    row0 = sub == 0
    row72 = sub == LAST

    def divergence(h_x, h_xn, h_y, h_z, v, v_prev, v_next, low_row, high_row):
        low = row_down(v)
        high = v
        if low_row is not None:
            low = replace(low, 0, row0, low_row)
            high = replace(v, 2, row72, high_row)
        else:
            low = replace(low, 0, jnp.logical_and(row0, cy == 0), ZERO)
            high = replace(v, 2, jnp.logical_and(row72, cy == 1), ZERO)
        f_y = h_y * (high - low)
        f_z = h_z * (v - lane_down(v))
        return ((h_x * (v - v_prev) - h_xn * (v_next - v)) + (f_y - row_up(f_y))) + (f_z - lane_up(f_z))

    def full(row):
        return jnp.broadcast_to(widen(row), (SUB, LANES))

    def add_up(h_x, h_xn, h_y, h_z):
        return ((h_x + h_xn) + (h_y + row_up(h_y))) + (h_z + lane_up(h_z))

    def start_own(n, carry):
        p0 = WIDTH * n
        first_trip, last_trip = n == 0, n == N // WIDTH - UNIT
        k_p = [load_chunk(k_nat, jnp.where(first_trip, E + cx, p0 - UNIT))]
        u_p = [load_chunk(u_nat, jnp.where(first_trip, E - UNIT, p0 - UNIT))]
        for w in range(WIDTH):
            k_p.append(load_chunk(k_nat, p0 + w))
            u_p.append(load_chunk(u_nat, p0 + w))
        k_p.append(load_chunk(k_nat, jnp.where(last_trip, E + UNIT - cx, p0 + WIDTH)))
        u_p.append(load_chunk(u_nat, p0 + WIDTH))
        h_x = [harmonic(k_p[w + UNIT], k_p[w]) for w in range(WIDTH + UNIT)]
        for w in range(WIDTH):
            p, kc = p0 + w, k_p[w + UNIT]
            wall, got = full(wy[pl.ds(p, 1), :]), full(row_r[0, pl.ds(p, 1), :])
            low = replace(row_down(kc), 0, row0, jnp.where(cy == 0, wall, got))
            high = replace(kc, 2, row72, jnp.where(cy == 0, got, wall))
            h_y = harmonic(high, low)
            h_z = harmonic(kc, lane_down(kc))
            inv = lax.rsqrt(add_up(h_x[w], h_x[w + UNIT], h_y, h_z))
            got = full(row_r[1, pl.ds(p, 1), :])
            a_u = divergence(h_x[w], h_x[w + UNIT], h_y, h_z, u_p[w + UNIT], u_p[w], u_p[w + 2],
                             jnp.where(cy == 0, ZERO, got), jnp.where(cy == 0, got, ZERO))
            y0 = (v0_a[p] - a_u) * inv
            for b in range(NB):
                v0_a[p, b] = y0[b] if b < 2 else pick(row72, zero, y0[b])
            z0 = y0 * inv
            for b in range(NB):
                if b < 2:
                    z_nat[p, pl.ds(b, SUB, stride=NB), :] = z0[b]
                else:
                    z_nat[p, pl.ds(b, LAST, stride=NB), :] = z0[b, :LAST]
        return carry
    lax.fori_loop(0, N // WIDTH, start_own, 0)

    z_y = send(LAST, z_nat.at[pl.ds(0, N), pl.ds(near_y, SUB), :], z_nat.at[pl.ds(0, N), pl.ds(N, SUB), :], (0, 1, 0))
    pack(z_nat, zs.at[1], ds_.at[1])
    z_z = send(8, zs.at[1], zr.at[1], (0, 0, 1))
    z_d = send(9, ds_.at[1], dr.at[1], (0, 1, 1))

    def spread(n, nat, take):
        take(SUB * (1 - cx), 0)
        copy = send(n, nat.at[pl.ds(near_x, SUB)], nat.at[pl.ds(N, SUB)], (1, 0, 0))
        lax.fori_loop(0, SUB, lambda o, carry: take(o + cx, carry), 0)
        return copy

    for copy in (k_y, k_z, k_d):
        copy.wait()
    spread(NB, k_nat, functools.partial(unpack, k_in, ky, k_nat, zr.at[0], dr.at[0], ones, wz_t)).wait()

    def faces(p, carry):
        kc = load_chunk(k_nat, p)
        before = jnp.where(jnp.logical_and(p == 0, cx == 0), E, jnp.where(p == 0, E - UNIT, p - UNIT))
        here = jnp.where(jnp.logical_and(p == N, cx == 1), E, p)
        cx_a[p] = harmonic(load_chunk(k_nat, here), load_chunk(k_nat, before))
        wall = full(wy[pl.ds(p, 1), :])
        low = replace(row_down(kc), 0, jnp.logical_and(row0, cy == 0), wall)
        high = replace(kc, 2, jnp.logical_and(row72, cy == 1), wall)
        cy_a[p] = harmonic(high, low)
        cz_a[p] = harmonic(kc, lane_down(kc))
        return carry
    planes(0, E, faces, 0, SUB)
    cx_a[E] = cx_a[0]
    cx_a[E + UNIT] = cx_a[1]

    def scales(own, p, carry):
        d = add_up(cx_a[p], cx_a[p + UNIT], cy_a[p], cz_a[p])
        inv = lax.rsqrt(d)
        isd_a[p] = inv
        if own:
            sd = d * inv
            for b in range(NB):
                k_nat[p, pl.ds(SUB * b, SUB), :] = sd[b] if b < 2 else pick(row72, zero, sd[b])
        return carry
    planes(0, N, functools.partial(scales, True), 0, SUB)
    planes(N, E, functools.partial(scales, False), 0, SUB)

    for copy in (z_y, z_z, z_d):
        copy.wait()
    z_x = spread(11, z_nat, functools.partial(unpack, z_nat, z_nat.at[:, pl.ds(N, SUB), :], z_nat, zr.at[1], dr.at[1],
                                              zero, None))

    def column(ref, p, b, width):
        return ref[pl.ds(p, width), b]

    def z_column(p, b, width=1):
        return z_nat[pl.ds(p, width), pl.ds(b, SUB, stride=NB), :]

    def tally(carry, b, products):
        return [c + jnp.sum(products[n // 2], axis=0) if n % 2 == (b > 1) else c for n, c in enumerate(carry)]

    def first(own, width, p, carry, before=None, after=None, x_after=None):
        before = p - UNIT if before is None else before
        z, inv, low, f_y, h_y = {}, {}, {}, {}, {}

        def load(b):
            z[b], inv[b], h_y[b] = z_column(p, b, width), column(isd_a, p, b, width), column(cy_a, p, b, width)
            under = z[b - UNIT] if b else pltpu.roll(z_column(p, NB - UNIT, width), 1, 1)
            over = z[b]
            if b == 0:
                under = jnp.where(jnp.logical_and(row0, cy == 0), ZERO, under)
            if b == 2:
                over = jnp.where(jnp.logical_and(row72, cy == 1), ZERO, over)
            f_y[b] = h_y[b] * (over - under)
        carry = list(carry)
        load(0)
        for b in range(NB):
            if b < NB - UNIT:
                load(b + UNIT)
            up = f_y[b + UNIT] if b < NB - UNIT else pltpu.roll(f_y[0], LAST, 1)
            z_p = z_column(before, b)
            z_n = z_column(p + width if after is None else after, b)
            if isinstance(p, int) and p == 0:
                z_p = jnp.where(cx == 0, ZERO, z_p)
            if isinstance(p, int) and p == N - UNIT:
                z_n = jnp.where(cx == 1, ZERO, z_n)
            if x_after is None:
                h_x = column(cx_a, p, b, width + UNIT)
            else:
                h_x = jnp.concatenate([column(cx_a, p, b, 1), column(cx_a, x_after, b, 1)], axis=0)
            f_x = h_x * (jnp.concatenate([z[b], z_n], axis=0) - jnp.concatenate([z_p, z[b]], axis=0))
            h_z = column(cz_a, p, b, width)
            f_z = h_z * (z[b] - lane_down(z[b]))
            b0 = inv[b] * (((f_x[:width] - f_x[1:]) + (f_y[b] - up)) + (f_z - lane_up(f_z)))
            b_a[0][pl.ds(p + UNIT, width), b] = b0
            twice = TWO * inv[b]
            side = column(isd_a, before, b, 1)
            if width > 1:
                side = jnp.concatenate([side, inv[b][:width - UNIT]], axis=0)
            cx_a[pl.ds(p, width), b] = h_x[:width] * (twice * side)
            side = inv[b - UNIT] if b else pltpu.roll(column(isd_a, p, NB - UNIT, width), 1, 1)
            c_y = h_y[b] * (twice * side)
            if b == 0:
                c_y = jnp.where(jnp.logical_and(row0, cy == 0), ZERO, c_y)
            if b == 2:
                c_y = jnp.where(jnp.logical_and(row72, cy == 1), ZERO, c_y)
            cy_a[pl.ds(p, width), b] = c_y
            cz_a[pl.ds(p, width), b] = jnp.where(at_edge, ZERO, h_z * (twice * lane_down(inv[b])))
            if own:
                v0 = column(v0_a, p, b, width)
                carry = tally(carry, b, (v0 * v0, v0 * b0, b0 * b0))
        return tuple(carry)

    at_edge = lane == N * cz

    def wrap(ref):
        ref[0] = ref[E]
        ref[E + UNIT] = ref[1]

    sums = lax.fori_loop(0, 14, lambda n, carry: first(True, PIECES, 1 + PIECES * n, carry), (zero,) * 6)
    z_x.wait()
    sums = first(True, 1, 0, sums, E - UNIT, None, E + UNIT)
    sums = first(True, 1, N - UNIT, sums)
    first(False, WIDTH, N, ())
    first(False, WIDTH, N + WIDTH, (), None, 0)
    cx_a[0] = jnp.where(cx == 0, ZERO, cx_a[0])
    cx_a[N] = jnp.where(cx == 1, ZERO, cx_a[N])
    cx_a[E] = cx_a[0]
    wrap(b_a[0])
    acc[0] = own_cells(sums[0], sums[1])
    acc[1] = own_cells(sums[2], sums[3])
    acc[TILES] = own_cells(sums[4], sums[PIECES])
    acc[23] = zero

    def advance(k, own, width, p, carry):
        old, carry = b_a[k - UNIT], list(carry)
        v_low = pltpu.roll(column(old, p + UNIT, NB - UNIT, width), 1, 1)
        v, c_y = column(old, p + UNIT, 0, width), column(cy_a, p, 0, width)
        t_first = c_y * v
        for b in range(NB):
            if b < NB - UNIT:
                v_high, c_high = column(old, p + UNIT, b + UNIT, width), column(cy_a, p, b + UNIT, width)
                t_high = c_high * v_high
            else:
                t_high = pltpu.roll(t_first, LAST, 1)
            c_x, c_z = column(cx_a, p, b, width + UNIT), column(cz_a, p, b, width)
            below, above = column(old, p, b, 1), column(old, p + width + UNIT, b, 1)
            if width > 1:
                below = jnp.concatenate([below, v[:width - UNIT]], axis=0)
                above = jnp.concatenate([v[1:], above], axis=0)
            new = c_x[:width] * below + c_x[1:] * above
            new = new + (c_y * v_low + t_high)
            new = new + (c_z * lane_down(v) + lane_up(c_z * v))
            new = HALF * new if k == 1 else new - column(b_a[k - 2], p + UNIT, b, width)
            b_a[k][pl.ds(p + UNIT, width), b] = new
            if own:
                carry = tally(carry, b, (column(v0_a, p, b, width) * new, v * new, new * new))
            v_low, v, c_y = v, v_high, c_high
        return tuple(carry)

    for k in range(1, STEPS):
        sums = lax.fori_loop(0, N // SUB, lambda n, carry: advance(k, True, SUB, SUB * n, carry), (zero,) * 6)
        if k < STEPS - UNIT:
            advance(k, False, SUB, N, ())
            wrap(b_a[k])
        acc[1 + k] = own_cells(sums[0], sums[1])
        acc[GROUPS + k - UNIT] = own_cells(sums[2], sums[3])
        if k < STEPS - UNIT:
            acc[TILES + k] = own_cells(sums[4], sums[PIECES])

    def gather(buf, n_sem):
        copies = []
        for n, flips in enumerate(OTHERS):
            copies.append(pltpu.make_async_remote_copy(
                src_ref=buf.at[me], dst_ref=buf.at[me], send_sem=all_send.at[n_sem, n], recv_sem=all_recv.at[n_sem, n],
                device_id=peer(*flips), device_id_type=MESH))
        for copy in copies:
            copy.start()
        return copies

    hi = acc[:, 0, :]
    lo = jnp.zeros((NDOT, LANES), F32)
    for s in range(1, SUB):
        hi, err = two_sum(hi, acc[:, s, :])
        lo = lo + err
    gath[me, 0:NDOT] = hi
    gath[me, NDOT:2 * NDOT] = lo
    gath_copies = gather(gath, 0)
    pair = {}
    for i in range(HEAD + UNIT):
        for j in range(i, HEAD + UNIT):
            pair[i, j] = len(pair)

    def products(n, carry):
        p, carry = WIDTH * n, list(carry)
        for b in range(NB):
            sd = k_nat[pl.ds(p, WIDTH), pl.ds(SUB * b, SUB), :]
            w = [sd * column(v0_a, p, b, WIDTH)] + [sd * column(b_a[j], p + UNIT, b, WIDTH) for j in range(HEAD)]
            for (i, j), at in pair.items():
                carry[at] = carry[at] + jnp.sum(w[i] * w[j], axis=0)
        return tuple(carry)
    gram = lax.fori_loop(0, N // WIDTH, products, (zero,) * len(pair))
    for copy in gath_copies:
        copy.wait()
    hi, lo = gath[0, 0:NDOT], gath[0, NDOT:2 * NDOT]
    for dev in range(1, SUB):
        hi, err = two_sum(hi, gath[dev, 0:NDOT])
        lo = lo + (gath[dev, NDOT:2 * NDOT] + err)
    for shift in (64, 32, GROUPS, SUB, 4, 2, 1):
        hi, err = two_sum(hi, pltpu.roll(hi, shift, 1))
        lo = (lo + pltpu.roll(lo, shift, 1)) + err
    hi, lo = quick(hi, lo)
    size = hi[0:1]
    factor = jnp.where(size > 1e30, TWO ** -110, jnp.where(size > 1e12, TWO ** -60, jnp.where(
        size < 1e-30, TWO ** 110, jnp.where(size < 1e-12, TWO ** 60, ONE)))).astype(F32)
    hi, lo = hi * factor, lo * factor

    def total(row):
        return jnp.broadcast_to(hi[row:row + UNIT], (SUB, LANES)), jnp.broadcast_to(lo[row:row + UNIT], (SUB, LANES))

    n_mom = [total(TILES), total(GROUPS)]
    for j in range(1, LAST):
        n_mom.append(dsub(dscale(total(TILES + j), TWO), n_mom[0]))
        n_mom.append(dsub(dscale(total(GROUPS + j), TWO), n_mom[1]))
    l_mom = [total(1 + j) for j in range(SUB)]
    for j in range(LAST, 14):
        l_mom.append(dsub(dscale(dsub(l_mom[j], n_mom[j]), TWO), l_mom[j - UNIT]))
    m_mom = [total(0)]
    m_mom.append(dsub(m_mom[0], l_mom[0]))
    for j in range(1, 15):
        m_mom.append(dsub(dscale(dsub(m_mom[j], l_mom[j]), TWO), m_mom[j - UNIT]))
    ys, xs = basis_coefs(*step_lengths(m_mom))
    slot = {}
    for t in range(STEPS):
        for j in range(t + UNIT):
            slot[t, j] = len(slot)
            coef[slot[t, j]] = ys[t][1 + j]
    for j in range(SUB):
        slot['x', j] = len(slot)
        coef[slot['x', j]] = xs[j]

    def put(ref, p, b0, val):
        for b in range(val.shape[0]):
            if b0 + b < 2:
                ref[p, pl.ds(b0 + b, SUB, stride=NB), :] = val[b, :, :N]
            else:
                ref[p, pl.ds(b0 + b, LAST, stride=NB), :] = val[b, :LAST, :N]

    def residuals(p, carry):
        carry = list(carry)
        for b0 in range(0, NB, 2):
            cut = pl.ds(b0, 2)
            v0 = v0_a[p, cut]
            sd = jnp.stack([k_nat[p, pl.ds(SUB * (b0 + b), SUB), :] for b in range(2)], axis=0)
            bs = [ref[p + UNIT, cut] for ref in b_a]
            for t in range(HEAD, STEPS):
                y = v0
                for j in range(t + UNIT):
                    y = y + coef[slot[t, j]] * bs[j]
                r = sd * y
                which = 2 * (t - HEAD) + (b0 > 0)
                carry[which] = carry[which] + jnp.sum(r * r, axis=0)
                if t == STEPS - UNIT:
                    put(f_in, p, b0, r)
        return tuple(carry)

    sums = lax.fori_loop(0, N, residuals, (zero,) * (2 * (STEPS - HEAD)))
    for t in range(STEPS):
        if t < HEAD:
            form = zero
            g = [None] + [coef[slot[t, j]] for j in range(t + 1)]
            for i in range(t + 2):
                part = gram[pair[0, i]] if not i else g[i] * gram[pair[0, i]]
                form = form + (part if not i else part + part)
            for i in range(UNIT, t + 2):
                part = zero
                for j in range(UNIT, t + 2):
                    part = part + g[j] * gram[pair[min(i, j), max(i, j)]]
                form = form + g[i] * part
            rsend[t] = pick(own_lane, form, zero)
        else:
            rsend[t] = own_cells(sums[2 * (t - HEAD)], sums[2 * (t - HEAD) + UNIT])
    part = rsend[:, 0, :]
    for s in range(1, SUB):
        part = part + rsend[:, s, :]
    rgath[me] = part
    rr_copies = gather(rgath, 1)

    def update(p, carry):
        for b0 in range(0, NB, 2):
            cut = pl.ds(b0, 2)
            x = coef[slot['x', 0]] * v0_a[p, cut]
            for j in range(1, SUB):
                x = x + coef[slot['x', j]] * b_a[j - UNIT][p + UNIT, cut]
            x = x * isd_a[p, cut]
            u = jnp.stack([u_nat[p, pl.ds(b0 + b, SUB, stride=NB), :] for b in range(2)], axis=0)
            put(k_in, p, b0, u + x)
        return carry

    lax.fori_loop(0, N, update, 0)
    for copy in rr_copies:
        copy.wait()
    part = rgath[0]
    for dev in range(1, SUB):
        part = part + rgath[dev]
    part = jnp.broadcast_to(jnp.sum(part, axis=1, keepdims=True), (SUB, LANES))
    rr_ref[...] = jnp.sum(jnp.where(lane == sub, part, ZERO), axis=0, keepdims=True)[:, :STEPS]


def solution(mesh):
    spec = P('gx', 'gy', 'gz')

    def local(k_cell, k_ghost, f_rhs, u_init):
        big = (E, NB, SUB, LANES)
        ext = (E + 2, NB, SUB, LANES)
        vm = lambda *shape: pltpu.VMEM(shape, F32)
        any_spec = pl.BlockSpec(memory_space=pl.ANY)
        u, r, rr = pl.pallas_call(
            kernel,
            out_shape=(vm(N, N, N), vm(N, N, N), vm(1, STEPS)),
            in_specs=[any_spec] * 4,
            out_specs=[pl.BlockSpec(memory_space=pltpu.VMEM)] * 3,
            scratch_shapes=[
                vm(N, N, N), vm(E + 2, E, LANES), vm(E, E, LANES), vm(E, E, LANES),
                vm(*ext), vm(*big), vm(*big), vm(*big), vm(N, NB, SUB, LANES),
                *[vm(E + 2, NB, SUB, LANES)] * STEPS,
                vm(3, 144, 144), vm(LANES, LANES), vm(LANES, LANES), vm(E, LANES), vm(N, SUB, N), vm(1, N, N), vm(1, N, N),
                vm(2, 45, SUB, LANES), vm(2, 45, SUB, LANES), vm(2, TILES, SUB, LANES), vm(2, TILES, SUB, LANES),
                vm(2, N, N), vm(2, N, N), vm(2, TILES, SUB, LANES), vm(2, TILES, SUB, LANES),
                vm(NDOT, SUB, LANES), vm(SUB, 2 * NDOT, LANES), vm(SUB, SUB, LANES), vm(SUB, SUB, LANES), vm(44, SUB, LANES),
                pltpu.SemaphoreType.DMA((6, 3)),
                pltpu.SemaphoreType.DMA((12,)), pltpu.SemaphoreType.DMA((12,)),
                pltpu.SemaphoreType.DMA((2, LAST)), pltpu.SemaphoreType.DMA((2, LAST)),
            ],
            compiler_params=pltpu.CompilerParams(collective_id=0, has_side_effects=True, vmem_limit_bytes=57 << 20),
        )(k_cell, f_rhs, u_init, k_ghost)
        return u, r, rr.reshape(STEPS)

    return jax.shard_map(local, mesh=mesh, in_specs=(spec, P(), spec, spec), out_specs=(spec, spec, P()), check_vma=False)
```

```python
import functools

import jax
import jax.numpy as jnp
from jax import lax
from jax.experimental import pallas as pl
from jax.experimental.pallas import tpu as pltpu
from jax.sharding import PartitionSpec as P


N = 72
H = 8
E = N + H
NB = 10
STEPS = 8
MESH = pl.DeviceIdType.MESH
F32 = jnp.float32
OTHERS = [(fx, fy, fz) for fx in (0, 1) for fy in (0, 1) for fz in (0, 1) if fx or fy or fz]
NDOT = 24
SUB = 8
LANES = 128
TILES = 9
PART = 24
WIDTH = 4
LAST = 7
GROUPS = 16
PIECES = 5
ZERO, ONE, HALF, TWO = 0.0, 1.0, 0.5, 2.0
UNIT = 1
HEAD = 4


def iota(axis):
    return lax.broadcasted_iota(jnp.int32, (SUB, LANES), axis)


def two_sum(a, b):
    s = a + b
    t = s - a
    return s, (a - (s - t)) + (b - t)


def quick(a, b):
    s = a + b
    return s, b - (s - a)


def two_prod(a, b):
    def split(x):
        t = x * 4097.0
        hi = t - (t - x)
        return hi, x - hi
    p = a * b
    ah, al = split(a)
    bh, bl = split(b)
    return p, ((ah * bh - p) + ah * bl + al * bh) + al * bl


def dadd(x, y):
    (xh, xl), (yh, yl) = x, y
    s, e = two_sum(xh, yh)
    return quick(s, e + (xl + yl))


def dsub(x, y):
    yh, yl = y
    return dadd(x, (-yh, -yl))


def dscale(x, c):
    hi, lo = x
    return hi * c, lo * c


def dmul(x, y):
    (xh, xl), (yh, yl) = x, y
    p, e = two_prod(xh, yh)
    return quick(p, e + (xh * yl + xl * yh))


def ddiv(x, y):
    (xh, xl), (yh, yl) = x, y
    q = xh / yh
    p, e = two_prod(q, yh)
    rest = ((xh - p) - e) + (xl - q * yl)
    return quick(q, rest / yh)


def step_lengths(m):
    alphas, betas = [], []
    y = dict(enumerate(m))
    p = {0: dsub(y[0], y[1])}
    for l in range(1, 15):
        p[l] = dsub(y[l], dscale(dadd(y[l + UNIT], y[l - UNIT]), HALF))
    for t in range(STEPS):
        alpha = ddiv(y[t], p[t])
        alphas.append(alpha[0])
        if t == STEPS - UNIT:
            break
        y_next = {l: dsub(y[l], dmul(alpha, p[l])) for l in range(t + UNIT, 15 - t)}
        beta = ddiv(y_next[t + UNIT], p[t])
        if t:
            beta = dscale(beta, HALF)
        betas.append(beta[0])
        p_next = {}
        for l in range(t + UNIT, 14 - t):
            side = y_next[l + UNIT] if l == t + UNIT else dadd(y_next[l + UNIT], y_next[l - UNIT])
            p_next[l] = dadd(dsub(y_next[l], dscale(side, HALF)), dmul(beta, p[l]))
        y, p = y_next, p_next
    return alphas, betas


def basis_coefs(alphas, betas):
    def add(a, b):
        return b if a is None else (a if b is None else a + b)

    def axpy(x, c, y):
        return [xi if yi is None else (c * yi if xi is None else xi + c * yi) for xi, yi in zip(x, y)]

    def apply_op(v):
        out = [None] * 11
        out[1] = v[0]
        for j in range(SUB):
            if v[1 + j] is None:
                continue
            c = v[1 + j]
            out[1 + j] = add(out[1 + j], c)
            if j == 0:
                out[2] = add(out[2], -c)
            else:
                half = -HALF * c
                out[2 + j] = add(out[2 + j], half)
                out[j] = add(out[j], half)
        return out[:TILES]

    one = jnp.ones_like(alphas[0])
    y = [one] + [None] * SUB
    p = list(y)
    x = [None] * TILES
    ys = []
    for t in range(STEPS):
        q = apply_op(p)
        x = axpy(x, alphas[t], p)
        y = axpy(y, -alphas[t], q)
        ys.append(y)
        if t < STEPS - UNIT:
            p = axpy(y, betas[t], p)
    return ys, x


def row_down(v):
    return jnp.concatenate([pltpu.roll(v[NB - UNIT], 1, 0)[None], v[:NB - UNIT]], axis=0)


def row_up(v):
    return jnp.concatenate([v[1:], pltpu.roll(v[0], LAST, 0)[None]], axis=0)


def lane_down(v):
    return pltpu.roll(v, 1, 2)


def lane_up(v):
    return pltpu.roll(v, 127, 2)


def load_chunk(ref, plane):
    return jnp.stack([ref[plane, pl.ds(b, SUB, stride=NB), :] for b in range(NB)], axis=0)


def replace(v, b, mask, value):
    return jnp.concatenate(([v[:b]] if b else []) + [jnp.where(mask, value, v[b])[None], v[b + UNIT:]], axis=0)


def harmonic(a, b):
    return TWO * a * b / (a + b)


def pick(mask, a, b):
    return lax.select_n(mask, b, a)


def planes(lo, hi, body, init, width=WIDTH):
    def some(n, carry):
        for w in range(width):
            carry = body(lo + n * width + w, carry)
        return carry
    return lax.fori_loop(0, (hi - lo) // width, some, init)


def own_cells(low, high):
    sub, lane = iota(0), iota(1)
    return jnp.where(lane < N, low + jnp.where(sub < LAST, high, ZERO), ZERO)


def kernel(k_hbm, f_hbm, u_hbm, kg_hbm, k_in, f_in, rr_ref,
           u_in, k_nat, u_nat, z_nat, cx_a, cy_a, cz_a, isd_a, v0_a, b0_a, b1_a, b2_a, b3_a, b4_a, b5_a, b6_a, b7_a,
           walls, wz, wz_t, wy, ky, kx, ux, zs, zr, ds_, dr, row_s, row_r, lane_s, lane_r, acc, gath, rsend, rgath, coef,
           load_sem, send_sem, recv_sem, all_send, all_recv):
    cx, cy, cz = lax.axis_index('gx'), lax.axis_index('gy'), lax.axis_index('gz')
    me = cx + 2 * cy + 4 * cz
    b_a = (b0_a, b1_a, b2_a, b3_a, b4_a, b5_a, b6_a, b7_a)
    lane, sub = iota(1), iota(0)

    def peer(fx, fy, fz):
        out = {}
        if fx:
            out['gx'] = 1 - cx
        if fy:
            out['gy'] = 1 - cy
        if fz:
            out['gz'] = 1 - cz
        return out

    loads = []
    for n, (src, dst) in enumerate([(k_hbm, k_in), (u_hbm, u_in), (f_hbm, f_in)]):
        loads.append([pltpu.make_async_copy(src.at[pl.ds(PART * q, PART)], dst.at[pl.ds(PART * q, PART)], load_sem.at[n, q])
                      for q in range(N // PART)])
    loads.append([pltpu.make_async_copy(kg_hbm.at[cx], walls.at[0], load_sem.at[3, 0])])
    loads.append([pltpu.make_async_copy(kg_hbm.at[2 + cy], walls.at[1], load_sem.at[4, 0])])
    loads.append([pltpu.make_async_copy(kg_hbm.at[4 + cz], walls.at[2], load_sem.at[PIECES, 0])])
    for n in (0, 1, 3, 4, PIECES, 2):
        for copy in loads[n]:
            copy.start()

    barrier = pltpu.get_barrier_semaphore()
    for flips in OTHERS:
        pl.semaphore_signal(barrier, inc=1, device_id=peer(*flips), device_id_type=MESH)

    def send(n, src, dst, flips):
        copy = pltpu.make_async_remote_copy(src_ref=src, dst_ref=dst, send_sem=send_sem.at[n], recv_sem=recv_sem.at[n],
                                            device_id=peer(*flips), device_id_type=MESH)
        copy.start()
        return copy

    near_y = pl.multiple_of((N - H) * (1 - cy), SUB)
    near_x = (N - H) * (1 - cx)
    src8 = (N - H) * (1 - cz)
    dst8 = N + 48 * cz
    ghost8 = jnp.logical_and(lane >= dst8, lane < dst8 + SUB)
    wall_lane = 127 - 55 * cz
    own_lane = lane < N
    at_wall = lane == wall_lane
    zero = jnp.zeros((SUB, LANES), F32)
    ones = jnp.ones((SUB, LANES), F32)

    def turn(x, by):
        return pltpu.roll(x, lax.rem(by + LANES, LANES), 1)

    def shift(x, by):
        return pltpu.roll(x, by % LANES, 1) if by % LANES else x

    def widen(x):
        return x if x.shape[1] == LANES else jnp.concatenate([x, jnp.zeros((x.shape[0], LANES - x.shape[1]), F32)], axis=1)

    def pack(nat, packed, corner, lo, hi):
        group8 = lax.rem(lane + (LANES - src8), LANES) // SUB
        groups = [group8 == g for g in range(GROUPS)]

        def body(o, carry):
            for q in range(PIECES):
                out = None
                for g in range(min(GROUPS, N - GROUPS * q)):
                    t = GROUPS * q + g
                    if t % TILES == 0:
                        plane = widen(nat[o * SUB + t // TILES, 0:N, :])
                    x = shift(plane[SUB * (t % TILES):SUB * (t % TILES) + SUB], SUB * g)
                    out = x if g == 0 else pick(groups[g], x, out)
                packed[o * PIECES + q] = out
            out = None
            for g in range(SUB):
                x = widen(nat[o * SUB + g, pl.ds(near_y, SUB), :])
                x = shift(x, SUB * g)
                out = x if g == 0 else pick(groups[g], x, out)
            corner[o] = out
            return carry
        lax.fori_loop(lo, hi, body, 0)

    def unpack(own, side, nat, packed, corner, fill, wall, o, carry):
        by = dst8 - (N - H - src8)
        packs, corner_in = [turn(packed[o * PIECES + q], by) for q in range(PIECES)], turn(corner[o], by)
        for pi in range(SUB):
            i, out = o * SUB + pi, []
            plane = widen(own[i, 0:N, :])
            for jt in range(NB):
                if jt < TILES:
                    t = pi * TILES + jt
                    got, g = packs[t // GROUPS], t % GROUPS
                else:
                    got, g = corner_in, pi
                x = plane[SUB * jt:SUB * jt + SUB] if jt < TILES else widen(side[i])
                other = fill if wall is None else pick(at_wall, wall_column(i, jt), fill)
                out.append(pick(own_lane, x, pick(ghost8, shift(got, -SUB * g), other)))
            nat[i, 0:E, :] = jnp.concatenate(out, axis=0)
        return carry

    def wall_column(i, jt):
        at = SUB * jt if jt < TILES else pl.multiple_of(N + 48 * cy, SUB)
        return pltpu.roll(wz_t[pl.ds(at, SUB), :], LANES - UNIT - i, 1)

    for copy in loads[0] + loads[1]:
        copy.wait()
    last_x, last_y, last_z = (N - UNIT) * (1 - cx), (N - UNIT) * (1 - cy), (N - UNIT) * (1 - cz)

    slots = lax.rem(lane + (LANES - last_z), LANES)

    def pack_one(o, carry):
        for n, src in enumerate((k_in, u_in)):
            row_s[n, pl.ds(pl.multiple_of(o * SUB, SUB), SUB), :] = jnp.concatenate(
                [src[o * SUB + r, pl.ds(last_y, 1), :] for r in range(SUB)], axis=0)
            out = None
            for t in range(N):
                if t % TILES == 0:
                    plane = widen(src[o * SUB + t // TILES])
                x = shift(plane[SUB * (t % TILES):SUB * (t % TILES) + SUB], t)
                out = x if t == 0 else pick(slots == t, x, out)
            lane_s[n, o] = out
        return carry
    planes(0, TILES, pack_one, 0, 3)
    pl.semaphore_wait(barrier, len(OTHERS))
    one_x = [send(0, k_in.at[pl.ds(last_x, 1)], kx, (1, 0, 0)), send(1, u_in.at[pl.ds(last_x, 1)], ux, (1, 0, 0))]
    one_y = send(2, row_s, row_r, (0, 1, 0))
    one_z = send(3, lane_s, lane_r, (0, 0, 1))
    k_y = send(4, k_in.at[:, pl.ds(near_y, SUB), :], ky, (0, 1, 0))
    pack(k_in, zs.at[0], ds_.at[0], 0, TILES)
    k_z = send(PIECES, zs.at[0], zr.at[0], (0, 0, 1))
    k_d = send(6, ds_.at[0], dr.at[0], (0, 1, 1))

    for n in (3, 4, PIECES):
        loads[n][0].wait()

    def lane_ring(w, at, c):
        left, right = walls[w, pl.ds(at, SUB), 0:LANES], walls[w, pl.ds(at, SUB), LANES:144]
        gap = jnp.zeros((SUB, 56), F32)
        right = jnp.concatenate([gap, right, gap], axis=1)
        turned = jnp.where(jnp.logical_and(lane >= 56, lane < N), right, pltpu.roll(left, 56, 1))
        return jnp.where(c == 0, left, turned)

    for jt in range(NB):
        at_j = pl.multiple_of(N * cy + SUB * jt if jt < TILES else N - H * cy, SUB)
        at_i = pl.multiple_of(N * cx + SUB * jt if jt < TILES else N - H * cx, SUB)
        k_nat[E, pl.ds(SUB * jt, SUB), :] = lane_ring(0, at_j, cz)
        wy[pl.ds(SUB * jt, SUB), :] = lane_ring(1, at_i, cz)
        if jt < TILES:
            wz[pl.ds(SUB * jt, SUB), :] = lane_ring(2, at_i, cy)
    wz_t[...] = turn(wz[...].T, wall_lane + UNIT)

    for copy in loads[2]:
        copy.wait()

    def take_f(p, carry):
        for b in range(NB):
            rows = SUB if b < 2 else LAST
            v0_a[p, b, 0:rows, 0:N] = f_in[p, pl.ds(b, rows, stride=NB), :]
        return carry
    planes(0, N, take_f, 0)

    def lay_out(i, carry):
        side = jnp.concatenate([pick(at_wall, wall_column(i, jt), ones) for jt in range(TILES)], axis=0)
        for nat, src, rest in ((k_nat, k_in, side), (u_nat, u_in, jnp.zeros((N, LANES), F32))):
            nat[i, 0:N, N:] = rest[:, N:]
            nat[i, 0:N, 0:N] = src[i]
        return carry
    planes(0, N, lay_out, 0)

    u_nat[E - UNIT - LAST * cx] = jnp.zeros((E, LANES), F32)
    one_lane = N + 55 * cz
    at_one = lane == one_lane
    for copy in one_x + [one_y, one_z]:
        copy.wait()
    u_nat[N + LAST * cx, 0:N, 0:N] = ux[0]
    k_nat[E + UNIT, 0:N, 0:N] = kx[0]

    def unpack_one(o, carry):
        for n, nat in enumerate((k_nat, u_nat)):
            got = turn(lane_r[n, o], one_lane - (N - 1 - last_z))
            for t in range(N):
                here = nat.at[o * SUB + t // TILES, pl.ds(SUB * (t % TILES), SUB), :]
                pltpu.store(here, shift(got, -t), mask=at_one)
        return carry
    lax.fori_loop(0, TILES, unpack_one, 0)

    row0 = sub == 0
    row72 = sub == LAST

    def divergence(h_x, h_xn, h_y, h_z, v, v_prev, v_next, low_row, high_row):
        low = row_down(v)
        high = v
        if low_row is not None:
            low = replace(low, 0, row0, low_row)
            high = replace(v, 2, row72, high_row)
        else:
            low = replace(low, 0, jnp.logical_and(row0, cy == 0), ZERO)
            high = replace(v, 2, jnp.logical_and(row72, cy == 1), ZERO)
        f_y = h_y * (high - low)
        f_z = h_z * (v - lane_down(v))
        return ((h_x * (v - v_prev) - h_xn * (v_next - v)) + (f_y - row_up(f_y))) + (f_z - lane_up(f_z))

    def full(row):
        return jnp.broadcast_to(widen(row), (SUB, LANES))

    def add_up(h_x, h_xn, h_y, h_z):
        return ((h_x + h_xn) + (h_y + row_up(h_y))) + (h_z + lane_up(h_z))

    def start_own(n, carry):
        p0 = WIDTH * n
        first_trip, last_trip = n == 0, n == N // WIDTH - UNIT
        k_p = [load_chunk(k_nat, jnp.where(first_trip, E + cx, p0 - UNIT))]
        u_p = [load_chunk(u_nat, jnp.where(first_trip, E - UNIT, p0 - UNIT))]
        for w in range(WIDTH):
            k_p.append(load_chunk(k_nat, p0 + w))
            u_p.append(load_chunk(u_nat, p0 + w))
        k_p.append(load_chunk(k_nat, jnp.where(last_trip, E + UNIT - cx, p0 + WIDTH)))
        u_p.append(load_chunk(u_nat, p0 + WIDTH))
        h_x = [harmonic(k_p[w + UNIT], k_p[w]) for w in range(WIDTH + UNIT)]
        for w in range(WIDTH):
            p, kc = p0 + w, k_p[w + UNIT]
            wall, got = full(wy[pl.ds(p, 1), :]), full(row_r[0, pl.ds(p, 1), :])
            low = replace(row_down(kc), 0, row0, jnp.where(cy == 0, wall, got))
            high = replace(kc, 2, row72, jnp.where(cy == 0, got, wall))
            h_y = harmonic(high, low)
            h_z = harmonic(kc, lane_down(kc))
            inv = lax.rsqrt(add_up(h_x[w], h_x[w + UNIT], h_y, h_z))
            got = full(row_r[1, pl.ds(p, 1), :])
            a_u = divergence(h_x[w], h_x[w + UNIT], h_y, h_z, u_p[w + UNIT], u_p[w], u_p[w + 2],
                             jnp.where(cy == 0, ZERO, got), jnp.where(cy == 0, got, ZERO))
            y0 = (v0_a[p] - a_u) * inv
            for b in range(NB):
                v0_a[p, b] = y0[b] if b < 2 else pick(row72, zero, y0[b])
            z0 = y0 * inv
            for b in range(NB):
                if b < 2:
                    z_nat[p, pl.ds(b, SUB, stride=NB), :] = z0[b]
                else:
                    z_nat[p, pl.ds(b, LAST, stride=NB), :] = z0[b, :LAST]
        return carry
    z_copies = []
    for q in range(3):
        lax.fori_loop(6 * q, 6 * q + 6, start_own, 0)
        rows = pl.ds(PART * q, PART)
        z_copies.append(send(7 + q, z_nat.at[rows, pl.ds(near_y, SUB), :], z_nat.at[rows, pl.ds(N, SUB), :], (0, 1, 0)))
        pack(z_nat, zs.at[1], ds_.at[1], 3 * q, 3 * q + 3)
        lanes = pl.ds(15 * q, 15)
        z_copies.append(send(12 + q, zs.at[1, lanes], zr.at[1, lanes], (0, 0, 1)))
    z_copies.append(send(15, ds_.at[1], dr.at[1], (0, 1, 1)))

    def spread(n, nat, take):
        take(SUB * (1 - cx), 0)
        copy = send(n, nat.at[pl.ds(near_x, SUB)], nat.at[pl.ds(N, SUB)], (1, 0, 0))
        lax.fori_loop(0, SUB, lambda o, carry: take(o + cx, carry), 0)
        return copy

    for copy in (k_y, k_z, k_d):
        copy.wait()
    spread(NB, k_nat, functools.partial(unpack, k_in, ky, k_nat, zr.at[0], dr.at[0], ones, wz_t)).wait()

    def faces(p, carry):
        kc = load_chunk(k_nat, p)
        before = jnp.where(jnp.logical_and(p == 0, cx == 0), E, jnp.where(p == 0, E - UNIT, p - UNIT))
        here = jnp.where(jnp.logical_and(p == N, cx == 1), E, p)
        cx_a[p] = harmonic(load_chunk(k_nat, here), load_chunk(k_nat, before))
        wall = full(wy[pl.ds(p, 1), :])
        low = replace(row_down(kc), 0, jnp.logical_and(row0, cy == 0), wall)
        high = replace(kc, 2, jnp.logical_and(row72, cy == 1), wall)
        cy_a[p] = harmonic(high, low)
        cz_a[p] = harmonic(kc, lane_down(kc))
        return carry
    planes(0, E, faces, 0, SUB)
    cx_a[E] = cx_a[0]
    cx_a[E + UNIT] = cx_a[1]

    def scales(own, p, carry):
        d = add_up(cx_a[p], cx_a[p + UNIT], cy_a[p], cz_a[p])
        inv = lax.rsqrt(d)
        isd_a[p] = inv
        if own:
            sd = d * inv
            for b in range(NB):
                k_nat[p, pl.ds(SUB * b, SUB), :] = sd[b] if b < 2 else pick(row72, zero, sd[b])
        return carry
    planes(0, N, functools.partial(scales, True), 0, SUB)
    planes(N, E, functools.partial(scales, False), 0, SUB)

    for copy in z_copies:
        copy.wait()
    z_x = spread(11, z_nat, functools.partial(unpack, z_nat, z_nat.at[:, pl.ds(N, SUB), :], z_nat, zr.at[1], dr.at[1],
                                              zero, None))

    def column(ref, p, b, width):
        return ref[pl.ds(p, width), b]

    def z_column(p, b, width=1):
        return z_nat[pl.ds(p, width), pl.ds(b, SUB, stride=NB), :]

    def tally(carry, b, products):
        return [c + jnp.sum(products[n // 2], axis=0) if n % 2 == (b > 1) else c for n, c in enumerate(carry)]

    def first(own, width, p, carry, before=None, after=None, x_after=None):
        before = p - UNIT if before is None else before
        z, inv, low, f_y, h_y = {}, {}, {}, {}, {}

        def load(b):
            z[b], inv[b], h_y[b] = z_column(p, b, width), column(isd_a, p, b, width), column(cy_a, p, b, width)
            under = z[b - UNIT] if b else pltpu.roll(z_column(p, NB - UNIT, width), 1, 1)
            over = z[b]
            if b == 0:
                under = jnp.where(jnp.logical_and(row0, cy == 0), ZERO, under)
            if b == 2:
                over = jnp.where(jnp.logical_and(row72, cy == 1), ZERO, over)
            f_y[b] = h_y[b] * (over - under)
        carry = list(carry)
        load(0)
        for b in range(NB):
            if b < NB - UNIT:
                load(b + UNIT)
            up = f_y[b + UNIT] if b < NB - UNIT else pltpu.roll(f_y[0], LAST, 1)
            z_p = z_column(before, b)
            z_n = z_column(p + width if after is None else after, b)
            if isinstance(p, int) and p == 0:
                z_p = jnp.where(cx == 0, ZERO, z_p)
            if isinstance(p, int) and p == N - UNIT:
                z_n = jnp.where(cx == 1, ZERO, z_n)
            if x_after is None:
                h_x = column(cx_a, p, b, width + UNIT)
            else:
                h_x = jnp.concatenate([column(cx_a, p, b, 1), column(cx_a, x_after, b, 1)], axis=0)
            f_x = h_x * (jnp.concatenate([z[b], z_n], axis=0) - jnp.concatenate([z_p, z[b]], axis=0))
            h_z = column(cz_a, p, b, width)
            f_z = h_z * (z[b] - lane_down(z[b]))
            b0 = inv[b] * (((f_x[:width] - f_x[1:]) + (f_y[b] - up)) + (f_z - lane_up(f_z)))
            b_a[0][pl.ds(p + UNIT, width), b] = b0
            twice = TWO * inv[b]
            side = column(isd_a, before, b, 1)
            if width > 1:
                side = jnp.concatenate([side, inv[b][:width - UNIT]], axis=0)
            cx_a[pl.ds(p, width), b] = h_x[:width] * (twice * side)
            side = inv[b - UNIT] if b else pltpu.roll(column(isd_a, p, NB - UNIT, width), 1, 1)
            c_y = h_y[b] * (twice * side)
            if b == 0:
                c_y = jnp.where(jnp.logical_and(row0, cy == 0), ZERO, c_y)
            if b == 2:
                c_y = jnp.where(jnp.logical_and(row72, cy == 1), ZERO, c_y)
            cy_a[pl.ds(p, width), b] = c_y
            cz_a[pl.ds(p, width), b] = jnp.where(at_edge, ZERO, h_z * (twice * lane_down(inv[b])))
            if own:
                v0 = column(v0_a, p, b, width)
                carry = tally(carry, b, (v0 * v0, v0 * b0, b0 * b0))
        return tuple(carry)

    at_edge = lane == N * cz

    def wrap(ref):
        ref[0] = ref[E]
        ref[E + UNIT] = ref[1]

    sums = lax.fori_loop(0, 14, lambda n, carry: first(True, PIECES, 1 + PIECES * n, carry), (zero,) * 6)
    z_x.wait()
    sums = first(True, 1, 0, sums, E - UNIT, None, E + UNIT)
    sums = first(True, 1, N - UNIT, sums)
    first(False, WIDTH, N, ())
    first(False, WIDTH, N + WIDTH, (), None, 0)
    cx_a[0] = jnp.where(cx == 0, ZERO, cx_a[0])
    cx_a[N] = jnp.where(cx == 1, ZERO, cx_a[N])
    cx_a[E] = cx_a[0]
    wrap(b_a[0])
    acc[0] = own_cells(sums[0], sums[1])
    acc[1] = own_cells(sums[2], sums[3])
    acc[TILES] = own_cells(sums[4], sums[PIECES])
    acc[23] = zero

    def advance(k, own, width, p, carry):
        old, carry = b_a[k - UNIT], list(carry)
        v_low = pltpu.roll(column(old, p + UNIT, NB - UNIT, width), 1, 1)
        v, c_y = column(old, p + UNIT, 0, width), column(cy_a, p, 0, width)
        t_first = c_y * v
        for b in range(NB):
            if b < NB - UNIT:
                v_high, c_high = column(old, p + UNIT, b + UNIT, width), column(cy_a, p, b + UNIT, width)
                t_high = c_high * v_high
            else:
                t_high = pltpu.roll(t_first, LAST, 1)
            c_x, c_z = column(cx_a, p, b, width + UNIT), column(cz_a, p, b, width)
            below, above = column(old, p, b, 1), column(old, p + width + UNIT, b, 1)
            if width > 1:
                below = jnp.concatenate([below, v[:width - UNIT]], axis=0)
                above = jnp.concatenate([v[1:], above], axis=0)
            new = c_x[:width] * below + c_x[1:] * above
            new = new + (c_y * v_low + t_high)
            new = new + (c_z * lane_down(v) + lane_up(c_z * v))
            new = HALF * new if k == 1 else new - column(b_a[k - 2], p + UNIT, b, width)
            b_a[k][pl.ds(p + UNIT, width), b] = new
            if own:
                carry = tally(carry, b, (column(v0_a, p, b, width) * new, v * new, new * new))
            v_low, v, c_y = v, v_high, c_high
        return tuple(carry)

    for k in range(1, STEPS):
        sums = lax.fori_loop(0, N // SUB, lambda n, carry: advance(k, True, SUB, SUB * n, carry), (zero,) * 6)
        if k < STEPS - UNIT:
            advance(k, False, SUB, N, ())
            wrap(b_a[k])
        acc[1 + k] = own_cells(sums[0], sums[1])
        acc[GROUPS + k - UNIT] = own_cells(sums[2], sums[3])
        if k < STEPS - UNIT:
            acc[TILES + k] = own_cells(sums[4], sums[PIECES])

    def gather(buf, n_sem):
        copies = []
        for n, flips in enumerate(OTHERS):
            copies.append(pltpu.make_async_remote_copy(
                src_ref=buf.at[me], dst_ref=buf.at[me], send_sem=all_send.at[n_sem, n], recv_sem=all_recv.at[n_sem, n],
                device_id=peer(*flips), device_id_type=MESH))
        for copy in copies:
            copy.start()
        return copies

    hi = acc[:, 0, :]
    lo = jnp.zeros((NDOT, LANES), F32)
    for s in range(1, SUB):
        hi, err = two_sum(hi, acc[:, s, :])
        lo = lo + err
    gath[me, 0:NDOT] = hi
    gath[me, NDOT:2 * NDOT] = lo
    gath_copies = gather(gath, 0)
    pair = {}
    for i in range(HEAD + UNIT):
        for j in range(i, HEAD + UNIT):
            pair[i, j] = len(pair)

    def products(n, carry):
        p, carry = WIDTH * n, list(carry)
        for b in range(NB):
            sd = k_nat[pl.ds(p, WIDTH), pl.ds(SUB * b, SUB), :]
            w = [sd * column(v0_a, p, b, WIDTH)] + [sd * column(b_a[j], p + UNIT, b, WIDTH) for j in range(HEAD)]
            for (i, j), at in pair.items():
                carry[at] = carry[at] + jnp.sum(w[i] * w[j], axis=0)
        return tuple(carry)
    gram = lax.fori_loop(0, N // WIDTH, products, (zero,) * len(pair))
    for copy in gath_copies:
        copy.wait()
    hi, lo = gath[0, 0:NDOT], gath[0, NDOT:2 * NDOT]
    for dev in range(1, SUB):
        hi, err = two_sum(hi, gath[dev, 0:NDOT])
        lo = lo + (gath[dev, NDOT:2 * NDOT] + err)
    for shift in (64, 32, GROUPS, SUB, 4, 2, 1):
        hi, err = two_sum(hi, pltpu.roll(hi, shift, 1))
        lo = (lo + pltpu.roll(lo, shift, 1)) + err
    hi, lo = quick(hi, lo)
    size = hi[0:1]
    factor = jnp.where(size > 1e30, TWO ** -110, jnp.where(size > 1e12, TWO ** -60, jnp.where(
        size < 1e-30, TWO ** 110, jnp.where(size < 1e-12, TWO ** 60, ONE)))).astype(F32)
    hi, lo = hi * factor, lo * factor

    def total(row):
        return jnp.broadcast_to(hi[row:row + UNIT], (SUB, LANES)), jnp.broadcast_to(lo[row:row + UNIT], (SUB, LANES))

    n_mom = [total(TILES), total(GROUPS)]
    for j in range(1, LAST):
        n_mom.append(dsub(dscale(total(TILES + j), TWO), n_mom[0]))
        n_mom.append(dsub(dscale(total(GROUPS + j), TWO), n_mom[1]))
    l_mom = [total(1 + j) for j in range(SUB)]
    for j in range(LAST, 14):
        l_mom.append(dsub(dscale(dsub(l_mom[j], n_mom[j]), TWO), l_mom[j - UNIT]))
    m_mom = [total(0)]
    m_mom.append(dsub(m_mom[0], l_mom[0]))
    for j in range(1, 15):
        m_mom.append(dsub(dscale(dsub(m_mom[j], l_mom[j]), TWO), m_mom[j - UNIT]))
    ys, xs = basis_coefs(*step_lengths(m_mom))
    slot = {}
    for t in range(STEPS):
        for j in range(t + UNIT):
            slot[t, j] = len(slot)
            coef[slot[t, j]] = ys[t][1 + j]
    for j in range(SUB):
        slot['x', j] = len(slot)
        coef[slot['x', j]] = xs[j]

    def put(ref, p, b0, val):
        for b in range(val.shape[0]):
            if b0 + b < 2:
                ref[p, pl.ds(b0 + b, SUB, stride=NB), :] = val[b, :, :N]
            else:
                ref[p, pl.ds(b0 + b, LAST, stride=NB), :] = val[b, :LAST, :N]

    def residuals(p, carry):
        carry = list(carry)
        for b0 in range(0, NB, 2):
            cut = pl.ds(b0, 2)
            v0 = v0_a[p, cut]
            sd = jnp.stack([k_nat[p, pl.ds(SUB * (b0 + b), SUB), :] for b in range(2)], axis=0)
            bs = [ref[p + UNIT, cut] for ref in b_a]
            for t in range(HEAD, STEPS):
                y = v0
                for j in range(t + UNIT):
                    y = y + coef[slot[t, j]] * bs[j]
                r = sd * y
                which = 2 * (t - HEAD) + (b0 > 0)
                carry[which] = carry[which] + jnp.sum(r * r, axis=0)
                if t == STEPS - UNIT:
                    put(f_in, p, b0, r)
        return tuple(carry)

    sums = lax.fori_loop(0, N, residuals, (zero,) * (2 * (STEPS - HEAD)))
    for t in range(STEPS):
        if t < HEAD:
            form = zero
            g = [None] + [coef[slot[t, j]] for j in range(t + 1)]
            for i in range(t + 2):
                part = gram[pair[0, i]] if not i else g[i] * gram[pair[0, i]]
                form = form + (part if not i else part + part)
            for i in range(UNIT, t + 2):
                part = zero
                for j in range(UNIT, t + 2):
                    part = part + g[j] * gram[pair[min(i, j), max(i, j)]]
                form = form + g[i] * part
            rsend[t] = pick(own_lane, form, zero)
        else:
            rsend[t] = own_cells(sums[2 * (t - HEAD)], sums[2 * (t - HEAD) + UNIT])
    part = rsend[:, 0, :]
    for s in range(1, SUB):
        part = part + rsend[:, s, :]
    rgath[me] = part
    rr_copies = gather(rgath, 1)

    def update(p, carry):
        for b0 in range(0, NB, 2):
            cut = pl.ds(b0, 2)
            x = coef[slot['x', 0]] * v0_a[p, cut]
            for j in range(1, SUB):
                x = x + coef[slot['x', j]] * b_a[j - UNIT][p + UNIT, cut]
            x = x * isd_a[p, cut]
            u = jnp.stack([u_nat[p, pl.ds(b0 + b, SUB, stride=NB), :] for b in range(2)], axis=0)
            put(k_in, p, b0, u + x)
        return carry

    lax.fori_loop(0, N, update, 0)
    for copy in rr_copies:
        copy.wait()
    part = rgath[0]
    for dev in range(1, SUB):
        part = part + rgath[dev]
    part = jnp.broadcast_to(jnp.sum(part, axis=1, keepdims=True), (SUB, LANES))
    rr_ref[...] = jnp.sum(jnp.where(lane == sub, part, ZERO), axis=0, keepdims=True)[:, :STEPS]


def solution(mesh):
    spec = P('gx', 'gy', 'gz')

    def local(k_cell, k_ghost, f_rhs, u_init):
        big = (E, NB, SUB, LANES)
        ext = (E + 2, NB, SUB, LANES)
        vm = lambda *shape: pltpu.VMEM(shape, F32)
        any_spec = pl.BlockSpec(memory_space=pl.ANY)
        u, r, rr = pl.pallas_call(
            kernel,
            out_shape=(vm(N, N, N), vm(N, N, N), vm(1, STEPS)),
            in_specs=[any_spec] * 4,
            out_specs=[pl.BlockSpec(memory_space=pltpu.VMEM)] * 3,
            scratch_shapes=[
                vm(N, N, N), vm(E + 2, E, LANES), vm(E, E, LANES), vm(E, E, LANES),
                vm(*ext), vm(*big), vm(*big), vm(*big), vm(N, NB, SUB, LANES),
                *[vm(E + 2, NB, SUB, LANES)] * STEPS,
                vm(3, 144, 144), vm(LANES, LANES), vm(LANES, LANES), vm(E, LANES), vm(N, SUB, N), vm(1, N, N), vm(1, N, N),
                vm(2, 45, SUB, LANES), vm(2, 45, SUB, LANES), vm(2, TILES, SUB, LANES), vm(2, TILES, SUB, LANES),
                vm(2, N, N), vm(2, N, N), vm(2, TILES, SUB, LANES), vm(2, TILES, SUB, LANES),
                vm(NDOT, SUB, LANES), vm(SUB, 2 * NDOT, LANES), vm(SUB, SUB, LANES), vm(SUB, SUB, LANES), vm(44, SUB, LANES),
                pltpu.SemaphoreType.DMA((6, 3)),
                pltpu.SemaphoreType.DMA((16,)), pltpu.SemaphoreType.DMA((16,)),
                pltpu.SemaphoreType.DMA((2, LAST)), pltpu.SemaphoreType.DMA((2, LAST)),
            ],
            compiler_params=pltpu.CompilerParams(collective_id=0, has_side_effects=True, vmem_limit_bytes=57 << 20),
        )(k_cell, f_rhs, u_init, k_ghost)
        return u, r, rr.reshape(STEPS)

    return jax.shard_map(local, mesh=mesh, in_specs=(spec, P(), spec, spec), out_specs=(spec, spec, P()), check_vma=False)
```

```python
import functools

import jax
import jax.numpy as jnp
from jax import lax
from jax.experimental import pallas as pl
from jax.experimental.pallas import tpu as pltpu
from jax.sharding import PartitionSpec as P


N = 72
H = 8
E = N + H
NB = 10
STEPS = 8
MESH = pl.DeviceIdType.MESH
F32 = jnp.float32
OTHERS = [(fx, fy, fz) for fx in (0, 1) for fy in (0, 1) for fz in (0, 1) if fx or fy or fz]
NDOT = 24
SUB = 8
LANES = 128
TILES = 9
PART = 24
WIDTH = 4
LAST = 7
GROUPS = 16
PIECES = 5
ZERO, ONE, HALF, TWO = 0.0, 1.0, 0.5, 2.0
UNIT = 1
HEAD = 4
PAIR = 2


def iota(axis):
    return lax.broadcasted_iota(jnp.int32, (SUB, LANES), axis)


def two_sum(a, b):
    s = a + b
    t = s - a
    return s, (a - (s - t)) + (b - t)


def quick(a, b):
    s = a + b
    return s, b - (s - a)


def two_prod(a, b):
    def split(x):
        t = x * 4097.0
        hi = t - (t - x)
        return hi, x - hi
    p = a * b
    ah, al = split(a)
    bh, bl = split(b)
    return p, ((ah * bh - p) + ah * bl + al * bh) + al * bl


def dadd(x, y):
    (xh, xl), (yh, yl) = x, y
    s, e = two_sum(xh, yh)
    return quick(s, e + (xl + yl))


def dsub(x, y):
    yh, yl = y
    return dadd(x, (-yh, -yl))


def dscale(x, c):
    hi, lo = x
    return hi * c, lo * c


def dmul(x, y):
    (xh, xl), (yh, yl) = x, y
    p, e = two_prod(xh, yh)
    return quick(p, e + (xh * yl + xl * yh))


def ddiv(x, y):
    (xh, xl), (yh, yl) = x, y
    q = xh / yh
    p, e = two_prod(q, yh)
    rest = ((xh - p) - e) + (xl - q * yl)
    return quick(q, rest / yh)


def step_lengths(m):
    alphas, betas = [], []
    y = dict(enumerate(m))
    p = {0: dsub(y[0], y[1])}
    for l in range(1, 15):
        p[l] = dsub(y[l], dscale(dadd(y[l + UNIT], y[l - UNIT]), HALF))
    for t in range(STEPS):
        alpha = ddiv(y[t], p[t])
        alphas.append(alpha[0])
        if t == STEPS - UNIT:
            break
        y_next = {l: dsub(y[l], dmul(alpha, p[l])) for l in range(t + UNIT, 15 - t)}
        beta = ddiv(y_next[t + UNIT], p[t])
        if t:
            beta = dscale(beta, HALF)
        betas.append(beta[0])
        p_next = {}
        for l in range(t + UNIT, 14 - t):
            side = y_next[l + UNIT] if l == t + UNIT else dadd(y_next[l + UNIT], y_next[l - UNIT])
            p_next[l] = dadd(dsub(y_next[l], dscale(side, HALF)), dmul(beta, p[l]))
        y, p = y_next, p_next
    return alphas, betas


def basis_coefs(alphas, betas):
    def add(a, b):
        return b if a is None else (a if b is None else a + b)

    def axpy(x, c, y):
        return [xi if yi is None else (c * yi if xi is None else xi + c * yi) for xi, yi in zip(x, y)]

    def apply_op(v):
        out = [None] * 11
        out[1] = v[0]
        for j in range(SUB):
            if v[1 + j] is None:
                continue
            c = v[1 + j]
            out[1 + j] = add(out[1 + j], c)
            if j == 0:
                out[2] = add(out[2], -c)
            else:
                half = -HALF * c
                out[2 + j] = add(out[2 + j], half)
                out[j] = add(out[j], half)
        return out[:TILES]

    one = jnp.ones_like(alphas[0])
    y = [one] + [None] * SUB
    p = list(y)
    x = [None] * TILES
    ys = []
    for t in range(STEPS):
        q = apply_op(p)
        x = axpy(x, alphas[t], p)
        y = axpy(y, -alphas[t], q)
        ys.append(y)
        if t < STEPS - UNIT:
            p = axpy(y, betas[t], p)
    return ys, x


def row_down(v):
    return jnp.concatenate([pltpu.roll(v[NB - UNIT], 1, 0)[None], v[:NB - UNIT]], axis=0)


def row_up(v):
    return jnp.concatenate([v[1:], pltpu.roll(v[0], LAST, 0)[None]], axis=0)


def lane_down(v):
    return pltpu.roll(v, 1, 2)


def lane_up(v):
    return pltpu.roll(v, 127, 2)


def load_chunk(ref, plane):
    return jnp.stack([ref[plane, pl.ds(b, SUB, stride=NB), :] for b in range(NB)], axis=0)


def replace(v, b, mask, value):
    return jnp.concatenate(([v[:b]] if b else []) + [jnp.where(mask, value, v[b])[None], v[b + UNIT:]], axis=0)


def harmonic(a, b):
    return TWO * a * b / (a + b)


def pick(mask, a, b):
    return lax.select_n(mask, b, a)


def planes(lo, hi, body, init, width=WIDTH):
    def some(n, carry):
        for w in range(width):
            carry = body(lo + n * width + w, carry)
        return carry
    return lax.fori_loop(0, (hi - lo) // width, some, init)


def own_cells(low, high):
    sub, lane = iota(0), iota(1)
    return jnp.where(lane < N, low + jnp.where(sub < LAST, high, ZERO), ZERO)


def kernel(k_hbm, f_hbm, u_hbm, kg_hbm, k_in, f_in, rr_ref,
           u_in, k_nat, u_nat, z_nat, cx_a, cy_a, cz_a, isd_a, v0_a, b0_a, b1_a, b2_a, b3_a, b4_a, b5_a, b6_a, b7_a,
           walls, wz, wz_t, wy, ky, kx, ux, zs, zr, ds_, dr, row_s, row_r, lane_s, lane_r, acc, gath, rsend, rgath, coef,
           load_sem, send_sem, recv_sem, all_send, all_recv):
    cx, cy, cz = lax.axis_index('gx'), lax.axis_index('gy'), lax.axis_index('gz')
    me = cx + 2 * cy + 4 * cz
    b_a = (b0_a, b1_a, b2_a, b3_a, b4_a, b5_a, b6_a, b7_a)
    lane, sub = iota(1), iota(0)

    def peer(fx, fy, fz):
        out = {}
        if fx:
            out['gx'] = 1 - cx
        if fy:
            out['gy'] = 1 - cy
        if fz:
            out['gz'] = 1 - cz
        return out

    loads = []
    for n, (src, dst) in enumerate([(k_hbm, k_in), (u_hbm, u_in), (f_hbm, f_in)]):
        loads.append([pltpu.make_async_copy(src.at[pl.ds(PART * q, PART)], dst.at[pl.ds(PART * q, PART)], load_sem.at[n, q])
                      for q in range(N // PART)])
    loads.append([pltpu.make_async_copy(kg_hbm.at[cx], walls.at[0], load_sem.at[3, 0])])
    loads.append([pltpu.make_async_copy(kg_hbm.at[2 + cy], walls.at[1], load_sem.at[4, 0])])
    loads.append([pltpu.make_async_copy(kg_hbm.at[4 + cz], walls.at[2], load_sem.at[PIECES, 0])])
    for n in (0, 1, 3, 4, PIECES, 2):
        for copy in loads[n]:
            copy.start()

    barrier = pltpu.get_barrier_semaphore()
    for flips in OTHERS:
        pl.semaphore_signal(barrier, inc=1, device_id=peer(*flips), device_id_type=MESH)

    def send(n, src, dst, flips):
        copy = pltpu.make_async_remote_copy(src_ref=src, dst_ref=dst, send_sem=send_sem.at[n], recv_sem=recv_sem.at[n],
                                            device_id=peer(*flips), device_id_type=MESH)
        copy.start()
        return copy

    near_y = pl.multiple_of((N - H) * (1 - cy), SUB)
    near_x = (N - H) * (1 - cx)
    src8 = (N - H) * (1 - cz)
    dst8 = N + 48 * cz
    ghost8 = jnp.logical_and(lane >= dst8, lane < dst8 + SUB)
    wall_lane = 127 - 55 * cz
    own_lane = lane < N
    at_wall = lane == wall_lane
    zero = jnp.zeros((SUB, LANES), F32)
    ones = jnp.ones((SUB, LANES), F32)

    def turn(x, by):
        return pltpu.roll(x, lax.rem(by + LANES, LANES), 1)

    def shift(x, by):
        return pltpu.roll(x, by % LANES, 1) if by % LANES else x

    def widen(x):
        return x if x.shape[1] == LANES else jnp.concatenate([x, jnp.zeros((x.shape[0], LANES - x.shape[1]), F32)], axis=1)

    def pack(nat, packed, corner, lo, hi):
        group8 = lax.rem(lane + (LANES - src8), LANES) // SUB
        groups = [group8 == g for g in range(GROUPS)]

        def body(o, carry):
            for q in range(PIECES):
                out = None
                for g in range(min(GROUPS, N - GROUPS * q)):
                    t = GROUPS * q + g
                    if t % TILES == 0:
                        plane = widen(nat[o * SUB + t // TILES, 0:N, :])
                    x = shift(plane[SUB * (t % TILES):SUB * (t % TILES) + SUB], SUB * g)
                    out = x if g == 0 else pick(groups[g], x, out)
                packed[o * PIECES + q] = out
            out = None
            for g in range(SUB):
                x = widen(nat[o * SUB + g, pl.ds(near_y, SUB), :])
                x = shift(x, SUB * g)
                out = x if g == 0 else pick(groups[g], x, out)
            corner[o] = out
            return carry
        lax.fori_loop(lo, hi, body, 0)

    def unpack(own, side, nat, packed, corner, fill, wall, o, carry):
        by = dst8 - (N - H - src8)
        packs, corner_in = [turn(packed[o * PIECES + q], by) for q in range(PIECES)], turn(corner[o], by)
        for pi in range(SUB):
            i, out = o * SUB + pi, []
            plane = widen(own[i, 0:N, :])
            for jt in range(NB):
                if jt < TILES:
                    t = pi * TILES + jt
                    got, g = packs[t // GROUPS], t % GROUPS
                else:
                    got, g = corner_in, pi
                x = plane[SUB * jt:SUB * jt + SUB] if jt < TILES else widen(side[i])
                other = fill if wall is None else pick(at_wall, wall_column(i, jt), fill)
                out.append(pick(own_lane, x, pick(ghost8, shift(got, -SUB * g), other)))
            nat[i, 0:E, :] = jnp.concatenate(out, axis=0)
        return carry

    def wall_column(i, jt):
        at = SUB * jt if jt < TILES else pl.multiple_of(N + 48 * cy, SUB)
        return pltpu.roll(wz_t[pl.ds(at, SUB), :], LANES - UNIT - i, 1)

    for copy in loads[0] + loads[1]:
        copy.wait()
    last_x, last_y, last_z = (N - UNIT) * (1 - cx), (N - UNIT) * (1 - cy), (N - UNIT) * (1 - cz)

    slots = lax.rem(lane + (LANES - last_z), LANES)

    def pack_one(o, carry):
        for n, src in enumerate((k_in, u_in)):
            row_s[n, pl.ds(pl.multiple_of(o * SUB, SUB), SUB), :] = jnp.concatenate(
                [src[o * SUB + r, pl.ds(last_y, 1), :] for r in range(SUB)], axis=0)
            out = None
            for t in range(N):
                if t % TILES == 0:
                    plane = widen(src[o * SUB + t // TILES])
                x = shift(plane[SUB * (t % TILES):SUB * (t % TILES) + SUB], t)
                out = x if t == 0 else pick(slots == t, x, out)
            lane_s[n, o] = out
        return carry
    planes(0, TILES, pack_one, 0, 3)
    pl.semaphore_wait(barrier, len(OTHERS))
    one_x = [send(0, k_in.at[pl.ds(last_x, 1)], kx, (1, 0, 0)), send(1, u_in.at[pl.ds(last_x, 1)], ux, (1, 0, 0))]
    one_y = send(2, row_s, row_r, (0, 1, 0))
    one_z = send(3, lane_s, lane_r, (0, 0, 1))
    k_y = send(4, k_in.at[:, pl.ds(near_y, SUB), :], ky, (0, 1, 0))
    pack(k_in, zs.at[0], ds_.at[0], 0, TILES)
    k_z = send(PIECES, zs.at[0], zr.at[0], (0, 0, 1))
    k_d = send(6, ds_.at[0], dr.at[0], (0, 1, 1))

    for n in (3, 4, PIECES):
        loads[n][0].wait()

    def lane_ring(w, at, c):
        left, right = walls[w, pl.ds(at, SUB), 0:LANES], walls[w, pl.ds(at, SUB), LANES:144]
        gap = jnp.zeros((SUB, 56), F32)
        right = jnp.concatenate([gap, right, gap], axis=1)
        turned = jnp.where(jnp.logical_and(lane >= 56, lane < N), right, pltpu.roll(left, 56, 1))
        return jnp.where(c == 0, left, turned)

    for jt in range(NB):
        at_j = pl.multiple_of(N * cy + SUB * jt if jt < TILES else N - H * cy, SUB)
        at_i = pl.multiple_of(N * cx + SUB * jt if jt < TILES else N - H * cx, SUB)
        k_nat[E, pl.ds(SUB * jt, SUB), :] = lane_ring(0, at_j, cz)
        wy[pl.ds(SUB * jt, SUB), :] = lane_ring(1, at_i, cz)
        if jt < TILES:
            wz[pl.ds(SUB * jt, SUB), :] = lane_ring(2, at_i, cy)
    wz_t[...] = turn(wz[...].T, wall_lane + UNIT)

    for copy in loads[2]:
        copy.wait()

    def take_f(p, carry):
        for b in range(NB):
            rows = SUB if b < 2 else LAST
            v0_a[p, b, 0:rows, 0:N] = f_in[p, pl.ds(b, rows, stride=NB), :]
        return carry
    planes(0, N, take_f, 0)

    def lay_out(i, carry):
        side = jnp.concatenate([pick(at_wall, wall_column(i, jt), ones) for jt in range(TILES)], axis=0)
        for nat, src, rest in ((k_nat, k_in, side), (u_nat, u_in, jnp.zeros((N, LANES), F32))):
            nat[i, 0:N, N:] = rest[:, N:]
            nat[i, 0:N, 0:N] = src[i]
        return carry
    planes(0, N, lay_out, 0)

    u_nat[E - UNIT - LAST * cx] = jnp.zeros((E, LANES), F32)
    one_lane = N + 55 * cz
    at_one = lane == one_lane
    for copy in one_x + [one_y, one_z]:
        copy.wait()
    u_nat[N + LAST * cx, 0:N, 0:N] = ux[0]
    k_nat[E + UNIT, 0:N, 0:N] = kx[0]

    def unpack_one(o, carry):
        for n, nat in enumerate((k_nat, u_nat)):
            got = turn(lane_r[n, o], one_lane - (N - 1 - last_z))
            for t in range(N):
                here = nat.at[o * SUB + t // TILES, pl.ds(SUB * (t % TILES), SUB), :]
                pltpu.store(here, shift(got, -t), mask=at_one)
        return carry
    lax.fori_loop(0, TILES, unpack_one, 0)

    row0 = sub == 0
    row72 = sub == LAST

    def divergence(h_x, h_xn, h_y, h_z, v, v_prev, v_next, low_row, high_row):
        low = row_down(v)
        high = v
        if low_row is not None:
            low = replace(low, 0, row0, low_row)
            high = replace(v, 2, row72, high_row)
        else:
            low = replace(low, 0, jnp.logical_and(row0, cy == 0), ZERO)
            high = replace(v, 2, jnp.logical_and(row72, cy == 1), ZERO)
        f_y = h_y * (high - low)
        f_z = h_z * (v - lane_down(v))
        return ((h_x * (v - v_prev) - h_xn * (v_next - v)) + (f_y - row_up(f_y))) + (f_z - lane_up(f_z))

    def full(row):
        return jnp.broadcast_to(widen(row), (SUB, LANES))

    def add_up(h_x, h_xn, h_y, h_z):
        return ((h_x + h_xn) + (h_y + row_up(h_y))) + (h_z + lane_up(h_z))

    def start_own(n, carry):
        p0 = PAIR * n
        first_trip, last_trip = n == 0, n == N // PAIR - UNIT
        k_p = [load_chunk(k_nat, jnp.where(first_trip, E + cx, p0 - UNIT))]
        u_p = [load_chunk(u_nat, jnp.where(first_trip, E - UNIT, p0 - UNIT))]
        for w in range(PAIR):
            k_p.append(load_chunk(k_nat, p0 + w))
            u_p.append(load_chunk(u_nat, p0 + w))
        k_p.append(load_chunk(k_nat, jnp.where(last_trip, E + UNIT - cx, p0 + PAIR)))
        u_p.append(load_chunk(u_nat, p0 + PAIR))
        h_x = [harmonic(k_p[w + UNIT], k_p[w]) for w in range(PAIR + UNIT)]
        for w in range(PAIR):
            p, kc = p0 + w, k_p[w + UNIT]
            wall, got = full(wy[pl.ds(p, 1), :]), full(row_r[0, pl.ds(p, 1), :])
            low = replace(row_down(kc), 0, row0, jnp.where(cy == 0, wall, got))
            high = replace(kc, 2, row72, jnp.where(cy == 0, got, wall))
            h_y = harmonic(high, low)
            h_z = harmonic(kc, lane_down(kc))
            inv = lax.rsqrt(add_up(h_x[w], h_x[w + UNIT], h_y, h_z))
            got = full(row_r[1, pl.ds(p, 1), :])
            a_u = divergence(h_x[w], h_x[w + UNIT], h_y, h_z, u_p[w + UNIT], u_p[w], u_p[w + 2],
                             jnp.where(cy == 0, ZERO, got), jnp.where(cy == 0, got, ZERO))
            y0 = (v0_a[p] - a_u) * inv
            for b in range(NB):
                v0_a[p, b] = y0[b] if b < 2 else pick(row72, zero, y0[b])
            z0 = y0 * inv
            for b in range(NB):
                if b < 2:
                    z_nat[p, pl.ds(b, SUB, stride=NB), :] = z0[b]
                else:
                    z_nat[p, pl.ds(b, LAST, stride=NB), :] = z0[b, :LAST]
        return carry
    z_copies = []
    for q in range(3):
        lax.fori_loop(12 * q, 12 * q + 12, start_own, 0)
        rows = pl.ds(PART * q, PART)
        z_copies.append(send(7 + q, z_nat.at[rows, pl.ds(near_y, SUB), :], z_nat.at[rows, pl.ds(N, SUB), :], (0, 1, 0)))
        pack(z_nat, zs.at[1], ds_.at[1], 3 * q, 3 * q + 3)
        lanes = pl.ds(15 * q, 15)
        z_copies.append(send(12 + q, zs.at[1, lanes], zr.at[1, lanes], (0, 0, 1)))
    z_copies.append(send(15, ds_.at[1], dr.at[1], (0, 1, 1)))

    def spread(n, nat, take):
        take(SUB * (1 - cx), 0)
        copy = send(n, nat.at[pl.ds(near_x, SUB)], nat.at[pl.ds(N, SUB)], (1, 0, 0))
        lax.fori_loop(0, SUB, lambda o, carry: take(o + cx, carry), 0)
        return copy

    for copy in (k_y, k_z, k_d):
        copy.wait()
    spread(NB, k_nat, functools.partial(unpack, k_in, ky, k_nat, zr.at[0], dr.at[0], ones, wz_t)).wait()

    def faces(p, carry):
        kc = load_chunk(k_nat, p)
        before = jnp.where(jnp.logical_and(p == 0, cx == 0), E, jnp.where(p == 0, E - UNIT, p - UNIT))
        here = jnp.where(jnp.logical_and(p == N, cx == 1), E, p)
        cx_a[p] = harmonic(load_chunk(k_nat, here), load_chunk(k_nat, before))
        wall = full(wy[pl.ds(p, 1), :])
        low = replace(row_down(kc), 0, jnp.logical_and(row0, cy == 0), wall)
        high = replace(kc, 2, jnp.logical_and(row72, cy == 1), wall)
        cy_a[p] = harmonic(high, low)
        cz_a[p] = harmonic(kc, lane_down(kc))
        return carry
    planes(0, E, faces, 0, SUB)
    cx_a[E] = cx_a[0]
    cx_a[E + UNIT] = cx_a[1]

    def scales(own, p, carry):
        d = add_up(cx_a[p], cx_a[p + UNIT], cy_a[p], cz_a[p])
        inv = lax.rsqrt(d)
        isd_a[p] = inv
        if own:
            sd = d * inv
            for b in range(NB):
                k_nat[p, pl.ds(SUB * b, SUB), :] = sd[b] if b < 2 else pick(row72, zero, sd[b])
        return carry
    planes(0, N, functools.partial(scales, True), 0, SUB)
    planes(N, E, functools.partial(scales, False), 0, SUB)

    for copy in z_copies:
        copy.wait()
    z_x = spread(11, z_nat, functools.partial(unpack, z_nat, z_nat.at[:, pl.ds(N, SUB), :], z_nat, zr.at[1], dr.at[1],
                                              zero, None))

    def column(ref, p, b, width):
        return ref[pl.ds(p, width), b]

    def z_column(p, b, width=1):
        return z_nat[pl.ds(p, width), pl.ds(b, SUB, stride=NB), :]

    def tally(carry, b, products):
        return [c + jnp.sum(products[n // 2], axis=0) if n % 2 == (b > 1) else c for n, c in enumerate(carry)]

    def first(own, width, p, carry, before=None, after=None, x_after=None):
        before = p - UNIT if before is None else before
        z, inv, low, f_y, h_y = {}, {}, {}, {}, {}

        def load(b):
            z[b], inv[b], h_y[b] = z_column(p, b, width), column(isd_a, p, b, width), column(cy_a, p, b, width)
            under = z[b - UNIT] if b else pltpu.roll(z_column(p, NB - UNIT, width), 1, 1)
            over = z[b]
            if b == 0:
                under = jnp.where(jnp.logical_and(row0, cy == 0), ZERO, under)
            if b == 2:
                over = jnp.where(jnp.logical_and(row72, cy == 1), ZERO, over)
            f_y[b] = h_y[b] * (over - under)
        carry = list(carry)
        load(0)
        for b in range(NB):
            if b < NB - UNIT:
                load(b + UNIT)
            up = f_y[b + UNIT] if b < NB - UNIT else pltpu.roll(f_y[0], LAST, 1)
            z_p = z_column(before, b)
            z_n = z_column(p + width if after is None else after, b)
            if isinstance(p, int) and p == 0:
                z_p = jnp.where(cx == 0, ZERO, z_p)
            if isinstance(p, int) and p == N - UNIT:
                z_n = jnp.where(cx == 1, ZERO, z_n)
            if x_after is None:
                h_x = column(cx_a, p, b, width + UNIT)
            else:
                h_x = jnp.concatenate([column(cx_a, p, b, 1), column(cx_a, x_after, b, 1)], axis=0)
            f_x = h_x * (jnp.concatenate([z[b], z_n], axis=0) - jnp.concatenate([z_p, z[b]], axis=0))
            h_z = column(cz_a, p, b, width)
            f_z = h_z * (z[b] - lane_down(z[b]))
            b0 = inv[b] * (((f_x[:width] - f_x[1:]) + (f_y[b] - up)) + (f_z - lane_up(f_z)))
            b_a[0][pl.ds(p + UNIT, width), b] = b0
            twice = TWO * inv[b]
            side = column(isd_a, before, b, 1)
            if width > 1:
                side = jnp.concatenate([side, inv[b][:width - UNIT]], axis=0)
            cx_a[pl.ds(p, width), b] = h_x[:width] * (twice * side)
            side = inv[b - UNIT] if b else pltpu.roll(column(isd_a, p, NB - UNIT, width), 1, 1)
            c_y = h_y[b] * (twice * side)
            if b == 0:
                c_y = jnp.where(jnp.logical_and(row0, cy == 0), ZERO, c_y)
            if b == 2:
                c_y = jnp.where(jnp.logical_and(row72, cy == 1), ZERO, c_y)
            cy_a[pl.ds(p, width), b] = c_y
            cz_a[pl.ds(p, width), b] = jnp.where(at_edge, ZERO, h_z * (twice * lane_down(inv[b])))
            if own:
                v0 = column(v0_a, p, b, width)
                carry = tally(carry, b, (v0 * v0, v0 * b0, b0 * b0))
        return tuple(carry)

    at_edge = lane == N * cz

    def wrap(ref):
        ref[0] = jnp.where(cx == 0, ref[1], ref[E])
        ref[E + UNIT] = ref[1]
        ref[N + UNIT] = jnp.where(cx == 1, ref[N], ref[N + UNIT])

    sums = lax.fori_loop(0, 14, lambda n, carry: first(True, PIECES, 1 + PIECES * n, carry), (zero,) * 6)
    z_x.wait()
    sums = first(True, 1, 0, sums, E - UNIT, None, E + UNIT)
    sums = first(True, 1, N - UNIT, sums)
    first(False, WIDTH, N, ())
    first(False, WIDTH, N + WIDTH, (), None, 0)
    cx_a[0] = jnp.where(cx == 0, ZERO, cx_a[0])
    cx_a[N] = jnp.where(cx == 1, ZERO, cx_a[N])
    cx_a[E] = cx_a[0]
    wrap(b_a[0])
    acc[0] = own_cells(sums[0], sums[1])
    acc[1] = own_cells(sums[2], sums[3])
    acc[TILES] = own_cells(sums[4], sums[PIECES])
    acc[23] = zero

    def advance(k, own, width, p, carry):
        old, carry = b_a[k - UNIT], list(carry)
        v_low = pltpu.roll(column(old, p + UNIT, NB - UNIT, width), 1, 1)
        v, c_y = column(old, p + UNIT, 0, width), column(cy_a, p, 0, width)
        t_first = c_y * v
        for b in range(NB):
            if b < NB - UNIT:
                v_high, c_high = column(old, p + UNIT, b + UNIT, width), column(cy_a, p, b + UNIT, width)
                t_high = c_high * v_high
            else:
                t_high = pltpu.roll(t_first, LAST, 1)
            c_x, c_z = column(cx_a, p, b, width + UNIT), column(cz_a, p, b, width)
            below, above = column(old, p, b, 1), column(old, p + width + UNIT, b, 1)
            if width > 1:
                below = jnp.concatenate([below, v[:width - UNIT]], axis=0)
                above = jnp.concatenate([v[1:], above], axis=0)
            new = c_x[:width] * below + c_x[1:] * above
            new = new + (c_y * v_low + t_high)
            new = new + (c_z * lane_down(v) + lane_up(c_z * v))
            new = HALF * new if k == 1 else new - column(b_a[k - 2], p + UNIT, b, width)
            b_a[k][pl.ds(p + UNIT, width), b] = new
            if own:
                carry = tally(carry, b, (column(v0_a, p, b, width) * new, v * new, new * new))
            v_low, v, c_y = v, v_high, c_high
        return tuple(carry)

    for k in range(1, STEPS):
        sums = lax.fori_loop(0, N // SUB, lambda n, carry: advance(k, True, SUB, SUB * n, carry), (zero,) * 6)
        if k < STEPS - UNIT:
            depth = (STEPS - k) // PAIR * PAIR
            advance(k, False, depth, N + (H - depth) * cx, ())
            wrap(b_a[k])
        acc[1 + k] = own_cells(sums[0], sums[1])
        acc[GROUPS + k - UNIT] = own_cells(sums[2], sums[3])
        if k < STEPS - UNIT:
            acc[TILES + k] = own_cells(sums[4], sums[PIECES])

    def gather(buf, n_sem):
        copies = []
        for n, flips in enumerate(OTHERS):
            copies.append(pltpu.make_async_remote_copy(
                src_ref=buf.at[me], dst_ref=buf.at[me], send_sem=all_send.at[n_sem, n], recv_sem=all_recv.at[n_sem, n],
                device_id=peer(*flips), device_id_type=MESH))
        for copy in copies:
            copy.start()
        return copies

    hi = acc[:, 0, :]
    lo = jnp.zeros((NDOT, LANES), F32)
    for s in range(1, SUB):
        hi, err = two_sum(hi, acc[:, s, :])
        lo = lo + err
    gath[me, 0:NDOT] = hi
    gath[me, NDOT:2 * NDOT] = lo
    gath_copies = gather(gath, 0)
    pair = {}
    for i in range(HEAD + UNIT):
        for j in range(i, HEAD + UNIT):
            pair[i, j] = len(pair)

    def products(n, carry):
        p, carry = WIDTH * n, list(carry)
        for b in range(NB):
            sd = k_nat[pl.ds(p, WIDTH), pl.ds(SUB * b, SUB), :]
            w = [sd * column(v0_a, p, b, WIDTH)] + [sd * column(b_a[j], p + UNIT, b, WIDTH) for j in range(HEAD)]
            for (i, j), at in pair.items():
                carry[at] = carry[at] + jnp.sum(w[i] * w[j], axis=0)
        return tuple(carry)
    gram = lax.fori_loop(0, N // WIDTH, products, (zero,) * len(pair))
    for copy in gath_copies:
        copy.wait()
    hi, lo = gath[0, 0:NDOT], gath[0, NDOT:2 * NDOT]
    for dev in range(1, SUB):
        hi, err = two_sum(hi, gath[dev, 0:NDOT])
        lo = lo + (gath[dev, NDOT:2 * NDOT] + err)
    for shift in (64, 32, GROUPS, SUB, 4, 2, 1):
        hi, err = two_sum(hi, pltpu.roll(hi, shift, 1))
        lo = (lo + pltpu.roll(lo, shift, 1)) + err
    hi, lo = quick(hi, lo)
    size = hi[0:1]
    factor = jnp.where(size > 1e30, TWO ** -110, jnp.where(size > 1e12, TWO ** -60, jnp.where(
        size < 1e-30, TWO ** 110, jnp.where(size < 1e-12, TWO ** 60, ONE)))).astype(F32)
    hi, lo = hi * factor, lo * factor

    def total(row):
        return jnp.broadcast_to(hi[row:row + UNIT], (SUB, LANES)), jnp.broadcast_to(lo[row:row + UNIT], (SUB, LANES))

    n_mom = [total(TILES), total(GROUPS)]
    for j in range(1, LAST):
        n_mom.append(dsub(dscale(total(TILES + j), TWO), n_mom[0]))
        n_mom.append(dsub(dscale(total(GROUPS + j), TWO), n_mom[1]))
    l_mom = [total(1 + j) for j in range(SUB)]
    for j in range(LAST, 14):
        l_mom.append(dsub(dscale(dsub(l_mom[j], n_mom[j]), TWO), l_mom[j - UNIT]))
    m_mom = [total(0)]
    m_mom.append(dsub(m_mom[0], l_mom[0]))
    for j in range(1, 15):
        m_mom.append(dsub(dscale(dsub(m_mom[j], l_mom[j]), TWO), m_mom[j - UNIT]))
    ys, xs = basis_coefs(*step_lengths(m_mom))
    slot = {}
    for t in range(STEPS):
        for j in range(t + UNIT):
            slot[t, j] = len(slot)
            coef[slot[t, j]] = ys[t][1 + j]
    for j in range(SUB):
        slot['x', j] = len(slot)
        coef[slot['x', j]] = xs[j]

    def put(ref, p, b0, val):
        for b in range(val.shape[0]):
            if b0 + b < 2:
                ref[p, pl.ds(b0 + b, SUB, stride=NB), :] = val[b, :, :N]
            else:
                ref[p, pl.ds(b0 + b, LAST, stride=NB), :] = val[b, :LAST, :N]

    def residuals(p, carry):
        carry = list(carry)
        for b0 in range(0, NB, 2):
            cut = pl.ds(b0, 2)
            v0 = v0_a[p, cut]
            sd = jnp.stack([k_nat[p, pl.ds(SUB * (b0 + b), SUB), :] for b in range(2)], axis=0)
            bs = [ref[p + UNIT, cut] for ref in b_a]
            for t in range(HEAD, STEPS):
                y = v0
                for j in range(t + UNIT):
                    y = y + coef[slot[t, j]] * bs[j]
                r = sd * y
                which = 2 * (t - HEAD) + (b0 > 0)
                carry[which] = carry[which] + jnp.sum(r * r, axis=0)
                if t == STEPS - UNIT:
                    put(f_in, p, b0, r)
        return tuple(carry)

    sums = lax.fori_loop(0, N, residuals, (zero,) * (2 * (STEPS - HEAD)))
    for t in range(STEPS):
        if t < HEAD:
            form = zero
            g = [None] + [coef[slot[t, j]] for j in range(t + 1)]
            for i in range(t + 2):
                part = gram[pair[0, i]] if not i else g[i] * gram[pair[0, i]]
                form = form + (part if not i else part + part)
            for i in range(UNIT, t + 2):
                part = zero
                for j in range(UNIT, t + 2):
                    part = part + g[j] * gram[pair[min(i, j), max(i, j)]]
                form = form + g[i] * part
            rsend[t] = pick(own_lane, form, zero)
        else:
            rsend[t] = own_cells(sums[2 * (t - HEAD)], sums[2 * (t - HEAD) + UNIT])
    part = rsend[:, 0, :]
    for s in range(1, SUB):
        part = part + rsend[:, s, :]
    rgath[me] = part
    rr_copies = gather(rgath, 1)

    def update(p, carry):
        for b0 in range(0, NB, 2):
            cut = pl.ds(b0, 2)
            x = coef[slot['x', 0]] * v0_a[p, cut]
            for j in range(1, SUB):
                x = x + coef[slot['x', j]] * b_a[j - UNIT][p + UNIT, cut]
            x = x * isd_a[p, cut]
            u = jnp.stack([u_nat[p, pl.ds(b0 + b, SUB, stride=NB), :] for b in range(2)], axis=0)
            put(k_in, p, b0, u + x)
        return carry

    lax.fori_loop(0, N, update, 0)
    for copy in rr_copies:
        copy.wait()
    part = rgath[0]
    for dev in range(1, SUB):
        part = part + rgath[dev]
    part = jnp.broadcast_to(jnp.sum(part, axis=1, keepdims=True), (SUB, LANES))
    rr_ref[...] = jnp.sum(jnp.where(lane == sub, part, ZERO), axis=0, keepdims=True)[:, :STEPS]


def solution(mesh):
    spec = P('gx', 'gy', 'gz')

    def local(k_cell, k_ghost, f_rhs, u_init):
        big = (E, NB, SUB, LANES)
        ext = (E + 2, NB, SUB, LANES)
        vm = lambda *shape: pltpu.VMEM(shape, F32)
        any_spec = pl.BlockSpec(memory_space=pl.ANY)
        u, r, rr = pl.pallas_call(
            kernel,
            out_shape=(vm(N, N, N), vm(N, N, N), vm(1, STEPS)),
            in_specs=[any_spec] * 4,
            out_specs=[pl.BlockSpec(memory_space=pltpu.VMEM)] * 3,
            scratch_shapes=[
                vm(N, N, N), vm(E + 2, E, LANES), vm(E, E, LANES), vm(E, E, LANES),
                vm(*ext), vm(*big), vm(*big), vm(*big), vm(N, NB, SUB, LANES),
                *[vm(E + 2, NB, SUB, LANES)] * STEPS,
                vm(3, 144, 144), vm(LANES, LANES), vm(LANES, LANES), vm(E, LANES), vm(N, SUB, N), vm(1, N, N), vm(1, N, N),
                vm(2, 45, SUB, LANES), vm(2, 45, SUB, LANES), vm(2, TILES, SUB, LANES), vm(2, TILES, SUB, LANES),
                vm(2, N, N), vm(2, N, N), vm(2, TILES, SUB, LANES), vm(2, TILES, SUB, LANES),
                vm(NDOT, SUB, LANES), vm(SUB, 2 * NDOT, LANES), vm(SUB, SUB, LANES), vm(SUB, SUB, LANES), vm(44, SUB, LANES),
                pltpu.SemaphoreType.DMA((6, 3)),
                pltpu.SemaphoreType.DMA((16,)), pltpu.SemaphoreType.DMA((16,)),
                pltpu.SemaphoreType.DMA((2, LAST)), pltpu.SemaphoreType.DMA((2, LAST)),
            ],
            compiler_params=pltpu.CompilerParams(collective_id=0, has_side_effects=True, vmem_limit_bytes=57 << 20),
        )(k_cell, f_rhs, u_init, k_ghost)
        return u, r, rr.reshape(STEPS)

    return jax.shard_map(local, mesh=mesh, in_specs=(spec, P(), spec, spec), out_specs=(spec, spec, P()), check_vma=False)
```

```python
import functools

import jax
import jax.numpy as jnp
from jax import lax
from jax.experimental import pallas as pl
from jax.experimental.pallas import tpu as pltpu
from jax.sharding import PartitionSpec as P


N = 72
H = 8
E = N + H
NB = 10
STEPS = 8
MESH = pl.DeviceIdType.MESH
F32 = jnp.float32
OTHERS = [(fx, fy, fz) for fx in (0, 1) for fy in (0, 1) for fz in (0, 1) if fx or fy or fz]
NDOT = 24
SUB = 8
LANES = 128
TILES = 9
PART = 24
WIDTH = 4
LAST = 7
GROUPS = 16
PIECES = 5
ZERO, ONE, HALF, TWO = 0.0, 1.0, 0.5, 2.0
UNIT = 1
HEAD = 4
PAIR = 2


def iota(axis):
    return lax.broadcasted_iota(jnp.int32, (SUB, LANES), axis)


def two_sum(a, b):
    s = a + b
    t = s - a
    return s, (a - (s - t)) + (b - t)


def quick(a, b):
    s = a + b
    return s, b - (s - a)


def two_prod(a, b):
    def split(x):
        t = x * 4097.0
        hi = t - (t - x)
        return hi, x - hi
    p = a * b
    ah, al = split(a)
    bh, bl = split(b)
    return p, ((ah * bh - p) + ah * bl + al * bh) + al * bl


def dadd(x, y):
    (xh, xl), (yh, yl) = x, y
    s, e = two_sum(xh, yh)
    return quick(s, e + (xl + yl))


def dsub(x, y):
    yh, yl = y
    return dadd(x, (-yh, -yl))


def dscale(x, c):
    hi, lo = x
    return hi * c, lo * c


def dmul(x, y):
    (xh, xl), (yh, yl) = x, y
    p, e = two_prod(xh, yh)
    return quick(p, e + (xh * yl + xl * yh))


def ddiv(x, y):
    (xh, xl), (yh, yl) = x, y
    q = xh / yh
    p, e = two_prod(q, yh)
    rest = ((xh - p) - e) + (xl - q * yl)
    return quick(q, rest / yh)


def step_lengths(m):
    alphas, betas = [], []
    y = dict(enumerate(m))
    p = {0: dsub(y[0], y[1])}
    for l in range(1, 15):
        p[l] = dsub(y[l], dscale(dadd(y[l + UNIT], y[l - UNIT]), HALF))
    for t in range(STEPS):
        alpha = ddiv(y[t], p[t])
        alphas.append(alpha[0])
        if t == STEPS - UNIT:
            break
        y_next = {l: dsub(y[l], dmul(alpha, p[l])) for l in range(t + UNIT, 15 - t)}
        beta = ddiv(y_next[t + UNIT], p[t])
        if t:
            beta = dscale(beta, HALF)
        betas.append(beta[0])
        p_next = {}
        for l in range(t + UNIT, 14 - t):
            side = y_next[l + UNIT] if l == t + UNIT else dadd(y_next[l + UNIT], y_next[l - UNIT])
            p_next[l] = dadd(dsub(y_next[l], dscale(side, HALF)), dmul(beta, p[l]))
        y, p = y_next, p_next
    return alphas, betas


def basis_coefs(alphas, betas):
    def add(a, b):
        return b if a is None else (a if b is None else a + b)

    def axpy(x, c, y):
        return [xi if yi is None else (c * yi if xi is None else xi + c * yi) for xi, yi in zip(x, y)]

    def apply_op(v):
        out = [None] * 11
        out[1] = v[0]
        for j in range(SUB):
            if v[1 + j] is None:
                continue
            c = v[1 + j]
            out[1 + j] = add(out[1 + j], c)
            if j == 0:
                out[2] = add(out[2], -c)
            else:
                half = -HALF * c
                out[2 + j] = add(out[2 + j], half)
                out[j] = add(out[j], half)
        return out[:TILES]

    one = jnp.ones_like(alphas[0])
    y = [one] + [None] * SUB
    p = list(y)
    x = [None] * TILES
    ys = []
    for t in range(STEPS):
        q = apply_op(p)
        x = axpy(x, alphas[t], p)
        y = axpy(y, -alphas[t], q)
        ys.append(y)
        if t < STEPS - UNIT:
            p = axpy(y, betas[t], p)
    return ys, x


def row_down(v):
    return jnp.concatenate([pltpu.roll(v[NB - UNIT], 1, 0)[None], v[:NB - UNIT]], axis=0)


def row_up(v):
    return jnp.concatenate([v[1:], pltpu.roll(v[0], LAST, 0)[None]], axis=0)


def lane_down(v):
    return pltpu.roll(v, 1, 2)


def lane_up(v):
    return pltpu.roll(v, 127, 2)


def load_chunk(ref, plane):
    return jnp.stack([ref[plane, pl.ds(b, SUB, stride=NB), :] for b in range(NB)], axis=0)


def replace(v, b, mask, value):
    return jnp.concatenate(([v[:b]] if b else []) + [jnp.where(mask, value, v[b])[None], v[b + UNIT:]], axis=0)


def harmonic(a, b):
    return TWO * a * b / (a + b)


def pick(mask, a, b):
    return lax.select_n(mask, b, a)


def planes(lo, hi, body, init, width=WIDTH):
    def some(n, carry):
        for w in range(width):
            carry = body(lo + n * width + w, carry)
        return carry
    return lax.fori_loop(0, (hi - lo) // width, some, init)


def own_cells(low, high):
    sub, lane = iota(0), iota(1)
    return jnp.where(lane < N, low + jnp.where(sub < LAST, high, ZERO), ZERO)


def kernel(k_hbm, f_hbm, u_hbm, kg_hbm, k_in, f_in, rr_ref,
           u_in, k_nat, u_nat, z_nat, cx_a, cy_a, cz_a, isd_a, v0_a, b0_a, b1_a, b2_a, b3_a, b4_a, b5_a, b6_a, b7_a,
           walls, wz, wz_t, wy, ky, kx, ux, zs, zr, ds_, dr, row_s, row_r, lane_s, lane_r, acc, gath, rsend, rgath, coef,
           load_sem, send_sem, recv_sem, all_send, all_recv):
    cx, cy, cz = lax.axis_index('gx'), lax.axis_index('gy'), lax.axis_index('gz')
    me = cx + 2 * cy + 4 * cz
    b_a = (b0_a, b1_a, b2_a, b3_a, b4_a, b5_a, b6_a, b7_a)
    lane, sub = iota(1), iota(0)

    def peer(fx, fy, fz):
        out = {}
        if fx:
            out['gx'] = 1 - cx
        if fy:
            out['gy'] = 1 - cy
        if fz:
            out['gz'] = 1 - cz
        return out

    loads = []
    for n, (src, dst) in enumerate([(k_hbm, k_in), (u_hbm, u_in), (f_hbm, f_in)]):
        loads.append([pltpu.make_async_copy(src.at[pl.ds(PART * q, PART)], dst.at[pl.ds(PART * q, PART)], load_sem.at[n, q])
                      for q in range(N // PART)])
    loads.append([pltpu.make_async_copy(kg_hbm.at[cx], walls.at[0], load_sem.at[3, 0])])
    loads.append([pltpu.make_async_copy(kg_hbm.at[2 + cy], walls.at[1], load_sem.at[4, 0])])
    loads.append([pltpu.make_async_copy(kg_hbm.at[4 + cz], walls.at[2], load_sem.at[PIECES, 0])])
    for n in (0, 1, 3, 4, PIECES, 2):
        for copy in loads[n]:
            copy.start()

    barrier = pltpu.get_barrier_semaphore()
    for flips in OTHERS:
        pl.semaphore_signal(barrier, inc=1, device_id=peer(*flips), device_id_type=MESH)

    def send(n, src, dst, flips):
        copy = pltpu.make_async_remote_copy(src_ref=src, dst_ref=dst, send_sem=send_sem.at[n], recv_sem=recv_sem.at[n],
                                            device_id=peer(*flips), device_id_type=MESH)
        copy.start()
        return copy

    near_y = pl.multiple_of((N - H) * (1 - cy), SUB)
    near_x = (N - H) * (1 - cx)
    src8 = (N - H) * (1 - cz)
    dst8 = N + 48 * cz
    ghost8 = jnp.logical_and(lane >= dst8, lane < dst8 + SUB)
    wall_lane = 127 - 55 * cz
    own_lane = lane < N
    at_wall = lane == wall_lane
    zero = jnp.zeros((SUB, LANES), F32)
    ones = jnp.ones((SUB, LANES), F32)

    def turn(x, by):
        return pltpu.roll(x, lax.rem(by + LANES, LANES), 1)

    def shift(x, by):
        return pltpu.roll(x, by % LANES, 1) if by % LANES else x

    def widen(x):
        return x if x.shape[1] == LANES else jnp.concatenate([x, jnp.zeros((x.shape[0], LANES - x.shape[1]), F32)], axis=1)

    def pack(nat, packed, corner, lo, hi):
        group8 = lax.rem(lane + (LANES - src8), LANES) // SUB
        groups = [group8 == g for g in range(GROUPS)]

        def body(o, carry):
            for q in range(PIECES):
                out = None
                for g in range(min(GROUPS, N - GROUPS * q)):
                    t = GROUPS * q + g
                    if t % TILES == 0:
                        plane = widen(nat[o * SUB + t // TILES, 0:N, :])
                    x = shift(plane[SUB * (t % TILES):SUB * (t % TILES) + SUB], SUB * g)
                    out = x if g == 0 else pick(groups[g], x, out)
                packed[o * PIECES + q] = out
            out = None
            for g in range(SUB):
                x = widen(nat[o * SUB + g, pl.ds(near_y, SUB), :])
                x = shift(x, SUB * g)
                out = x if g == 0 else pick(groups[g], x, out)
            corner[o] = out
            return carry
        lax.fori_loop(lo, hi, body, 0)

    def unpack(own, side, nat, packed, corner, fill, wall, o, carry):
        by = dst8 - (N - H - src8)
        packs, corner_in = [turn(packed[o * PIECES + q], by) for q in range(PIECES)], turn(corner[o], by)
        for pi in range(SUB):
            i, out = o * SUB + pi, []
            plane = widen(own[i, 0:N, :])
            for jt in range(NB):
                if jt < TILES:
                    t = pi * TILES + jt
                    got, g = packs[t // GROUPS], t % GROUPS
                else:
                    got, g = corner_in, pi
                x = plane[SUB * jt:SUB * jt + SUB] if jt < TILES else widen(side[i])
                other = fill if wall is None else pick(at_wall, wall_column(i, jt), fill)
                out.append(pick(own_lane, x, pick(ghost8, shift(got, -SUB * g), other)))
            nat[i, 0:E, :] = jnp.concatenate(out, axis=0)
        return carry

    def wall_column(i, jt):
        at = SUB * jt if jt < TILES else pl.multiple_of(N + 48 * cy, SUB)
        return pltpu.roll(wz_t[pl.ds(at, SUB), :], LANES - UNIT - i, 1)

    for copy in loads[0] + loads[1]:
        copy.wait()
    last_x, last_y, last_z = (N - UNIT) * (1 - cx), (N - UNIT) * (1 - cy), (N - UNIT) * (1 - cz)

    slots = lax.rem(lane + (LANES - last_z), LANES)

    def pack_one(o, carry):
        for n, src in enumerate((k_in, u_in)):
            row_s[n, pl.ds(pl.multiple_of(o * SUB, SUB), SUB), :] = jnp.concatenate(
                [src[o * SUB + r, pl.ds(last_y, 1), :] for r in range(SUB)], axis=0)
            out = None
            for t in range(N):
                if t % TILES == 0:
                    plane = widen(src[o * SUB + t // TILES])
                x = shift(plane[SUB * (t % TILES):SUB * (t % TILES) + SUB], t)
                out = x if t == 0 else pick(slots == t, x, out)
            lane_s[n, o] = out
        return carry
    planes(0, TILES, pack_one, 0, 3)
    pl.semaphore_wait(barrier, len(OTHERS))
    one_x = [send(0, k_in.at[pl.ds(last_x, 1)], kx, (1, 0, 0)), send(1, u_in.at[pl.ds(last_x, 1)], ux, (1, 0, 0))]
    one_y = send(2, row_s, row_r, (0, 1, 0))
    one_z = send(3, lane_s, lane_r, (0, 0, 1))
    k_y = send(4, k_in.at[:, pl.ds(near_y, SUB), :], ky, (0, 1, 0))
    pack(k_in, zs.at[0], ds_.at[0], 0, TILES)
    k_z = send(PIECES, zs.at[0], zr.at[0], (0, 0, 1))
    k_d = send(6, ds_.at[0], dr.at[0], (0, 1, 1))

    for n in (3, 4, PIECES):
        loads[n][0].wait()

    def lane_ring(w, at, c):
        left, right = walls[w, pl.ds(at, SUB), 0:LANES], walls[w, pl.ds(at, SUB), LANES:144]
        gap = jnp.zeros((SUB, 56), F32)
        right = jnp.concatenate([gap, right, gap], axis=1)
        turned = jnp.where(jnp.logical_and(lane >= 56, lane < N), right, pltpu.roll(left, 56, 1))
        return jnp.where(c == 0, left, turned)

    for jt in range(NB):
        at_j = pl.multiple_of(N * cy + SUB * jt if jt < TILES else N - H * cy, SUB)
        at_i = pl.multiple_of(N * cx + SUB * jt if jt < TILES else N - H * cx, SUB)
        k_nat[E, pl.ds(SUB * jt, SUB), :] = lane_ring(0, at_j, cz)
        wy[pl.ds(SUB * jt, SUB), :] = lane_ring(1, at_i, cz)
        if jt < TILES:
            wz[pl.ds(SUB * jt, SUB), :] = lane_ring(2, at_i, cy)
    wz_t[...] = turn(wz[...].T, wall_lane + UNIT)

    for copy in loads[2]:
        copy.wait()

    def take_f(p, carry):
        for b in range(NB):
            rows = SUB if b < 2 else LAST
            v0_a[p, b, 0:rows, 0:N] = f_in[p, pl.ds(b, rows, stride=NB), :]
        return carry
    planes(0, N, take_f, 0)

    def lay_out(i, carry):
        side = jnp.concatenate([pick(at_wall, wall_column(i, jt), ones) for jt in range(TILES)], axis=0)
        for nat, src, rest in ((k_nat, k_in, side), (u_nat, u_in, jnp.zeros((N, LANES), F32))):
            nat[i, 0:N, N:] = rest[:, N:]
            nat[i, 0:N, 0:N] = src[i]
        return carry
    planes(0, N, lay_out, 0)

    u_nat[E - UNIT - LAST * cx] = jnp.zeros((E, LANES), F32)
    one_lane = N + 55 * cz
    at_one = lane == one_lane
    for copy in one_x + [one_y, one_z]:
        copy.wait()
    u_nat[N + LAST * cx, 0:N, 0:N] = ux[0]
    k_nat[E + UNIT, 0:N, 0:N] = kx[0]

    def unpack_one(o, carry):
        for n, nat in enumerate((k_nat, u_nat)):
            got = turn(lane_r[n, o], one_lane - (N - 1 - last_z))
            for t in range(N):
                here = nat.at[o * SUB + t // TILES, pl.ds(SUB * (t % TILES), SUB), :]
                pltpu.store(here, shift(got, -t), mask=at_one)
        return carry
    lax.fori_loop(0, TILES, unpack_one, 0)

    row0 = sub == 0
    row72 = sub == LAST

    def divergence(h_x, h_xn, h_y, h_z, v, v_prev, v_next, low_row, high_row):
        low = row_down(v)
        high = v
        if low_row is not None:
            low = replace(low, 0, row0, low_row)
            high = replace(v, 2, row72, high_row)
        else:
            low = replace(low, 0, jnp.logical_and(row0, cy == 0), ZERO)
            high = replace(v, 2, jnp.logical_and(row72, cy == 1), ZERO)
        f_y = h_y * (high - low)
        f_z = h_z * (v - lane_down(v))
        return ((h_x * (v - v_prev) - h_xn * (v_next - v)) + (f_y - row_up(f_y))) + (f_z - lane_up(f_z))

    def full(row):
        return jnp.broadcast_to(widen(row), (SUB, LANES))

    def add_up(h_x, h_xn, h_y, h_z):
        return ((h_x + h_xn) + (h_y + row_up(h_y))) + (h_z + lane_up(h_z))

    def start_own(n, carry):
        p0 = WIDTH * n
        first_trip, last_trip = n == 0, n == N // WIDTH - UNIT
        k_p = [load_chunk(k_nat, jnp.where(first_trip, E + cx, p0 - UNIT))]
        u_p = [load_chunk(u_nat, jnp.where(first_trip, E - UNIT, p0 - UNIT))]
        for w in range(WIDTH):
            k_p.append(load_chunk(k_nat, p0 + w))
            u_p.append(load_chunk(u_nat, p0 + w))
        k_p.append(load_chunk(k_nat, jnp.where(last_trip, E + UNIT - cx, p0 + WIDTH)))
        u_p.append(load_chunk(u_nat, p0 + WIDTH))
        h_x = [harmonic(k_p[w + UNIT], k_p[w]) for w in range(WIDTH + UNIT)]
        for w in range(WIDTH):
            p, kc = p0 + w, k_p[w + UNIT]
            wall, got = full(wy[pl.ds(p, 1), :]), full(row_r[0, pl.ds(p, 1), :])
            low = replace(row_down(kc), 0, row0, jnp.where(cy == 0, wall, got))
            high = replace(kc, 2, row72, jnp.where(cy == 0, got, wall))
            h_y = harmonic(high, low)
            h_z = harmonic(kc, lane_down(kc))
            inv = lax.rsqrt(add_up(h_x[w], h_x[w + UNIT], h_y, h_z))
            got = full(row_r[1, pl.ds(p, 1), :])
            a_u = divergence(h_x[w], h_x[w + UNIT], h_y, h_z, u_p[w + UNIT], u_p[w], u_p[w + 2],
                             jnp.where(cy == 0, ZERO, got), jnp.where(cy == 0, got, ZERO))
            y0 = (v0_a[p] - a_u) * inv
            for b in range(NB):
                v0_a[p, b] = y0[b] if b < 2 else pick(row72, zero, y0[b])
            z0 = y0 * inv
            for b in range(NB):
                if b < 2:
                    z_nat[p, pl.ds(b, SUB, stride=NB), :] = z0[b]
                else:
                    z_nat[p, pl.ds(b, LAST, stride=NB), :] = z0[b, :LAST]
        return carry
    z_copies = []
    for q in range(3):
        lax.fori_loop(6 * q, 6 * q + 6, start_own, 0)
        rows = pl.ds(PART * q, PART)
        z_copies.append(send(7 + q, z_nat.at[rows, pl.ds(near_y, SUB), :], z_nat.at[rows, pl.ds(N, SUB), :], (0, 1, 0)))
        pack(z_nat, zs.at[1], ds_.at[1], 3 * q, 3 * q + 3)
        lanes = pl.ds(15 * q, 15)
        z_copies.append(send(12 + q, zs.at[1, lanes], zr.at[1, lanes], (0, 0, 1)))
    z_copies.append(send(15, ds_.at[1], dr.at[1], (0, 1, 1)))

    def spread(n, nat, take):
        take(SUB * (1 - cx), 0)
        copy = send(n, nat.at[pl.ds(near_x, SUB)], nat.at[pl.ds(N, SUB)], (1, 0, 0))
        lax.fori_loop(0, SUB, lambda o, carry: take(o + cx, carry), 0)
        return copy

    for copy in (k_y, k_z, k_d):
        copy.wait()
    spread(NB, k_nat, functools.partial(unpack, k_in, ky, k_nat, zr.at[0], dr.at[0], ones, wz_t)).wait()

    def faces(p, carry):
        kc = load_chunk(k_nat, p)
        before = jnp.where(jnp.logical_and(p == 0, cx == 0), E, jnp.where(p == 0, E - UNIT, p - UNIT))
        here = jnp.where(jnp.logical_and(p == N, cx == 1), E, p)
        cx_a[p] = harmonic(load_chunk(k_nat, here), load_chunk(k_nat, before))
        wall = full(wy[pl.ds(p, 1), :])
        low = replace(row_down(kc), 0, jnp.logical_and(row0, cy == 0), wall)
        high = replace(kc, 2, jnp.logical_and(row72, cy == 1), wall)
        cy_a[p] = harmonic(high, low)
        cz_a[p] = harmonic(kc, lane_down(kc))
        return carry
    planes(0, E, faces, 0, SUB)
    cx_a[E] = cx_a[0]
    cx_a[E + UNIT] = cx_a[1]

    def scales(own, p, carry):
        d = add_up(cx_a[p], cx_a[p + UNIT], cy_a[p], cz_a[p])
        inv = lax.rsqrt(d)
        isd_a[p] = inv
        if own:
            sd = d * inv
            for b in range(NB):
                k_nat[p, pl.ds(SUB * b, SUB), :] = sd[b] if b < 2 else pick(row72, zero, sd[b])
        return carry
    planes(0, N, functools.partial(scales, True), 0, SUB)
    planes(N, E, functools.partial(scales, False), 0, SUB)

    for copy in z_copies:
        copy.wait()
    z_x = spread(11, z_nat, functools.partial(unpack, z_nat, z_nat.at[:, pl.ds(N, SUB), :], z_nat, zr.at[1], dr.at[1],
                                              zero, None))

    def column(ref, p, b, width):
        return ref[pl.ds(p, width), b]

    def z_column(p, b, width=1):
        return z_nat[pl.ds(p, width), pl.ds(b, SUB, stride=NB), :]

    def tally(carry, b, products):
        return [c + jnp.sum(products[n // 2], axis=0) if n % 2 == (b > 1) else c for n, c in enumerate(carry)]

    def first(own, width, p, carry, before=None, after=None, x_after=None):
        before = p - UNIT if before is None else before
        z, inv, low, f_y, h_y = {}, {}, {}, {}, {}

        def load(b):
            z[b], inv[b], h_y[b] = z_column(p, b, width), column(isd_a, p, b, width), column(cy_a, p, b, width)
            under = z[b - UNIT] if b else pltpu.roll(z_column(p, NB - UNIT, width), 1, 1)
            over = z[b]
            if b == 0:
                under = jnp.where(jnp.logical_and(row0, cy == 0), ZERO, under)
            if b == 2:
                over = jnp.where(jnp.logical_and(row72, cy == 1), ZERO, over)
            f_y[b] = h_y[b] * (over - under)
        carry = list(carry)
        load(0)
        for b in range(NB):
            if b < NB - UNIT:
                load(b + UNIT)
            up = f_y[b + UNIT] if b < NB - UNIT else pltpu.roll(f_y[0], LAST, 1)
            z_p = z_column(before, b)
            z_n = z_column(p + width if after is None else after, b)
            if isinstance(p, int) and p == 0:
                z_p = jnp.where(cx == 0, ZERO, z_p)
            if isinstance(p, int) and p == N - UNIT:
                z_n = jnp.where(cx == 1, ZERO, z_n)
            if x_after is None:
                h_x = column(cx_a, p, b, width + UNIT)
            else:
                h_x = jnp.concatenate([column(cx_a, p, b, 1), column(cx_a, x_after, b, 1)], axis=0)
            f_x = h_x * (jnp.concatenate([z[b], z_n], axis=0) - jnp.concatenate([z_p, z[b]], axis=0))
            h_z = column(cz_a, p, b, width)
            f_z = h_z * (z[b] - lane_down(z[b]))
            b0 = inv[b] * (((f_x[:width] - f_x[1:]) + (f_y[b] - up)) + (f_z - lane_up(f_z)))
            b_a[0][pl.ds(p + UNIT, width), b] = b0
            twice = TWO * inv[b]
            side = column(isd_a, before, b, 1)
            if width > 1:
                side = jnp.concatenate([side, inv[b][:width - UNIT]], axis=0)
            cx_a[pl.ds(p, width), b] = h_x[:width] * (twice * side)
            side = inv[b - UNIT] if b else pltpu.roll(column(isd_a, p, NB - UNIT, width), 1, 1)
            c_y = h_y[b] * (twice * side)
            if b == 0:
                c_y = jnp.where(jnp.logical_and(row0, cy == 0), ZERO, c_y)
            if b == 2:
                c_y = jnp.where(jnp.logical_and(row72, cy == 1), ZERO, c_y)
            cy_a[pl.ds(p, width), b] = c_y
            cz_a[pl.ds(p, width), b] = jnp.where(at_edge, ZERO, h_z * (twice * lane_down(inv[b])))
            if own:
                v0 = column(v0_a, p, b, width)
                carry = tally(carry, b, (v0 * v0, v0 * b0, b0 * b0))
        return tuple(carry)

    at_edge = lane == N * cz

    def wrap(ref):
        ref[0] = jnp.where(cx == 0, ref[1], ref[E])
        ref[E + UNIT] = ref[1]
        ref[N + UNIT] = jnp.where(cx == 1, ref[N], ref[N + UNIT])

    sums = lax.fori_loop(0, 14, lambda n, carry: first(True, PIECES, 1 + PIECES * n, carry), (zero,) * 6)
    z_x.wait()
    sums = first(True, 1, 0, sums, E - UNIT, None, E + UNIT)
    sums = first(True, 1, N - UNIT, sums)
    first(False, WIDTH, N, ())
    first(False, WIDTH, N + WIDTH, (), None, 0)
    cx_a[0] = jnp.where(cx == 0, ZERO, cx_a[0])
    cx_a[N] = jnp.where(cx == 1, ZERO, cx_a[N])
    cx_a[E] = cx_a[0]
    wrap(b_a[0])
    acc[0] = own_cells(sums[0], sums[1])
    acc[1] = own_cells(sums[2], sums[3])
    acc[TILES] = own_cells(sums[4], sums[PIECES])
    acc[23] = zero

    def advance(k, own, width, p, carry):
        old, carry = b_a[k - UNIT], list(carry)
        v_low = pltpu.roll(column(old, p + UNIT, NB - UNIT, width), 1, 1)
        v, c_y = column(old, p + UNIT, 0, width), column(cy_a, p, 0, width)
        t_first = c_y * v
        for b in range(NB):
            if b < NB - UNIT:
                v_high, c_high = column(old, p + UNIT, b + UNIT, width), column(cy_a, p, b + UNIT, width)
                t_high = c_high * v_high
            else:
                t_high = pltpu.roll(t_first, LAST, 1)
            c_x, c_z = column(cx_a, p, b, width + UNIT), column(cz_a, p, b, width)
            below, above = column(old, p, b, 1), column(old, p + width + UNIT, b, 1)
            if width > 1:
                below = jnp.concatenate([below, v[:width - UNIT]], axis=0)
                above = jnp.concatenate([v[1:], above], axis=0)
            new = c_x[:width] * below + c_x[1:] * above
            new = new + (c_y * v_low + t_high)
            new = new + (c_z * lane_down(v) + lane_up(c_z * v))
            new = HALF * new if k == 1 else new - column(b_a[k - 2], p + UNIT, b, width)
            b_a[k][pl.ds(p + UNIT, width), b] = new
            if own:
                carry = tally(carry, b, (column(v0_a, p, b, width) * new, v * new, new * new))
            v_low, v, c_y = v, v_high, c_high
        return tuple(carry)

    for k in range(1, STEPS):
        sums = lax.fori_loop(0, N // SUB, lambda n, carry: advance(k, True, SUB, SUB * n, carry), (zero,) * 6)
        if k < STEPS - UNIT:
            depth = (STEPS - k) // PAIR * PAIR
            advance(k, False, depth, N + (H - depth) * cx, ())
            wrap(b_a[k])
        acc[1 + k] = own_cells(sums[0], sums[1])
        acc[GROUPS + k - UNIT] = own_cells(sums[2], sums[3])
        if k < STEPS - UNIT:
            acc[TILES + k] = own_cells(sums[4], sums[PIECES])

    def gather(buf, n_sem):
        copies = []
        for n, flips in enumerate(OTHERS):
            copies.append(pltpu.make_async_remote_copy(
                src_ref=buf.at[me], dst_ref=buf.at[me], send_sem=all_send.at[n_sem, n], recv_sem=all_recv.at[n_sem, n],
                device_id=peer(*flips), device_id_type=MESH))
        for copy in copies:
            copy.start()
        return copies

    hi = acc[:, 0, :]
    lo = jnp.zeros((NDOT, LANES), F32)
    for s in range(1, SUB):
        hi, err = two_sum(hi, acc[:, s, :])
        lo = lo + err
    gath[me, 0:NDOT] = hi
    gath[me, NDOT:2 * NDOT] = lo
    gath_copies = gather(gath, 0)
    pair = {}
    for i in range(HEAD + UNIT):
        for j in range(i, HEAD + UNIT):
            pair[i, j] = len(pair)

    def products(n, carry):
        p, carry = WIDTH * n, list(carry)
        for b in range(NB):
            sd = k_nat[pl.ds(p, WIDTH), pl.ds(SUB * b, SUB), :]
            w = [sd * column(v0_a, p, b, WIDTH)] + [sd * column(b_a[j], p + UNIT, b, WIDTH) for j in range(HEAD)]
            for (i, j), at in pair.items():
                carry[at] = carry[at] + jnp.sum(w[i] * w[j], axis=0)
        return tuple(carry)
    gram = lax.fori_loop(0, N // WIDTH, products, (zero,) * len(pair))
    for copy in gath_copies:
        copy.wait()
    hi, lo = gath[0, 0:NDOT], gath[0, NDOT:2 * NDOT]
    for dev in range(1, SUB):
        hi, err = two_sum(hi, gath[dev, 0:NDOT])
        lo = lo + (gath[dev, NDOT:2 * NDOT] + err)
    for shift in (64, 32, GROUPS, SUB, 4, 2, 1):
        hi, err = two_sum(hi, pltpu.roll(hi, shift, 1))
        lo = (lo + pltpu.roll(lo, shift, 1)) + err
    hi, lo = quick(hi, lo)
    size = hi[0:1]
    factor = jnp.where(size > 1e30, TWO ** -110, jnp.where(size > 1e12, TWO ** -60, jnp.where(
        size < 1e-30, TWO ** 110, jnp.where(size < 1e-12, TWO ** 60, ONE)))).astype(F32)
    hi, lo = hi * factor, lo * factor

    def total(row):
        return jnp.broadcast_to(hi[row:row + UNIT], (SUB, LANES)), jnp.broadcast_to(lo[row:row + UNIT], (SUB, LANES))

    n_mom = [total(TILES), total(GROUPS)]
    for j in range(1, LAST):
        n_mom.append(dsub(dscale(total(TILES + j), TWO), n_mom[0]))
        n_mom.append(dsub(dscale(total(GROUPS + j), TWO), n_mom[1]))
    l_mom = [total(1 + j) for j in range(SUB)]
    for j in range(LAST, 14):
        l_mom.append(dsub(dscale(dsub(l_mom[j], n_mom[j]), TWO), l_mom[j - UNIT]))
    m_mom = [total(0)]
    m_mom.append(dsub(m_mom[0], l_mom[0]))
    for j in range(1, 15):
        m_mom.append(dsub(dscale(dsub(m_mom[j], l_mom[j]), TWO), m_mom[j - UNIT]))
    ys, xs = basis_coefs(*step_lengths(m_mom))
    slot = {}
    for t in range(STEPS):
        for j in range(t + UNIT):
            slot[t, j] = len(slot)
            coef[slot[t, j]] = ys[t][1 + j]
    for j in range(SUB):
        slot['x', j] = len(slot)
        coef[slot['x', j]] = xs[j]

    def put(ref, p, b0, val):
        for b in range(val.shape[0]):
            if b0 + b < 2:
                ref[p, pl.ds(b0 + b, SUB, stride=NB), :] = val[b, :, :N]
            else:
                ref[p, pl.ds(b0 + b, LAST, stride=NB), :] = val[b, :LAST, :N]

    def residuals(p, carry):
        carry = list(carry)
        for b0 in range(0, NB, 2):
            cut = pl.ds(b0, 2)
            v0 = v0_a[p, cut]
            sd = jnp.stack([k_nat[p, pl.ds(SUB * (b0 + b), SUB), :] for b in range(2)], axis=0)
            bs = [ref[p + UNIT, cut] for ref in b_a]
            for t in range(HEAD, STEPS):
                y = v0
                for j in range(t + UNIT):
                    y = y + coef[slot[t, j]] * bs[j]
                r = sd * y
                which = 2 * (t - HEAD) + (b0 > 0)
                carry[which] = carry[which] + jnp.sum(r * r, axis=0)
                if t == STEPS - UNIT:
                    put(f_in, p, b0, r)
        return tuple(carry)

    sums = lax.fori_loop(0, N, residuals, (zero,) * (2 * (STEPS - HEAD)))
    for t in range(STEPS):
        if t < HEAD:
            form = zero
            g = [None] + [coef[slot[t, j]] for j in range(t + 1)]
            for i in range(t + 2):
                part = gram[pair[0, i]] if not i else g[i] * gram[pair[0, i]]
                form = form + (part if not i else part + part)
            for i in range(UNIT, t + 2):
                part = zero
                for j in range(UNIT, t + 2):
                    part = part + g[j] * gram[pair[min(i, j), max(i, j)]]
                form = form + g[i] * part
            rsend[t] = pick(own_lane, form, zero)
        else:
            rsend[t] = own_cells(sums[2 * (t - HEAD)], sums[2 * (t - HEAD) + UNIT])
    part = rsend[:, 0, :]
    for s in range(1, SUB):
        part = part + rsend[:, s, :]
    rgath[me] = part
    rr_copies = gather(rgath, 1)

    def update(p, carry):
        for b0 in range(0, NB, 2):
            cut = pl.ds(b0, 2)
            x = coef[slot['x', 0]] * v0_a[p, cut]
            for j in range(1, SUB):
                x = x + coef[slot['x', j]] * b_a[j - UNIT][p + UNIT, cut]
            x = x * isd_a[p, cut]
            u = jnp.stack([u_nat[p, pl.ds(b0 + b, SUB, stride=NB), :] for b in range(2)], axis=0)
            put(k_in, p, b0, u + x)
        return carry

    lax.fori_loop(0, N, update, 0)
    for copy in rr_copies:
        copy.wait()
    part = rgath[0]
    for dev in range(1, SUB):
        part = part + rgath[dev]
    part = jnp.broadcast_to(jnp.sum(part, axis=1, keepdims=True), (SUB, LANES))
    rr_ref[...] = jnp.sum(jnp.where(lane == sub, part, ZERO), axis=0, keepdims=True)[:, :STEPS]


def solution(mesh):
    spec = P('gx', 'gy', 'gz')

    def local(k_cell, k_ghost, f_rhs, u_init):
        big = (E, NB, SUB, LANES)
        ext = (E + 2, NB, SUB, LANES)
        vm = lambda *shape: pltpu.VMEM(shape, F32)
        any_spec = pl.BlockSpec(memory_space=pl.ANY)
        u, r, rr = pl.pallas_call(
            kernel,
            out_shape=(vm(N, N, N), vm(N, N, N), vm(1, STEPS)),
            in_specs=[any_spec] * 4,
            out_specs=[pl.BlockSpec(memory_space=pltpu.VMEM)] * 3,
            scratch_shapes=[
                vm(N, N, N), vm(E + 2, E, LANES), vm(E, E, LANES), vm(E, E, LANES),
                vm(*ext), vm(*big), vm(*big), vm(*big), vm(N, NB, SUB, LANES),
                *[vm(E + 2, NB, SUB, LANES)] * STEPS,
                vm(3, 144, 144), vm(LANES, LANES), vm(LANES, LANES), vm(E, LANES), vm(N, SUB, N), vm(1, N, N), vm(1, N, N),
                vm(2, 45, SUB, LANES), vm(2, 45, SUB, LANES), vm(2, TILES, SUB, LANES), vm(2, TILES, SUB, LANES),
                vm(2, N, N), vm(2, N, N), vm(2, TILES, SUB, LANES), vm(2, TILES, SUB, LANES),
                vm(NDOT, SUB, LANES), vm(SUB, 2 * NDOT, LANES), vm(SUB, SUB, LANES), vm(SUB, SUB, LANES), vm(44, SUB, LANES),
                pltpu.SemaphoreType.DMA((6, 3)),
                pltpu.SemaphoreType.DMA((16,)), pltpu.SemaphoreType.DMA((16,)),
                pltpu.SemaphoreType.DMA((2, LAST)), pltpu.SemaphoreType.DMA((2, LAST)),
            ],
            compiler_params=pltpu.CompilerParams(collective_id=0, has_side_effects=True, vmem_limit_bytes=57 << 20),
        )(k_cell, f_rhs, u_init, k_ghost)
        return u, r, rr.reshape(STEPS)

    return jax.shard_map(local, mesh=mesh, in_specs=(spec, P(), spec, spec), out_specs=(spec, spec, P()), check_vma=False)
```

```python
import functools

import jax
import jax.numpy as jnp
from jax import lax
from jax.experimental import pallas as pl
from jax.experimental.pallas import tpu as pltpu
from jax.sharding import PartitionSpec as P


N = 72
H = 8
E = N + H
NB = 10
STEPS = 8
MESH = pl.DeviceIdType.MESH
F32 = jnp.float32
OTHERS = [(fx, fy, fz) for fx in (0, 1) for fy in (0, 1) for fz in (0, 1) if fx or fy or fz]
NDOT = 24
SUB = 8
LANES = 128
TILES = 9
PART = 24
WIDTH = 4
LAST = 7
GROUPS = 16
PIECES = 5
ZERO, ONE, HALF, TWO = 0.0, 1.0, 0.5, 2.0
UNIT = 1
HEAD = 4
PAIR = 2


def iota(axis):
    return lax.broadcasted_iota(jnp.int32, (SUB, LANES), axis)


def two_sum(a, b):
    s = a + b
    t = s - a
    return s, (a - (s - t)) + (b - t)


def quick(a, b):
    s = a + b
    return s, b - (s - a)


def two_prod(a, b):
    def split(x):
        t = x * 4097.0
        hi = t - (t - x)
        return hi, x - hi
    p = a * b
    ah, al = split(a)
    bh, bl = split(b)
    return p, ((ah * bh - p) + ah * bl + al * bh) + al * bl


def dadd(x, y):
    (xh, xl), (yh, yl) = x, y
    s, e = two_sum(xh, yh)
    return quick(s, e + (xl + yl))


def dsub(x, y):
    yh, yl = y
    return dadd(x, (-yh, -yl))


def dscale(x, c):
    hi, lo = x
    return hi * c, lo * c


def dmul(x, y):
    (xh, xl), (yh, yl) = x, y
    p, e = two_prod(xh, yh)
    return quick(p, e + (xh * yl + xl * yh))


def ddiv(x, y):
    (xh, xl), (yh, yl) = x, y
    q = xh / yh
    p, e = two_prod(q, yh)
    rest = ((xh - p) - e) + (xl - q * yl)
    return quick(q, rest / yh)


def step_lengths(m):
    alphas, betas = [], []
    y = dict(enumerate(m))
    p = {0: dsub(y[0], y[1])}
    for l in range(1, 15):
        p[l] = dsub(y[l], dscale(dadd(y[l + UNIT], y[l - UNIT]), HALF))
    for t in range(STEPS):
        alpha = ddiv(y[t], p[t])
        alphas.append(alpha[0])
        if t == STEPS - UNIT:
            break
        y_next = {l: dsub(y[l], dmul(alpha, p[l])) for l in range(t + UNIT, 15 - t)}
        beta = ddiv(y_next[t + UNIT], p[t])
        if t:
            beta = dscale(beta, HALF)
        betas.append(beta[0])
        p_next = {}
        for l in range(t + UNIT, 14 - t):
            side = y_next[l + UNIT] if l == t + UNIT else dadd(y_next[l + UNIT], y_next[l - UNIT])
            p_next[l] = dadd(dsub(y_next[l], dscale(side, HALF)), dmul(beta, p[l]))
        y, p = y_next, p_next
    return alphas, betas


def basis_coefs(alphas, betas):
    def add(a, b):
        return b if a is None else (a if b is None else a + b)

    def axpy(x, c, y):
        return [xi if yi is None else (c * yi if xi is None else xi + c * yi) for xi, yi in zip(x, y)]

    def apply_op(v):
        out = [None] * 11
        out[1] = v[0]
        for j in range(SUB):
            if v[1 + j] is None:
                continue
            c = v[1 + j]
            out[1 + j] = add(out[1 + j], c)
            if j == 0:
                out[2] = add(out[2], -c)
            else:
                half = -HALF * c
                out[2 + j] = add(out[2 + j], half)
                out[j] = add(out[j], half)
        return out[:TILES]

    one = jnp.ones_like(alphas[0])
    y = [one] + [None] * SUB
    p = list(y)
    x = [None] * TILES
    ys = []
    for t in range(STEPS):
        q = apply_op(p)
        x = axpy(x, alphas[t], p)
        y = axpy(y, -alphas[t], q)
        ys.append(y)
        if t < STEPS - UNIT:
            p = axpy(y, betas[t], p)
    return ys, x


def row_down(v):
    return jnp.concatenate([pltpu.roll(v[NB - UNIT], 1, 0)[None], v[:NB - UNIT]], axis=0)


def row_up(v):
    return jnp.concatenate([v[1:], pltpu.roll(v[0], LAST, 0)[None]], axis=0)


def lane_down(v):
    return pltpu.roll(v, 1, 2)


def lane_up(v):
    return pltpu.roll(v, 127, 2)


def load_chunk(ref, plane):
    return jnp.stack([ref[plane, pl.ds(b, SUB, stride=NB), :] for b in range(NB)], axis=0)


def replace(v, b, mask, value):
    return jnp.concatenate(([v[:b]] if b else []) + [jnp.where(mask, value, v[b])[None], v[b + UNIT:]], axis=0)


def harmonic(a, b):
    return TWO * a * b / (a + b)


def pick(mask, a, b):
    return lax.select_n(mask, b, a)


def planes(lo, hi, body, init, width=WIDTH):
    def some(n, carry):
        for w in range(width):
            carry = body(lo + n * width + w, carry)
        return carry
    return lax.fori_loop(0, (hi - lo) // width, some, init)


def own_cells(low, high):
    sub, lane = iota(0), iota(1)
    return jnp.where(lane < N, low + jnp.where(sub < LAST, high, ZERO), ZERO)


def kernel(k_hbm, f_hbm, u_hbm, kg_hbm, k_in, f_in, rr_ref,
           u_in, k_nat, u_nat, z_nat, cx_a, cy_a, cz_a, isd_a, v0_a, b0_a, b1_a, b2_a, b3_a, b4_a, b5_a, b6_a, b7_a,
           walls, wz, wz_t, wy, ky, kx, ux, zs, zr, ds_, dr, row_s, row_r, lane_s, lane_r, acc, gath, rsend, rgath, coef,
           load_sem, send_sem, recv_sem, all_send, all_recv):
    cx, cy, cz = lax.axis_index('gx'), lax.axis_index('gy'), lax.axis_index('gz')
    me = cx + 2 * cy + 4 * cz
    b_a = (b0_a, b1_a, b2_a, b3_a, b4_a, b5_a, b6_a, b7_a)
    lane, sub = iota(1), iota(0)

    def peer(fx, fy, fz):
        out = {}
        if fx:
            out['gx'] = 1 - cx
        if fy:
            out['gy'] = 1 - cy
        if fz:
            out['gz'] = 1 - cz
        return out

    loads = []
    for n, (src, dst) in enumerate([(k_hbm, k_in), (u_hbm, u_in), (f_hbm, f_in)]):
        loads.append([pltpu.make_async_copy(src.at[pl.ds(PART * q, PART)], dst.at[pl.ds(PART * q, PART)], load_sem.at[n, q])
                      for q in range(N // PART)])
    loads.append([pltpu.make_async_copy(kg_hbm.at[cx], walls.at[0], load_sem.at[3, 0])])
    loads.append([pltpu.make_async_copy(kg_hbm.at[2 + cy], walls.at[1], load_sem.at[4, 0])])
    loads.append([pltpu.make_async_copy(kg_hbm.at[4 + cz], walls.at[2], load_sem.at[PIECES, 0])])
    for n in (0, 1, 3, 4, PIECES, 2):
        for copy in loads[n]:
            copy.start()

    barrier = pltpu.get_barrier_semaphore()
    for flips in OTHERS:
        pl.semaphore_signal(barrier, inc=1, device_id=peer(*flips), device_id_type=MESH)

    def send(n, src, dst, flips):
        copy = pltpu.make_async_remote_copy(src_ref=src, dst_ref=dst, send_sem=send_sem.at[n], recv_sem=recv_sem.at[n],
                                            device_id=peer(*flips), device_id_type=MESH)
        copy.start()
        return copy

    near_y = pl.multiple_of((N - H) * (1 - cy), SUB)
    near_x = (N - H) * (1 - cx)
    src8 = (N - H) * (1 - cz)
    dst8 = N + 48 * cz
    ghost8 = jnp.logical_and(lane >= dst8, lane < dst8 + SUB)
    wall_lane = 127 - 55 * cz
    own_lane = lane < N
    at_wall = lane == wall_lane
    zero = jnp.zeros((SUB, LANES), F32)
    ones = jnp.ones((SUB, LANES), F32)

    def turn(x, by):
        return pltpu.roll(x, lax.rem(by + LANES, LANES), 1)

    def shift(x, by):
        return pltpu.roll(x, by % LANES, 1) if by % LANES else x

    def widen(x):
        return x if x.shape[1] == LANES else jnp.concatenate([x, jnp.zeros((x.shape[0], LANES - x.shape[1]), F32)], axis=1)

    def pack(nat, packed, corner, lo, hi, width):
        group8 = lax.rem(lane + (LANES - src8), LANES) // SUB
        groups = [group8 == g for g in range(GROUPS)]

        def body(o, carry):
            for q in range(PIECES):
                out = None
                for g in range(min(GROUPS, N - GROUPS * q)):
                    t = GROUPS * q + g
                    if t % TILES == 0:
                        plane = widen(nat[o * SUB + t // TILES, 0:N, :])
                    x = shift(plane[SUB * (t % TILES):SUB * (t % TILES) + SUB], SUB * g)
                    out = x if g == 0 else pick(groups[g], x, out)
                packed[o * PIECES + q] = out
            out = None
            for g in range(SUB):
                x = widen(nat[o * SUB + g, pl.ds(near_y, SUB), :])
                x = shift(x, SUB * g)
                out = x if g == 0 else pick(groups[g], x, out)
            corner[o] = out
            return carry
        planes(lo, hi, body, 0, width)

    def unpack(own, side, nat, packed, corner, fill, wall, o, carry):
        by = dst8 - (N - H - src8)
        packs, corner_in = [turn(packed[o * PIECES + q], by) for q in range(PIECES)], turn(corner[o], by)
        for pi in range(SUB):
            i, out = o * SUB + pi, []
            plane = widen(own[i, 0:N, :])
            for jt in range(NB):
                if jt < TILES:
                    t = pi * TILES + jt
                    got, g = packs[t // GROUPS], t % GROUPS
                else:
                    got, g = corner_in, pi
                x = plane[SUB * jt:SUB * jt + SUB] if jt < TILES else widen(side[i])
                other = fill if wall is None else pick(at_wall, wall_column(i, jt), fill)
                out.append(pick(own_lane, x, pick(ghost8, shift(got, -SUB * g), other)))
            nat[i, 0:E, :] = jnp.concatenate(out, axis=0)
        return carry

    def wall_column(i, jt):
        at = SUB * jt if jt < TILES else pl.multiple_of(N + 48 * cy, SUB)
        return pltpu.roll(wz_t[pl.ds(at, SUB), :], LANES - UNIT - i, 1)

    for copy in loads[0] + loads[1]:
        copy.wait()
    last_x, last_y, last_z = (N - UNIT) * (1 - cx), (N - UNIT) * (1 - cy), (N - UNIT) * (1 - cz)

    slots = lax.rem(lane + (LANES - last_z), LANES)

    def pack_one(o, carry):
        for n, src in enumerate((k_in, u_in)):
            row_s[n, pl.ds(pl.multiple_of(o * SUB, SUB), SUB), :] = jnp.concatenate(
                [src[o * SUB + r, pl.ds(last_y, 1), :] for r in range(SUB)], axis=0)
            out = None
            for t in range(N):
                if t % TILES == 0:
                    plane = widen(src[o * SUB + t // TILES])
                x = shift(plane[SUB * (t % TILES):SUB * (t % TILES) + SUB], t)
                out = x if t == 0 else pick(slots == t, x, out)
            lane_s[n, o] = out
        return carry
    planes(0, TILES, pack_one, 0, 3)
    pl.semaphore_wait(barrier, len(OTHERS))
    one_x = [send(0, k_in.at[pl.ds(last_x, 1)], kx, (1, 0, 0)), send(1, u_in.at[pl.ds(last_x, 1)], ux, (1, 0, 0))]
    one_y = send(2, row_s, row_r, (0, 1, 0))
    one_z = send(3, lane_s, lane_r, (0, 0, 1))
    k_y = send(4, k_in.at[:, pl.ds(near_y, SUB), :], ky, (0, 1, 0))
    pack(k_in, zs.at[0], ds_.at[0], 0, TILES, UNIT)
    k_z = send(PIECES, zs.at[0], zr.at[0], (0, 0, 1))
    k_d = send(6, ds_.at[0], dr.at[0], (0, 1, 1))

    for n in (3, 4, PIECES):
        loads[n][0].wait()

    def lane_ring(w, at, c):
        left, right = walls[w, pl.ds(at, SUB), 0:LANES], walls[w, pl.ds(at, SUB), LANES:144]
        gap = jnp.zeros((SUB, 56), F32)
        right = jnp.concatenate([gap, right, gap], axis=1)
        turned = jnp.where(jnp.logical_and(lane >= 56, lane < N), right, pltpu.roll(left, 56, 1))
        return jnp.where(c == 0, left, turned)

    for jt in range(NB):
        at_j = pl.multiple_of(N * cy + SUB * jt if jt < TILES else N - H * cy, SUB)
        at_i = pl.multiple_of(N * cx + SUB * jt if jt < TILES else N - H * cx, SUB)
        k_nat[E, pl.ds(SUB * jt, SUB), :] = lane_ring(0, at_j, cz)
        wy[pl.ds(SUB * jt, SUB), :] = lane_ring(1, at_i, cz)
        if jt < TILES:
            wz[pl.ds(SUB * jt, SUB), :] = lane_ring(2, at_i, cy)
    wz_t[...] = turn(wz[...].T, wall_lane + UNIT)

    for copy in loads[2]:
        copy.wait()

    def take_f(p, carry):
        for b in range(NB):
            rows = SUB if b < 2 else LAST
            v0_a[p, b, 0:rows, 0:N] = f_in[p, pl.ds(b, rows, stride=NB), :]
        return carry
    planes(0, N, take_f, 0)

    def lay_out(i, carry):
        side = jnp.concatenate([pick(at_wall, wall_column(i, jt), ones) for jt in range(TILES)], axis=0)
        for nat, src, rest in ((k_nat, k_in, side), (u_nat, u_in, jnp.zeros((N, LANES), F32))):
            nat[i, 0:N, N:] = rest[:, N:]
            nat[i, 0:N, 0:N] = src[i]
        return carry
    planes(0, N, lay_out, 0)

    u_nat[E - UNIT - LAST * cx] = jnp.zeros((E, LANES), F32)
    one_lane = N + 55 * cz
    at_one = lane == one_lane
    for copy in one_x + [one_y, one_z]:
        copy.wait()
    u_nat[N + LAST * cx, 0:N, 0:N] = ux[0]
    k_nat[E + UNIT, 0:N, 0:N] = kx[0]

    def unpack_one(o, carry):
        for n, nat in enumerate((k_nat, u_nat)):
            got = turn(lane_r[n, o], one_lane - (N - 1 - last_z))
            for t in range(N):
                here = nat.at[o * SUB + t // TILES, pl.ds(SUB * (t % TILES), SUB), :]
                pltpu.store(here, shift(got, -t), mask=at_one)
        return carry
    lax.fori_loop(0, TILES, unpack_one, 0)

    row0 = sub == 0
    row72 = sub == LAST

    def divergence(h_x, h_xn, h_y, h_z, v, v_prev, v_next, low_row, high_row):
        low = row_down(v)
        high = v
        if low_row is not None:
            low = replace(low, 0, row0, low_row)
            high = replace(v, 2, row72, high_row)
        else:
            low = replace(low, 0, jnp.logical_and(row0, cy == 0), ZERO)
            high = replace(v, 2, jnp.logical_and(row72, cy == 1), ZERO)
        f_y = h_y * (high - low)
        f_z = h_z * (v - lane_down(v))
        return ((h_x * (v - v_prev) - h_xn * (v_next - v)) + (f_y - row_up(f_y))) + (f_z - lane_up(f_z))

    def full(row):
        return jnp.broadcast_to(widen(row), (SUB, LANES))

    def add_up(h_x, h_xn, h_y, h_z):
        return ((h_x + h_xn) + (h_y + row_up(h_y))) + (h_z + lane_up(h_z))

    def start_own(n, carry):
        p0 = WIDTH * n
        first_trip, last_trip = n == 0, n == N // WIDTH - UNIT
        k_p = [load_chunk(k_nat, jnp.where(first_trip, E + cx, p0 - UNIT))]
        u_p = [load_chunk(u_nat, jnp.where(first_trip, E - UNIT, p0 - UNIT))]
        for w in range(WIDTH):
            k_p.append(load_chunk(k_nat, p0 + w))
            u_p.append(load_chunk(u_nat, p0 + w))
        k_p.append(load_chunk(k_nat, jnp.where(last_trip, E + UNIT - cx, p0 + WIDTH)))
        u_p.append(load_chunk(u_nat, p0 + WIDTH))
        h_x = [harmonic(k_p[w + UNIT], k_p[w]) for w in range(WIDTH + UNIT)]
        for w in range(WIDTH):
            p, kc = p0 + w, k_p[w + UNIT]
            wall, got = full(wy[pl.ds(p, 1), :]), full(row_r[0, pl.ds(p, 1), :])
            low = replace(row_down(kc), 0, row0, jnp.where(cy == 0, wall, got))
            high = replace(kc, 2, row72, jnp.where(cy == 0, got, wall))
            h_y = harmonic(high, low)
            h_z = harmonic(kc, lane_down(kc))
            inv = lax.rsqrt(add_up(h_x[w], h_x[w + UNIT], h_y, h_z))
            got = full(row_r[1, pl.ds(p, 1), :])
            a_u = divergence(h_x[w], h_x[w + UNIT], h_y, h_z, u_p[w + UNIT], u_p[w], u_p[w + 2],
                             jnp.where(cy == 0, ZERO, got), jnp.where(cy == 0, got, ZERO))
            y0 = (v0_a[p] - a_u) * inv
            for b in range(NB):
                v0_a[p, b] = y0[b] if b < 2 else pick(row72, zero, y0[b])
            z0 = y0 * inv
            for b in range(NB):
                if b < 2:
                    z_nat[p, pl.ds(b, SUB, stride=NB), :] = z0[b]
                else:
                    z_nat[p, pl.ds(b, LAST, stride=NB), :] = z0[b, :LAST]
        return carry
    z_copies = []
    for q in range(3):
        lax.fori_loop(6 * q, 6 * q + 6, start_own, 0)
        rows = pl.ds(PART * q, PART)
        z_copies.append(send(7 + q, z_nat.at[rows, pl.ds(near_y, SUB), :], z_nat.at[rows, pl.ds(N, SUB), :], (0, 1, 0)))
        pack(z_nat, zs.at[1], ds_.at[1], 3 * q, 3 * q + 3, 3)
        lanes = pl.ds(15 * q, 15)
        z_copies.append(send(12 + q, zs.at[1, lanes], zr.at[1, lanes], (0, 0, 1)))
    z_copies.append(send(15, ds_.at[1], dr.at[1], (0, 1, 1)))

    def spread(n, nat, take):
        take(SUB * (1 - cx), 0)
        copy = send(n, nat.at[pl.ds(near_x, SUB)], nat.at[pl.ds(N, SUB)], (1, 0, 0))
        lax.fori_loop(0, SUB, lambda o, carry: take(o + cx, carry), 0)
        return copy

    for copy in (k_y, k_z, k_d):
        copy.wait()
    spread(NB, k_nat, functools.partial(unpack, k_in, ky, k_nat, zr.at[0], dr.at[0], ones, wz_t)).wait()

    def faces(p, carry):
        kc = load_chunk(k_nat, p)
        before = jnp.where(jnp.logical_and(p == 0, cx == 0), E, jnp.where(p == 0, E - UNIT, p - UNIT))
        here = jnp.where(jnp.logical_and(p == N, cx == 1), E, p)
        cx_a[p] = harmonic(load_chunk(k_nat, here), load_chunk(k_nat, before))
        wall = full(wy[pl.ds(p, 1), :])
        low = replace(row_down(kc), 0, jnp.logical_and(row0, cy == 0), wall)
        high = replace(kc, 2, jnp.logical_and(row72, cy == 1), wall)
        cy_a[p] = harmonic(high, low)
        cz_a[p] = harmonic(kc, lane_down(kc))
        return carry
    planes(0, E, faces, 0, SUB)
    cx_a[E] = cx_a[0]
    cx_a[E + UNIT] = cx_a[1]

    def scales(own, p, carry):
        d = add_up(cx_a[p], cx_a[p + UNIT], cy_a[p], cz_a[p])
        inv = lax.rsqrt(d)
        isd_a[p] = inv
        if own:
            sd = d * inv
            for b in range(NB):
                k_nat[p, pl.ds(SUB * b, SUB), :] = sd[b] if b < 2 else pick(row72, zero, sd[b])
        return carry
    planes(0, N, functools.partial(scales, True), 0, SUB)
    planes(N, E, functools.partial(scales, False), 0, SUB)

    for copy in z_copies:
        copy.wait()
    z_x = spread(11, z_nat, functools.partial(unpack, z_nat, z_nat.at[:, pl.ds(N, SUB), :], z_nat, zr.at[1], dr.at[1],
                                              zero, None))

    def column(ref, p, b, width):
        return ref[pl.ds(p, width), b]

    def z_column(p, b, width=1):
        return z_nat[pl.ds(p, width), pl.ds(b, SUB, stride=NB), :]

    def tally(carry, b, products):
        return [c + jnp.sum(products[n // 2], axis=0) if n % 2 == (b > 1) else c for n, c in enumerate(carry)]

    def first(own, width, p, carry, before=None, after=None, x_after=None):
        before = p - UNIT if before is None else before
        z, inv, low, f_y, h_y = {}, {}, {}, {}, {}

        def load(b):
            z[b], inv[b], h_y[b] = z_column(p, b, width), column(isd_a, p, b, width), column(cy_a, p, b, width)
            under = z[b - UNIT] if b else pltpu.roll(z_column(p, NB - UNIT, width), 1, 1)
            over = z[b]
            if b == 0:
                under = jnp.where(jnp.logical_and(row0, cy == 0), ZERO, under)
            if b == 2:
                over = jnp.where(jnp.logical_and(row72, cy == 1), ZERO, over)
            f_y[b] = h_y[b] * (over - under)
        carry = list(carry)
        load(0)
        for b in range(NB):
            if b < NB - UNIT:
                load(b + UNIT)
            up = f_y[b + UNIT] if b < NB - UNIT else pltpu.roll(f_y[0], LAST, 1)
            z_p = z_column(before, b)
            z_n = z_column(p + width if after is None else after, b)
            if isinstance(p, int) and p == 0:
                z_p = jnp.where(cx == 0, ZERO, z_p)
            if isinstance(p, int) and p == N - UNIT:
                z_n = jnp.where(cx == 1, ZERO, z_n)
            if x_after is None:
                h_x = column(cx_a, p, b, width + UNIT)
            else:
                h_x = jnp.concatenate([column(cx_a, p, b, 1), column(cx_a, x_after, b, 1)], axis=0)
            f_x = h_x * (jnp.concatenate([z[b], z_n], axis=0) - jnp.concatenate([z_p, z[b]], axis=0))
            h_z = column(cz_a, p, b, width)
            f_z = h_z * (z[b] - lane_down(z[b]))
            b0 = inv[b] * (((f_x[:width] - f_x[1:]) + (f_y[b] - up)) + (f_z - lane_up(f_z)))
            b_a[0][pl.ds(p + UNIT, width), b] = b0
            twice = TWO * inv[b]
            side = column(isd_a, before, b, 1)
            if width > 1:
                side = jnp.concatenate([side, inv[b][:width - UNIT]], axis=0)
            cx_a[pl.ds(p, width), b] = h_x[:width] * (twice * side)
            side = inv[b - UNIT] if b else pltpu.roll(column(isd_a, p, NB - UNIT, width), 1, 1)
            c_y = h_y[b] * (twice * side)
            if b == 0:
                c_y = jnp.where(jnp.logical_and(row0, cy == 0), ZERO, c_y)
            if b == 2:
                c_y = jnp.where(jnp.logical_and(row72, cy == 1), ZERO, c_y)
            cy_a[pl.ds(p, width), b] = c_y
            cz_a[pl.ds(p, width), b] = jnp.where(at_edge, ZERO, h_z * (twice * lane_down(inv[b])))
            if own:
                v0 = column(v0_a, p, b, width)
                carry = tally(carry, b, (v0 * v0, v0 * b0, b0 * b0))
        return tuple(carry)

    at_edge = lane == N * cz

    def wrap(ref):
        ref[0] = jnp.where(cx == 0, ref[1], ref[E])
        ref[E + UNIT] = ref[1]
        ref[N + UNIT] = jnp.where(cx == 1, ref[N], ref[N + UNIT])

    sums = lax.fori_loop(0, 14, lambda n, carry: first(True, PIECES, 1 + PIECES * n, carry), (zero,) * 6)
    z_x.wait()
    sums = first(True, 1, 0, sums, E - UNIT, None, E + UNIT)
    sums = first(True, 1, N - UNIT, sums)
    first(False, WIDTH, N, ())
    first(False, WIDTH, N + WIDTH, (), None, 0)
    cx_a[0] = jnp.where(cx == 0, ZERO, cx_a[0])
    cx_a[N] = jnp.where(cx == 1, ZERO, cx_a[N])
    cx_a[E] = cx_a[0]
    wrap(b_a[0])
    acc[0] = own_cells(sums[0], sums[1])
    acc[1] = own_cells(sums[2], sums[3])
    acc[TILES] = own_cells(sums[4], sums[PIECES])
    acc[23] = zero

    def advance(k, own, width, p, carry):
        old, carry = b_a[k - UNIT], list(carry)
        v_low = pltpu.roll(column(old, p + UNIT, NB - UNIT, width), 1, 1)
        v, c_y = column(old, p + UNIT, 0, width), column(cy_a, p, 0, width)
        t_first = c_y * v
        for b in range(NB):
            if b < NB - UNIT:
                v_high, c_high = column(old, p + UNIT, b + UNIT, width), column(cy_a, p, b + UNIT, width)
                t_high = c_high * v_high
            else:
                t_high = pltpu.roll(t_first, LAST, 1)
            c_x, c_z = column(cx_a, p, b, width + UNIT), column(cz_a, p, b, width)
            below, above = column(old, p, b, 1), column(old, p + width + UNIT, b, 1)
            if width > 1:
                below = jnp.concatenate([below, v[:width - UNIT]], axis=0)
                above = jnp.concatenate([v[1:], above], axis=0)
            new = c_x[:width] * below + c_x[1:] * above
            new = new + (c_y * v_low + t_high)
            new = new + (c_z * lane_down(v) + lane_up(c_z * v))
            new = HALF * new if k == 1 else new - column(b_a[k - 2], p + UNIT, b, width)
            b_a[k][pl.ds(p + UNIT, width), b] = new
            if own:
                carry = tally(carry, b, (column(v0_a, p, b, width) * new, v * new, new * new))
            v_low, v, c_y = v, v_high, c_high
        return tuple(carry)

    for k in range(1, STEPS):
        sums = lax.fori_loop(0, N // SUB, lambda n, carry: advance(k, True, SUB, SUB * n, carry), (zero,) * 6)
        if k < STEPS - UNIT:
            depth = (STEPS - k) // PAIR * PAIR
            advance(k, False, depth, N + (H - depth) * cx, ())
            wrap(b_a[k])
        acc[1 + k] = own_cells(sums[0], sums[1])
        acc[GROUPS + k - UNIT] = own_cells(sums[2], sums[3])
        if k < STEPS - UNIT:
            acc[TILES + k] = own_cells(sums[4], sums[PIECES])

    def gather(buf, n_sem):
        copies = []
        for n, flips in enumerate(OTHERS):
            copies.append(pltpu.make_async_remote_copy(
                src_ref=buf.at[me], dst_ref=buf.at[me], send_sem=all_send.at[n_sem, n], recv_sem=all_recv.at[n_sem, n],
                device_id=peer(*flips), device_id_type=MESH))
        for copy in copies:
            copy.start()
        return copies

    hi = acc[:, 0, :]
    lo = jnp.zeros((NDOT, LANES), F32)
    for s in range(1, SUB):
        hi, err = two_sum(hi, acc[:, s, :])
        lo = lo + err
    gath[me, 0:NDOT] = hi
    gath[me, NDOT:2 * NDOT] = lo
    gath_copies = gather(gath, 0)
    pair = {}
    for i in range(HEAD + UNIT):
        for j in range(i, HEAD + UNIT):
            pair[i, j] = len(pair)

    def products(n, carry):
        p, carry = WIDTH * n, list(carry)
        for b in range(NB):
            sd = k_nat[pl.ds(p, WIDTH), pl.ds(SUB * b, SUB), :]
            w = [sd * column(v0_a, p, b, WIDTH)] + [sd * column(b_a[j], p + UNIT, b, WIDTH) for j in range(HEAD)]
            for (i, j), at in pair.items():
                carry[at] = carry[at] + jnp.sum(w[i] * w[j], axis=0)
        return tuple(carry)
    gram = lax.fori_loop(0, N // WIDTH, products, (zero,) * len(pair))
    for copy in gath_copies:
        copy.wait()
    hi, lo = gath[0, 0:NDOT], gath[0, NDOT:2 * NDOT]
    for dev in range(1, SUB):
        hi, err = two_sum(hi, gath[dev, 0:NDOT])
        lo = lo + (gath[dev, NDOT:2 * NDOT] + err)
    for shift in (64, 32, GROUPS, SUB, 4, 2, 1):
        hi, err = two_sum(hi, pltpu.roll(hi, shift, 1))
        lo = (lo + pltpu.roll(lo, shift, 1)) + err
    hi, lo = quick(hi, lo)
    size = hi[0:1]
    factor = jnp.where(size > 1e30, TWO ** -110, jnp.where(size > 1e12, TWO ** -60, jnp.where(
        size < 1e-30, TWO ** 110, jnp.where(size < 1e-12, TWO ** 60, ONE)))).astype(F32)
    hi, lo = hi * factor, lo * factor

    def total(row):
        return jnp.broadcast_to(hi[row:row + UNIT], (SUB, LANES)), jnp.broadcast_to(lo[row:row + UNIT], (SUB, LANES))

    n_mom = [total(TILES), total(GROUPS)]
    for j in range(1, LAST):
        n_mom.append(dsub(dscale(total(TILES + j), TWO), n_mom[0]))
        n_mom.append(dsub(dscale(total(GROUPS + j), TWO), n_mom[1]))
    l_mom = [total(1 + j) for j in range(SUB)]
    for j in range(LAST, 14):
        l_mom.append(dsub(dscale(dsub(l_mom[j], n_mom[j]), TWO), l_mom[j - UNIT]))
    m_mom = [total(0)]
    m_mom.append(dsub(m_mom[0], l_mom[0]))
    for j in range(1, 15):
        m_mom.append(dsub(dscale(dsub(m_mom[j], l_mom[j]), TWO), m_mom[j - UNIT]))
    ys, xs = basis_coefs(*step_lengths(m_mom))
    slot = {}
    for t in range(STEPS):
        for j in range(t + UNIT):
            slot[t, j] = len(slot)
            coef[slot[t, j]] = ys[t][1 + j]
    for j in range(SUB):
        slot['x', j] = len(slot)
        coef[slot['x', j]] = xs[j]

    def put(ref, p, b0, val):
        for b in range(val.shape[0]):
            if b0 + b < 2:
                ref[p, pl.ds(b0 + b, SUB, stride=NB), :] = val[b, :, :N]
            else:
                ref[p, pl.ds(b0 + b, LAST, stride=NB), :] = val[b, :LAST, :N]

    def residuals(p, carry):
        carry = list(carry)
        for b0 in range(0, NB, 2):
            cut = pl.ds(b0, 2)
            v0 = v0_a[p, cut]
            sd = jnp.stack([k_nat[p, pl.ds(SUB * (b0 + b), SUB), :] for b in range(2)], axis=0)
            bs = [ref[p + UNIT, cut] for ref in b_a]
            for t in range(HEAD, STEPS):
                y = v0
                for j in range(t + UNIT):
                    y = y + coef[slot[t, j]] * bs[j]
                r = sd * y
                which = 2 * (t - HEAD) + (b0 > 0)
                carry[which] = carry[which] + jnp.sum(r * r, axis=0)
                if t == STEPS - UNIT:
                    put(f_in, p, b0, r)
        return tuple(carry)

    sums = lax.fori_loop(0, N, residuals, (zero,) * (2 * (STEPS - HEAD)))
    for t in range(STEPS):
        if t < HEAD:
            form = zero
            g = [None] + [coef[slot[t, j]] for j in range(t + 1)]
            for i in range(t + 2):
                part = gram[pair[0, i]] if not i else g[i] * gram[pair[0, i]]
                form = form + (part if not i else part + part)
            for i in range(UNIT, t + 2):
                part = zero
                for j in range(UNIT, t + 2):
                    part = part + g[j] * gram[pair[min(i, j), max(i, j)]]
                form = form + g[i] * part
            rsend[t] = pick(own_lane, form, zero)
        else:
            rsend[t] = own_cells(sums[2 * (t - HEAD)], sums[2 * (t - HEAD) + UNIT])
    part = rsend[:, 0, :]
    for s in range(1, SUB):
        part = part + rsend[:, s, :]
    rgath[me] = part
    rr_copies = gather(rgath, 1)

    def update(p, carry):
        for b0 in range(0, NB, 2):
            cut = pl.ds(b0, 2)
            x = coef[slot['x', 0]] * v0_a[p, cut]
            for j in range(1, SUB):
                x = x + coef[slot['x', j]] * b_a[j - UNIT][p + UNIT, cut]
            x = x * isd_a[p, cut]
            u = jnp.stack([u_nat[p, pl.ds(b0 + b, SUB, stride=NB), :] for b in range(2)], axis=0)
            put(k_in, p, b0, u + x)
        return carry

    lax.fori_loop(0, N, update, 0)
    for copy in rr_copies:
        copy.wait()
    part = rgath[0]
    for dev in range(1, SUB):
        part = part + rgath[dev]
    part = jnp.broadcast_to(jnp.sum(part, axis=1, keepdims=True), (SUB, LANES))
    rr_ref[...] = jnp.sum(jnp.where(lane == sub, part, ZERO), axis=0, keepdims=True)[:, :STEPS]


def solution(mesh):
    spec = P('gx', 'gy', 'gz')

    def local(k_cell, k_ghost, f_rhs, u_init):
        big = (E, NB, SUB, LANES)
        ext = (E + 2, NB, SUB, LANES)
        vm = lambda *shape: pltpu.VMEM(shape, F32)
        any_spec = pl.BlockSpec(memory_space=pl.ANY)
        u, r, rr = pl.pallas_call(
            kernel,
            out_shape=(vm(N, N, N), vm(N, N, N), vm(1, STEPS)),
            in_specs=[any_spec] * 4,
            out_specs=[pl.BlockSpec(memory_space=pltpu.VMEM)] * 3,
            scratch_shapes=[
                vm(N, N, N), vm(E + 2, E, LANES), vm(E, E, LANES), vm(E, E, LANES),
                vm(*ext), vm(*big), vm(*big), vm(*big), vm(N, NB, SUB, LANES),
                *[vm(E + 2, NB, SUB, LANES)] * STEPS,
                vm(3, 144, 144), vm(LANES, LANES), vm(LANES, LANES), vm(E, LANES), vm(N, SUB, N), vm(1, N, N), vm(1, N, N),
                vm(2, 45, SUB, LANES), vm(2, 45, SUB, LANES), vm(2, TILES, SUB, LANES), vm(2, TILES, SUB, LANES),
                vm(2, N, N), vm(2, N, N), vm(2, TILES, SUB, LANES), vm(2, TILES, SUB, LANES),
                vm(NDOT, SUB, LANES), vm(SUB, 2 * NDOT, LANES), vm(SUB, SUB, LANES), vm(SUB, SUB, LANES), vm(44, SUB, LANES),
                pltpu.SemaphoreType.DMA((6, 3)),
                pltpu.SemaphoreType.DMA((16,)), pltpu.SemaphoreType.DMA((16,)),
                pltpu.SemaphoreType.DMA((2, LAST)), pltpu.SemaphoreType.DMA((2, LAST)),
            ],
            compiler_params=pltpu.CompilerParams(collective_id=0, has_side_effects=True, vmem_limit_bytes=57 << 20),
        )(k_cell, f_rhs, u_init, k_ghost)
        return u, r, rr.reshape(STEPS)

    return jax.shard_map(local, mesh=mesh, in_specs=(spec, P(), spec, spec), out_specs=(spec, spec, P()), check_vma=False)
```

```python
import functools

import jax
import jax.numpy as jnp
from jax import lax
from jax.experimental import pallas as pl
from jax.experimental.pallas import tpu as pltpu
from jax.sharding import PartitionSpec as P


N = 72
H = 8
E = N + H
NB = 10
STEPS = 8
MESH = pl.DeviceIdType.MESH
F32 = jnp.float32
OTHERS = [(fx, fy, fz) for fx in (0, 1) for fy in (0, 1) for fz in (0, 1) if fx or fy or fz]
OTHERS.sort(key=lambda flips: -sum(flips[1:]))
NDOT = 24
SUB = 8
LANES = 128
TILES = 9
PART = 24
WIDTH = 4
LAST = 7
GROUPS = 16
PIECES = 5
ZERO, ONE, HALF, TWO = 0.0, 1.0, 0.5, 2.0
UNIT = 1
HEAD = 4
PAIR = 2


def iota(axis):
    return lax.broadcasted_iota(jnp.int32, (SUB, LANES), axis)


def two_sum(a, b):
    s = a + b
    t = s - a
    return s, (a - (s - t)) + (b - t)


def quick(a, b):
    s = a + b
    return s, b - (s - a)


def two_prod(a, b):
    def split(x):
        t = x * 4097.0
        hi = t - (t - x)
        return hi, x - hi
    p = a * b
    ah, al = split(a)
    bh, bl = split(b)
    return p, ((ah * bh - p) + ah * bl + al * bh) + al * bl


def dadd(x, y):
    (xh, xl), (yh, yl) = x, y
    s, e = two_sum(xh, yh)
    return quick(s, e + (xl + yl))


def dsub(x, y):
    yh, yl = y
    return dadd(x, (-yh, -yl))


def dscale(x, c):
    hi, lo = x
    return hi * c, lo * c


def dmul(x, y):
    (xh, xl), (yh, yl) = x, y
    p, e = two_prod(xh, yh)
    return quick(p, e + (xh * yl + xl * yh))


def ddiv(x, y):
    (xh, xl), (yh, yl) = x, y
    q = xh / yh
    p, e = two_prod(q, yh)
    rest = ((xh - p) - e) + (xl - q * yl)
    return quick(q, rest / yh)


def step_lengths(m):
    alphas, betas = [], []
    y = dict(enumerate(m))
    p = {0: dsub(y[0], y[1])}
    for l in range(1, 15):
        p[l] = dsub(y[l], dscale(dadd(y[l + UNIT], y[l - UNIT]), HALF))
    for t in range(STEPS):
        alpha = ddiv(y[t], p[t])
        alphas.append(alpha[0])
        if t == STEPS - UNIT:
            break
        y_next = {l: dsub(y[l], dmul(alpha, p[l])) for l in range(t + UNIT, 15 - t)}
        beta = ddiv(y_next[t + UNIT], p[t])
        if t:
            beta = dscale(beta, HALF)
        betas.append(beta[0])
        p_next = {}
        for l in range(t + UNIT, 14 - t):
            side = y_next[l + UNIT] if l == t + UNIT else dadd(y_next[l + UNIT], y_next[l - UNIT])
            p_next[l] = dadd(dsub(y_next[l], dscale(side, HALF)), dmul(beta, p[l]))
        y, p = y_next, p_next
    return alphas, betas


def basis_coefs(alphas, betas):
    def add(a, b):
        return b if a is None else (a if b is None else a + b)

    def axpy(x, c, y):
        return [xi if yi is None else (c * yi if xi is None else xi + c * yi) for xi, yi in zip(x, y)]

    def apply_op(v):
        out = [None] * 11
        out[1] = v[0]
        for j in range(SUB):
            if v[1 + j] is None:
                continue
            c = v[1 + j]
            out[1 + j] = add(out[1 + j], c)
            if j == 0:
                out[2] = add(out[2], -c)
            else:
                half = -HALF * c
                out[2 + j] = add(out[2 + j], half)
                out[j] = add(out[j], half)
        return out[:TILES]

    one = jnp.ones_like(alphas[0])
    y = [one] + [None] * SUB
    p = list(y)
    x = [None] * TILES
    ys = []
    for t in range(STEPS):
        q = apply_op(p)
        x = axpy(x, alphas[t], p)
        y = axpy(y, -alphas[t], q)
        ys.append(y)
        if t < STEPS - UNIT:
            p = axpy(y, betas[t], p)
    return ys, x


def row_down(v):
    return jnp.concatenate([pltpu.roll(v[NB - UNIT], 1, 0)[None], v[:NB - UNIT]], axis=0)


def row_up(v):
    return jnp.concatenate([v[1:], pltpu.roll(v[0], LAST, 0)[None]], axis=0)


def lane_down(v):
    return pltpu.roll(v, 1, 2)


def lane_up(v):
    return pltpu.roll(v, 127, 2)


def load_chunk(ref, plane):
    return jnp.stack([ref[plane, pl.ds(b, SUB, stride=NB), :] for b in range(NB)], axis=0)


def replace(v, b, mask, value):
    return jnp.concatenate(([v[:b]] if b else []) + [jnp.where(mask, value, v[b])[None], v[b + UNIT:]], axis=0)


def harmonic(a, b):
    return TWO * a * b / (a + b)


def pick(mask, a, b):
    return lax.select_n(mask, b, a)


def planes(lo, hi, body, init, width=WIDTH):
    def some(n, carry):
        for w in range(width):
            carry = body(lo + n * width + w, carry)
        return carry
    return lax.fori_loop(0, (hi - lo) // width, some, init)


def own_cells(low, high):
    sub, lane = iota(0), iota(1)
    return jnp.where(lane < N, low + jnp.where(sub < LAST, high, ZERO), ZERO)


def kernel(k_hbm, f_hbm, u_hbm, kg_hbm, k_in, f_in, rr_ref,
           u_in, k_nat, u_nat, z_nat, cx_a, cy_a, cz_a, isd_a, v0_a, b0_a, b1_a, b2_a, b3_a, b4_a, b5_a, b6_a, b7_a,
           walls, wz, wz_t, wy, ky, kx, ux, zs, zr, ds_, dr, row_s, row_r, lane_s, lane_r, acc, gath, rsend, rgath, coef,
           load_sem, send_sem, recv_sem, all_send, all_recv):
    cx, cy, cz = lax.axis_index('gx'), lax.axis_index('gy'), lax.axis_index('gz')
    me = cx + 2 * cy + 4 * cz
    b_a = (b0_a, b1_a, b2_a, b3_a, b4_a, b5_a, b6_a, b7_a)
    lane, sub = iota(1), iota(0)

    def peer(fx, fy, fz):
        out = {}
        if fx:
            out['gx'] = 1 - cx
        if fy:
            out['gy'] = 1 - cy
        if fz:
            out['gz'] = 1 - cz
        return out

    loads = []
    for n, (src, dst) in enumerate([(k_hbm, k_in), (u_hbm, u_in), (f_hbm, f_in)]):
        loads.append([pltpu.make_async_copy(src.at[pl.ds(PART * q, PART)], dst.at[pl.ds(PART * q, PART)], load_sem.at[n, q])
                      for q in range(N // PART)])
    loads.append([pltpu.make_async_copy(kg_hbm.at[cx], walls.at[0], load_sem.at[3, 0])])
    loads.append([pltpu.make_async_copy(kg_hbm.at[2 + cy], walls.at[1], load_sem.at[4, 0])])
    loads.append([pltpu.make_async_copy(kg_hbm.at[4 + cz], walls.at[2], load_sem.at[PIECES, 0])])
    for n in (0, 1, 3, 4, PIECES, 2):
        for copy in loads[n]:
            copy.start()

    barrier = pltpu.get_barrier_semaphore()
    for flips in OTHERS:
        pl.semaphore_signal(barrier, inc=1, device_id=peer(*flips), device_id_type=MESH)

    def send(n, src, dst, flips):
        copy = pltpu.make_async_remote_copy(src_ref=src, dst_ref=dst, send_sem=send_sem.at[n], recv_sem=recv_sem.at[n],
                                            device_id=peer(*flips), device_id_type=MESH)
        copy.start()
        return copy

    near_y = pl.multiple_of((N - H) * (1 - cy), SUB)
    near_x = (N - H) * (1 - cx)
    src8 = (N - H) * (1 - cz)
    dst8 = N + 48 * cz
    ghost8 = jnp.logical_and(lane >= dst8, lane < dst8 + SUB)
    wall_lane = 127 - 55 * cz
    own_lane = lane < N
    at_wall = lane == wall_lane
    zero = jnp.zeros((SUB, LANES), F32)
    ones = jnp.ones((SUB, LANES), F32)

    def turn(x, by):
        return pltpu.roll(x, lax.rem(by + LANES, LANES), 1)

    def shift(x, by):
        return pltpu.roll(x, by % LANES, 1) if by % LANES else x

    def widen(x):
        return x if x.shape[1] == LANES else jnp.concatenate([x, jnp.zeros((x.shape[0], LANES - x.shape[1]), F32)], axis=1)

    def pack(nat, packed, corner, lo, hi, width):
        group8 = lax.rem(lane + (LANES - src8), LANES) // SUB
        groups = [group8 == g for g in range(GROUPS)]

        def body(o, carry):
            for q in range(PIECES):
                out = None
                for g in range(min(GROUPS, N - GROUPS * q)):
                    t = GROUPS * q + g
                    if t % TILES == 0:
                        plane = widen(nat[o * SUB + t // TILES, 0:N, :])
                    x = shift(plane[SUB * (t % TILES):SUB * (t % TILES) + SUB], SUB * g)
                    out = x if g == 0 else pick(groups[g], x, out)
                packed[o * PIECES + q] = out
            out = None
            for g in range(SUB):
                x = widen(nat[o * SUB + g, pl.ds(near_y, SUB), :])
                x = shift(x, SUB * g)
                out = x if g == 0 else pick(groups[g], x, out)
            corner[o] = out
            return carry
        planes(lo, hi, body, 0, width)

    def unpack(own, side, nat, packed, corner, fill, wall, o, carry):
        by = dst8 - (N - H - src8)
        packs, corner_in = [turn(packed[o * PIECES + q], by) for q in range(PIECES)], turn(corner[o], by)
        for pi in range(SUB):
            i, out = o * SUB + pi, []
            plane = widen(own[i, 0:N, :])
            for jt in range(NB):
                if jt < TILES:
                    t = pi * TILES + jt
                    got, g = packs[t // GROUPS], t % GROUPS
                else:
                    got, g = corner_in, pi
                x = plane[SUB * jt:SUB * jt + SUB] if jt < TILES else widen(side[i])
                other = fill if wall is None else pick(at_wall, wall_column(i, jt), fill)
                out.append(pick(own_lane, x, pick(ghost8, shift(got, -SUB * g), other)))
            nat[i, 0:E, :] = jnp.concatenate(out, axis=0)
        return carry

    def wall_column(i, jt):
        at = SUB * jt if jt < TILES else pl.multiple_of(N + 48 * cy, SUB)
        return pltpu.roll(wz_t[pl.ds(at, SUB), :], LANES - UNIT - i, 1)

    for copy in loads[0] + loads[1]:
        copy.wait()
    last_x, last_y, last_z = (N - UNIT) * (1 - cx), (N - UNIT) * (1 - cy), (N - UNIT) * (1 - cz)

    slots = lax.rem(lane + (LANES - last_z), LANES)

    def pack_one(o, carry):
        for n, src in enumerate((k_in, u_in)):
            row_s[n, pl.ds(pl.multiple_of(o * SUB, SUB), SUB), :] = jnp.concatenate(
                [src[o * SUB + r, pl.ds(last_y, 1), :] for r in range(SUB)], axis=0)
            out = None
            for t in range(N):
                if t % TILES == 0:
                    plane = widen(src[o * SUB + t // TILES])
                x = shift(plane[SUB * (t % TILES):SUB * (t % TILES) + SUB], t)
                out = x if t == 0 else pick(slots == t, x, out)
            lane_s[n, o] = out
        return carry
    planes(0, TILES, pack_one, 0, 3)
    pl.semaphore_wait(barrier, len(OTHERS))
    one_x = [send(0, k_in.at[pl.ds(last_x, 1)], kx, (1, 0, 0)), send(1, u_in.at[pl.ds(last_x, 1)], ux, (1, 0, 0))]
    one_y = send(2, row_s, row_r, (0, 1, 0))
    one_z = send(3, lane_s, lane_r, (0, 0, 1))
    k_y = send(4, k_in.at[:, pl.ds(near_y, SUB), :], ky, (0, 1, 0))
    pack(k_in, zs.at[0], ds_.at[0], 0, TILES, UNIT)
    k_z = send(PIECES, zs.at[0], zr.at[0], (0, 0, 1))
    k_d = send(6, ds_.at[0], dr.at[0], (0, 1, 1))

    for n in (3, 4, PIECES):
        loads[n][0].wait()

    def lane_ring(w, at, c):
        left, right = walls[w, pl.ds(at, SUB), 0:LANES], walls[w, pl.ds(at, SUB), LANES:144]
        gap = jnp.zeros((SUB, 56), F32)
        right = jnp.concatenate([gap, right, gap], axis=1)
        turned = jnp.where(jnp.logical_and(lane >= 56, lane < N), right, pltpu.roll(left, 56, 1))
        return jnp.where(c == 0, left, turned)

    for jt in range(NB):
        at_j = pl.multiple_of(N * cy + SUB * jt if jt < TILES else N - H * cy, SUB)
        at_i = pl.multiple_of(N * cx + SUB * jt if jt < TILES else N - H * cx, SUB)
        k_nat[E, pl.ds(SUB * jt, SUB), :] = lane_ring(0, at_j, cz)
        wy[pl.ds(SUB * jt, SUB), :] = lane_ring(1, at_i, cz)
        if jt < TILES:
            wz[pl.ds(SUB * jt, SUB), :] = lane_ring(2, at_i, cy)
    wz_t[...] = turn(wz[...].T, wall_lane + UNIT)

    for copy in loads[2]:
        copy.wait()

    def take_f(p, carry):
        for b in range(NB):
            rows = SUB if b < 2 else LAST
            v0_a[p, b, 0:rows, 0:N] = f_in[p, pl.ds(b, rows, stride=NB), :]
        return carry
    planes(0, N, take_f, 0)

    def lay_out(i, carry):
        side = jnp.concatenate([pick(at_wall, wall_column(i, jt), ones) for jt in range(TILES)], axis=0)
        for nat, src, rest in ((k_nat, k_in, side), (u_nat, u_in, jnp.zeros((N, LANES), F32))):
            nat[i, 0:N, N:] = rest[:, N:]
            nat[i, 0:N, 0:N] = src[i]
        return carry
    planes(0, N, lay_out, 0)

    u_nat[E - UNIT - LAST * cx] = jnp.zeros((E, LANES), F32)
    one_lane = N + 55 * cz
    at_one = lane == one_lane
    for copy in one_x + [one_y, one_z]:
        copy.wait()
    u_nat[N + LAST * cx, 0:N, 0:N] = ux[0]
    k_nat[E + UNIT, 0:N, 0:N] = kx[0]

    def unpack_one(o, carry):
        for n, nat in enumerate((k_nat, u_nat)):
            got = turn(lane_r[n, o], one_lane - (N - 1 - last_z))
            for t in range(N):
                here = nat.at[o * SUB + t // TILES, pl.ds(SUB * (t % TILES), SUB), :]
                pltpu.store(here, shift(got, -t), mask=at_one)
        return carry
    lax.fori_loop(0, TILES, unpack_one, 0)

    row0 = sub == 0
    row72 = sub == LAST

    def divergence(h_x, h_xn, h_y, h_z, v, v_prev, v_next, low_row, high_row):
        low = row_down(v)
        high = v
        if low_row is not None:
            low = replace(low, 0, row0, low_row)
            high = replace(v, 2, row72, high_row)
        else:
            low = replace(low, 0, jnp.logical_and(row0, cy == 0), ZERO)
            high = replace(v, 2, jnp.logical_and(row72, cy == 1), ZERO)
        f_y = h_y * (high - low)
        f_z = h_z * (v - lane_down(v))
        return ((h_x * (v - v_prev) - h_xn * (v_next - v)) + (f_y - row_up(f_y))) + (f_z - lane_up(f_z))

    def full(row):
        return jnp.broadcast_to(widen(row), (SUB, LANES))

    def add_up(h_x, h_xn, h_y, h_z):
        return ((h_x + h_xn) + (h_y + row_up(h_y))) + (h_z + lane_up(h_z))

    def start_own(n, carry):
        p0 = WIDTH * n
        first_trip, last_trip = n == 0, n == N // WIDTH - UNIT
        k_p = [load_chunk(k_nat, jnp.where(first_trip, E + cx, p0 - UNIT))]
        u_p = [load_chunk(u_nat, jnp.where(first_trip, E - UNIT, p0 - UNIT))]
        for w in range(WIDTH):
            k_p.append(load_chunk(k_nat, p0 + w))
            u_p.append(load_chunk(u_nat, p0 + w))
        k_p.append(load_chunk(k_nat, jnp.where(last_trip, E + UNIT - cx, p0 + WIDTH)))
        u_p.append(load_chunk(u_nat, p0 + WIDTH))
        h_x = [harmonic(k_p[w + UNIT], k_p[w]) for w in range(WIDTH + UNIT)]
        for w in range(WIDTH):
            p, kc = p0 + w, k_p[w + UNIT]
            wall, got = full(wy[pl.ds(p, 1), :]), full(row_r[0, pl.ds(p, 1), :])
            low = replace(row_down(kc), 0, row0, jnp.where(cy == 0, wall, got))
            high = replace(kc, 2, row72, jnp.where(cy == 0, got, wall))
            h_y = harmonic(high, low)
            h_z = harmonic(kc, lane_down(kc))
            inv = lax.rsqrt(add_up(h_x[w], h_x[w + UNIT], h_y, h_z))
            got = full(row_r[1, pl.ds(p, 1), :])
            a_u = divergence(h_x[w], h_x[w + UNIT], h_y, h_z, u_p[w + UNIT], u_p[w], u_p[w + 2],
                             jnp.where(cy == 0, ZERO, got), jnp.where(cy == 0, got, ZERO))
            y0 = (v0_a[p] - a_u) * inv
            for b in range(NB):
                v0_a[p, b] = y0[b] if b < 2 else pick(row72, zero, y0[b])
            z0 = y0 * inv
            for b in range(NB):
                if b < 2:
                    z_nat[p, pl.ds(b, SUB, stride=NB), :] = z0[b]
                else:
                    z_nat[p, pl.ds(b, LAST, stride=NB), :] = z0[b, :LAST]
        return carry
    z_copies = []
    for q in range(3):
        lax.fori_loop(6 * q, 6 * q + 6, start_own, 0)
        rows = pl.ds(PART * q, PART)
        z_copies.append(send(7 + q, z_nat.at[rows, pl.ds(near_y, SUB), :], z_nat.at[rows, pl.ds(N, SUB), :], (0, 1, 0)))
        pack(z_nat, zs.at[1], ds_.at[1], 3 * q, 3 * q + 3, 3)
        lanes = pl.ds(15 * q, 15)
        z_copies.append(send(12 + q, zs.at[1, lanes], zr.at[1, lanes], (0, 0, 1)))
    z_copies.append(send(15, ds_.at[1], dr.at[1], (0, 1, 1)))

    def spread(n, nat, take):
        take(SUB * (1 - cx), 0)
        copy = send(n, nat.at[pl.ds(near_x, SUB)], nat.at[pl.ds(N, SUB)], (1, 0, 0))
        lax.fori_loop(0, SUB, lambda o, carry: take(o + cx, carry), 0)
        return copy

    for copy in (k_y, k_z, k_d):
        copy.wait()
    spread(NB, k_nat, functools.partial(unpack, k_in, ky, k_nat, zr.at[0], dr.at[0], ones, wz_t)).wait()

    def faces(p, carry):
        kc = load_chunk(k_nat, p)
        before = jnp.where(jnp.logical_and(p == 0, cx == 0), E, jnp.where(p == 0, E - UNIT, p - UNIT))
        here = jnp.where(jnp.logical_and(p == N, cx == 1), E, p)
        cx_a[p] = harmonic(load_chunk(k_nat, here), load_chunk(k_nat, before))
        wall = full(wy[pl.ds(p, 1), :])
        low = replace(row_down(kc), 0, jnp.logical_and(row0, cy == 0), wall)
        high = replace(kc, 2, jnp.logical_and(row72, cy == 1), wall)
        cy_a[p] = harmonic(high, low)
        cz_a[p] = harmonic(kc, lane_down(kc))
        return carry
    planes(0, E, faces, 0, SUB)
    cx_a[E] = cx_a[0]
    cx_a[E + UNIT] = cx_a[1]

    def scales(own, p, carry):
        d = add_up(cx_a[p], cx_a[p + UNIT], cy_a[p], cz_a[p])
        inv = lax.rsqrt(d)
        isd_a[p] = inv
        if own:
            sd = d * inv
            for b in range(NB):
                k_nat[p, pl.ds(SUB * b, SUB), :] = sd[b] if b < 2 else pick(row72, zero, sd[b])
        return carry
    planes(0, N, functools.partial(scales, True), 0, SUB)
    planes(N, E, functools.partial(scales, False), 0, SUB)

    for copy in z_copies:
        copy.wait()
    z_x = spread(11, z_nat, functools.partial(unpack, z_nat, z_nat.at[:, pl.ds(N, SUB), :], z_nat, zr.at[1], dr.at[1],
                                              zero, None))

    def column(ref, p, b, width):
        return ref[pl.ds(p, width), b]

    def z_column(p, b, width=1):
        return z_nat[pl.ds(p, width), pl.ds(b, SUB, stride=NB), :]

    def tally(carry, b, products):
        return [c + jnp.sum(products[n // 2], axis=0) if n % 2 == (b > 1) else c for n, c in enumerate(carry)]

    def first(own, width, p, carry, before=None, after=None, x_after=None):
        before = p - UNIT if before is None else before
        z, inv, low, f_y, h_y = {}, {}, {}, {}, {}

        def load(b):
            z[b], inv[b], h_y[b] = z_column(p, b, width), column(isd_a, p, b, width), column(cy_a, p, b, width)
            under = z[b - UNIT] if b else pltpu.roll(z_column(p, NB - UNIT, width), 1, 1)
            over = z[b]
            if b == 0:
                under = jnp.where(jnp.logical_and(row0, cy == 0), ZERO, under)
            if b == 2:
                over = jnp.where(jnp.logical_and(row72, cy == 1), ZERO, over)
            f_y[b] = h_y[b] * (over - under)
        carry = list(carry)
        load(0)
        for b in range(NB):
            if b < NB - UNIT:
                load(b + UNIT)
            up = f_y[b + UNIT] if b < NB - UNIT else pltpu.roll(f_y[0], LAST, 1)
            z_p = z_column(before, b)
            z_n = z_column(p + width if after is None else after, b)
            if isinstance(p, int) and p == 0:
                z_p = jnp.where(cx == 0, ZERO, z_p)
            if isinstance(p, int) and p == N - UNIT:
                z_n = jnp.where(cx == 1, ZERO, z_n)
            if x_after is None:
                h_x = column(cx_a, p, b, width + UNIT)
            else:
                h_x = jnp.concatenate([column(cx_a, p, b, 1), column(cx_a, x_after, b, 1)], axis=0)
            f_x = h_x * (jnp.concatenate([z[b], z_n], axis=0) - jnp.concatenate([z_p, z[b]], axis=0))
            h_z = column(cz_a, p, b, width)
            f_z = h_z * (z[b] - lane_down(z[b]))
            b0 = inv[b] * (((f_x[:width] - f_x[1:]) + (f_y[b] - up)) + (f_z - lane_up(f_z)))
            b_a[0][pl.ds(p + UNIT, width), b] = b0
            twice = TWO * inv[b]
            side = column(isd_a, before, b, 1)
            if width > 1:
                side = jnp.concatenate([side, inv[b][:width - UNIT]], axis=0)
            cx_a[pl.ds(p, width), b] = h_x[:width] * (twice * side)
            side = inv[b - UNIT] if b else pltpu.roll(column(isd_a, p, NB - UNIT, width), 1, 1)
            c_y = h_y[b] * (twice * side)
            if b == 0:
                c_y = jnp.where(jnp.logical_and(row0, cy == 0), ZERO, c_y)
            if b == 2:
                c_y = jnp.where(jnp.logical_and(row72, cy == 1), ZERO, c_y)
            cy_a[pl.ds(p, width), b] = c_y
            cz_a[pl.ds(p, width), b] = jnp.where(at_edge, ZERO, h_z * (twice * lane_down(inv[b])))
            if own:
                v0 = column(v0_a, p, b, width)
                carry = tally(carry, b, (v0 * v0, v0 * b0, b0 * b0))
        return tuple(carry)

    at_edge = lane == N * cz

    def wrap(ref):
        ref[0] = jnp.where(cx == 0, ref[1], ref[E])
        ref[E + UNIT] = ref[1]
        ref[N + UNIT] = jnp.where(cx == 1, ref[N], ref[N + UNIT])

    sums = lax.fori_loop(0, 14, lambda n, carry: first(True, PIECES, 1 + PIECES * n, carry), (zero,) * 6)
    z_x.wait()
    sums = first(True, 1, 0, sums, E - UNIT, None, E + UNIT)
    sums = first(True, 1, N - UNIT, sums)
    first(False, WIDTH, N, ())
    first(False, WIDTH, N + WIDTH, (), None, 0)
    cx_a[0] = jnp.where(cx == 0, ZERO, cx_a[0])
    cx_a[N] = jnp.where(cx == 1, ZERO, cx_a[N])
    cx_a[E] = cx_a[0]
    wrap(b_a[0])
    acc[0] = own_cells(sums[0], sums[1])
    acc[1] = own_cells(sums[2], sums[3])
    acc[TILES] = own_cells(sums[4], sums[PIECES])
    acc[23] = zero

    def advance(k, own, width, p, carry):
        old, carry = b_a[k - UNIT], list(carry)
        v_low = pltpu.roll(column(old, p + UNIT, NB - UNIT, width), 1, 1)
        v, c_y = column(old, p + UNIT, 0, width), column(cy_a, p, 0, width)
        t_first = c_y * v
        for b in range(NB):
            if b < NB - UNIT:
                v_high, c_high = column(old, p + UNIT, b + UNIT, width), column(cy_a, p, b + UNIT, width)
                t_high = c_high * v_high
            else:
                t_high = pltpu.roll(t_first, LAST, 1)
            c_x, c_z = column(cx_a, p, b, width + UNIT), column(cz_a, p, b, width)
            below, above = column(old, p, b, 1), column(old, p + width + UNIT, b, 1)
            if width > 1:
                below = jnp.concatenate([below, v[:width - UNIT]], axis=0)
                above = jnp.concatenate([v[1:], above], axis=0)
            new = c_x[:width] * below + c_x[1:] * above
            new = new + (c_y * v_low + t_high)
            new = new + (c_z * lane_down(v) + lane_up(c_z * v))
            new = HALF * new if k == 1 else new - column(b_a[k - 2], p + UNIT, b, width)
            b_a[k][pl.ds(p + UNIT, width), b] = new
            if own:
                carry = tally(carry, b, (column(v0_a, p, b, width) * new, v * new, new * new))
            v_low, v, c_y = v, v_high, c_high
        return tuple(carry)

    for k in range(1, STEPS):
        sums = lax.fori_loop(0, N // SUB, lambda n, carry: advance(k, True, SUB, SUB * n, carry), (zero,) * 6)
        if k < STEPS - UNIT:
            depth = (STEPS - k) // PAIR * PAIR
            advance(k, False, depth, N + (H - depth) * cx, ())
            wrap(b_a[k])
        acc[1 + k] = own_cells(sums[0], sums[1])
        acc[GROUPS + k - UNIT] = own_cells(sums[2], sums[3])
        if k < STEPS - UNIT:
            acc[TILES + k] = own_cells(sums[4], sums[PIECES])

    def gather(buf, n_sem):
        copies = []
        for n, flips in enumerate(OTHERS):
            copies.append(pltpu.make_async_remote_copy(
                src_ref=buf.at[me], dst_ref=buf.at[me], send_sem=all_send.at[n_sem, n], recv_sem=all_recv.at[n_sem, n],
                device_id=peer(*flips), device_id_type=MESH))
        for copy in copies:
            copy.start()
        return copies

    hi = acc[:, 0, :]
    lo = jnp.zeros((NDOT, LANES), F32)
    for s in range(1, SUB):
        hi, err = two_sum(hi, acc[:, s, :])
        lo = lo + err
    gath[me, 0:NDOT] = hi
    gath[me, NDOT:2 * NDOT] = lo
    gath_copies = gather(gath, 0)
    pair = {}
    for i in range(HEAD + UNIT):
        for j in range(i, HEAD + UNIT):
            pair[i, j] = len(pair)

    def products(n, carry):
        p, carry = WIDTH * n, list(carry)
        for b in range(NB):
            sd = k_nat[pl.ds(p, WIDTH), pl.ds(SUB * b, SUB), :]
            w = [sd * column(v0_a, p, b, WIDTH)] + [sd * column(b_a[j], p + UNIT, b, WIDTH) for j in range(HEAD)]
            for (i, j), at in pair.items():
                carry[at] = carry[at] + jnp.sum(w[i] * w[j], axis=0)
        return tuple(carry)
    gram = lax.fori_loop(0, N // WIDTH, products, (zero,) * len(pair))
    for copy in gath_copies:
        copy.wait()
    hi, lo = gath[0, 0:NDOT], gath[0, NDOT:2 * NDOT]
    for dev in range(1, SUB):
        hi, err = two_sum(hi, gath[dev, 0:NDOT])
        lo = lo + (gath[dev, NDOT:2 * NDOT] + err)
    for shift in (64, 32, GROUPS, SUB, 4, 2, 1):
        hi, err = two_sum(hi, pltpu.roll(hi, shift, 1))
        lo = (lo + pltpu.roll(lo, shift, 1)) + err
    hi, lo = quick(hi, lo)
    size = hi[0:1]
    factor = jnp.where(size > 1e30, TWO ** -110, jnp.where(size > 1e12, TWO ** -60, jnp.where(
        size < 1e-30, TWO ** 110, jnp.where(size < 1e-12, TWO ** 60, ONE)))).astype(F32)
    hi, lo = hi * factor, lo * factor

    def total(row):
        return jnp.broadcast_to(hi[row:row + UNIT], (SUB, LANES)), jnp.broadcast_to(lo[row:row + UNIT], (SUB, LANES))

    n_mom = [total(TILES), total(GROUPS)]
    for j in range(1, LAST):
        n_mom.append(dsub(dscale(total(TILES + j), TWO), n_mom[0]))
        n_mom.append(dsub(dscale(total(GROUPS + j), TWO), n_mom[1]))
    l_mom = [total(1 + j) for j in range(SUB)]
    for j in range(LAST, 14):
        l_mom.append(dsub(dscale(dsub(l_mom[j], n_mom[j]), TWO), l_mom[j - UNIT]))
    m_mom = [total(0)]
    m_mom.append(dsub(m_mom[0], l_mom[0]))
    for j in range(1, 15):
        m_mom.append(dsub(dscale(dsub(m_mom[j], l_mom[j]), TWO), m_mom[j - UNIT]))
    ys, xs = basis_coefs(*step_lengths(m_mom))
    slot = {}
    for t in range(STEPS):
        for j in range(t + UNIT):
            slot[t, j] = len(slot)
            coef[slot[t, j]] = ys[t][1 + j]
    for j in range(SUB):
        slot['x', j] = len(slot)
        coef[slot['x', j]] = xs[j]

    def put(ref, p, b0, val):
        for b in range(val.shape[0]):
            if b0 + b < 2:
                ref[p, pl.ds(b0 + b, SUB, stride=NB), :] = val[b, :, :N]
            else:
                ref[p, pl.ds(b0 + b, LAST, stride=NB), :] = val[b, :LAST, :N]

    def residuals(p, carry):
        carry = list(carry)
        for b0 in range(0, NB, 2):
            cut = pl.ds(b0, 2)
            v0 = v0_a[p, cut]
            sd = jnp.stack([k_nat[p, pl.ds(SUB * (b0 + b), SUB), :] for b in range(2)], axis=0)
            bs = [ref[p + UNIT, cut] for ref in b_a]
            for t in range(HEAD, STEPS):
                y = v0
                for j in range(t + UNIT):
                    y = y + coef[slot[t, j]] * bs[j]
                r = sd * y
                which = 2 * (t - HEAD) + (b0 > 0)
                carry[which] = carry[which] + jnp.sum(r * r, axis=0)
                if t == STEPS - UNIT:
                    put(f_in, p, b0, r)
        return tuple(carry)

    sums = lax.fori_loop(0, N, residuals, (zero,) * (2 * (STEPS - HEAD)))
    for t in range(STEPS):
        if t < HEAD:
            form = zero
            g = [None] + [coef[slot[t, j]] for j in range(t + 1)]
            for i in range(t + 2):
                part = gram[pair[0, i]] if not i else g[i] * gram[pair[0, i]]
                form = form + (part if not i else part + part)
            for i in range(UNIT, t + 2):
                part = zero
                for j in range(UNIT, t + 2):
                    part = part + g[j] * gram[pair[min(i, j), max(i, j)]]
                form = form + g[i] * part
            rsend[t] = pick(own_lane, form, zero)
        else:
            rsend[t] = own_cells(sums[2 * (t - HEAD)], sums[2 * (t - HEAD) + UNIT])
    part = rsend[:, 0, :]
    for s in range(1, SUB):
        part = part + rsend[:, s, :]
    rgath[me] = part
    rr_copies = gather(rgath, 1)

    def update(p, carry):
        for b0 in range(0, NB, 2):
            cut = pl.ds(b0, 2)
            x = coef[slot['x', 0]] * v0_a[p, cut]
            for j in range(1, SUB):
                x = x + coef[slot['x', j]] * b_a[j - UNIT][p + UNIT, cut]
            x = x * isd_a[p, cut]
            u = jnp.stack([u_nat[p, pl.ds(b0 + b, SUB, stride=NB), :] for b in range(2)], axis=0)
            put(k_in, p, b0, u + x)
        return carry

    lax.fori_loop(0, N, update, 0)
    for copy in rr_copies:
        copy.wait()
    part = rgath[0]
    for dev in range(1, SUB):
        part = part + rgath[dev]
    part = jnp.broadcast_to(jnp.sum(part, axis=1, keepdims=True), (SUB, LANES))
    rr_ref[...] = jnp.sum(jnp.where(lane == sub, part, ZERO), axis=0, keepdims=True)[:, :STEPS]


def solution(mesh):
    spec = P('gx', 'gy', 'gz')

    def local(k_cell, k_ghost, f_rhs, u_init):
        big = (E, NB, SUB, LANES)
        ext = (E + 2, NB, SUB, LANES)
        vm = lambda *shape: pltpu.VMEM(shape, F32)
        any_spec = pl.BlockSpec(memory_space=pl.ANY)
        u, r, rr = pl.pallas_call(
            kernel,
            out_shape=(vm(N, N, N), vm(N, N, N), vm(1, STEPS)),
            in_specs=[any_spec] * 4,
            out_specs=[pl.BlockSpec(memory_space=pltpu.VMEM)] * 3,
            scratch_shapes=[
                vm(N, N, N), vm(E + 2, E, LANES), vm(E, E, LANES), vm(E, E, LANES),
                vm(*ext), vm(*big), vm(*big), vm(*big), vm(N, NB, SUB, LANES),
                *[vm(E + 2, NB, SUB, LANES)] * STEPS,
                vm(3, 144, 144), vm(LANES, LANES), vm(LANES, LANES), vm(E, LANES), vm(N, SUB, N), vm(1, N, N), vm(1, N, N),
                vm(2, 45, SUB, LANES), vm(2, 45, SUB, LANES), vm(2, TILES, SUB, LANES), vm(2, TILES, SUB, LANES),
                vm(2, N, N), vm(2, N, N), vm(2, TILES, SUB, LANES), vm(2, TILES, SUB, LANES),
                vm(NDOT, SUB, LANES), vm(SUB, 2 * NDOT, LANES), vm(SUB, SUB, LANES), vm(SUB, SUB, LANES), vm(44, SUB, LANES),
                pltpu.SemaphoreType.DMA((6, 3)),
                pltpu.SemaphoreType.DMA((16,)), pltpu.SemaphoreType.DMA((16,)),
                pltpu.SemaphoreType.DMA((2, LAST)), pltpu.SemaphoreType.DMA((2, LAST)),
            ],
            compiler_params=pltpu.CompilerParams(collective_id=0, has_side_effects=True, vmem_limit_bytes=57 << 20),
        )(k_cell, f_rhs, u_init, k_ghost)
        return u, r, rr.reshape(STEPS)

    return jax.shard_map(local, mesh=mesh, in_specs=(spec, P(), spec, spec), out_specs=(spec, spec, P()), check_vma=False)
```
